256 devices in a mesh: seg: 256 (over x, z, y, core).
Axes of the slice: x: 4, y: 4, z: 8, core: 2. Of those that a mesh axis runs over, the one named last changes fastest.
Arguments:
- cam_jac: bfloat16 [18, 4096, 512], P(None, 'seg'), may hold values from -0.25 to 0.25
- point_jac: bfloat16 [6, 4096, 512], P(None, 'seg'), may hold values from -6 to 6
- obs_point: int32 [4096, 512], P('seg'), may hold values from 0 to 1791, as said below
- obs_count: int32 [4096], P('seg'), may hold values from 64 to 512, as said below
- back_list: int32 [256, 384], P('seg'), may hold values from 0 to 1023, as said below
- front_list: int32 [256, 384], P('seg'), may hold values from 0 to 1023, as said below
- point_damp: float32 [262144], P('seg'), may hold values from 0.5 to 4
- cam_damp: float32 [4096], P('seg'), may hold values from 0.1 to 1
- right_side: float32 [9, 4096], P(None, 'seg'), may hold values from -25 to 25
- start_guess: float32 [9, 4096], P(None, 'seg'), may hold values from -3 to 3
Outputs:
- camera_step: float32 [9, 4096], P(None, 'seg')
- residual: float32 [9, 4096], P(None, 'seg')
The draws below stay inside these ranges and needn't reach their ends.
Inputs may be any that keep to these rules, and one draw needn't show every extreme that they name: `obs_point`: entries below 1024 name the segment's own points; an entry e from 1024 to 1407 names entry e - 1024 of the previous segment's back_list, and a larger one entry e - 1408 of the next segment's front_list. Keyframes of the first segment name no back slot, those of the last segment no front slot. `obs_count`: slots at or past a keyframe's count are padding. Every segment has a keyframe whose slots are all used. `back_list`: each row holds 384 distinct own points of the segment; no point stands on both lists of its segment. `front_list`: each row holds 384 distinct own points of the segment; no point stands on both lists of its segment.
All inputs are finite; a program needn't handle non-finite values.
Results may differ from the reference program's by a relative error of at most 0.0005.
Values sent between devices are 32-bit elements; how exact they have to be, the bound alone decides.
No kernel may reach another device: no remote copies, remote signals or barrier semaphores. Data moves between devices by JAX's collectives and lax.ppermute only.
A program may use at most 64 MiB of HBM per device.

```python
import math
import jax
import jax.numpy as jnp
from jax import lax

CAM_DEV = 16
OBS_CAM = 512
P_DEV = 1024
ITERS = 2
BORDER = 384
SEGMENTS = 256
CAMERAS = 4096
POINTS = 262144


def border_lists(key):
    seg_keys = jax.random.split(jax.random.fold_in(key, 11), SEGMENTS)
    orders = jax.vmap(lambda seg_key: jax.random.permutation(seg_key, P_DEV))(seg_keys)
    return (orders[:, :BORDER].astype(jnp.int32), orders[:, BORDER:2 * BORDER].astype(jnp.int32))


def draw_back_list(key, part):
    return border_lists(key)[0]


def draw_front_list(key, part):
    return border_lists(key)[1]


def draw_obs_point(key, part):
    side_key, own_key, slot_key = jax.random.split(jax.random.fold_in(key, 3), 3)
    side_pick = jax.random.randint(side_key, (CAMERAS, OBS_CAM), 0, 4)
    segment = (jnp.arange(CAMERAS, dtype=jnp.int32) // CAM_DEV)[:, None]
    own_pick = jax.random.randint(own_key, (CAMERAS, OBS_CAM), 0, P_DEV)
    slot_pick = jax.random.randint(slot_key, (CAMERAS, OBS_CAM), 0, BORDER)
    back_side = (side_pick == 0) & (segment > 0)
    front_side = (side_pick == 1) & (segment < SEGMENTS - 1)
    result = jnp.where(back_side, P_DEV + slot_pick, jnp.where(front_side, P_DEV + BORDER + slot_pick, own_pick))
    return result.astype(jnp.int32)


def draw_obs_count(key, part):
    high_key, count_key, full_key = jax.random.split(jax.random.fold_in(key, 5), 3)
    high_cap = jax.random.randint(high_key, (SEGMENTS,), OBS_CAM // 2, OBS_CAM + 1)
    high_rows = jnp.repeat(high_cap, CAM_DEV)
    low_rows = high_rows // 4
    counts = jax.random.randint(count_key, (CAMERAS,), low_rows, high_rows + 1)
    full_pos = jnp.repeat(jax.random.randint(full_key, (SEGMENTS,), 0, CAM_DEV), CAM_DEV)
    marked = jnp.arange(CAMERAS, dtype=jnp.int32) % CAM_DEV == full_pos
    return jnp.where(marked, OBS_CAM, counts).astype(jnp.int32)


def draw_right_side(key, part):
    first_key = jax.random.fold_in(jax.random.fold_in(key, 9), 0)
    position = jnp.arange(CAMERAS, dtype=jnp.float32) / CAMERAS
    random_part = jnp.clip(jax.random.normal(first_key, (9, CAMERAS), jnp.float32), -6.0, 6.0)
    rising = 3.0 ** position
    return (random_part * rising[None, :]).astype(jnp.float32)


def steps_of(key, extent, pieces, low, top_value):
    def one(dim, shards_of):
        steps = jax.random.uniform(jax.random.fold_in(jax.random.fold_in(key, 6), dim), (shards_of,), jnp.float32, low / len(pieces), top_value / len(pieces))
        return jnp.repeat(jnp.exp(steps), extent[dim] // shards_of).reshape((-1,) + (1,) * (len(extent) - dim - 1))

    gain = one(*pieces[0])
    for cut in pieces[1:]:
        gain = gain * one(*cut)
    return gain


def scatter_about(rng, shape, width, most, pieces=(), kind=jnp.bfloat16):
    values = width * jax.random.normal(rng, shape, jnp.float32)
    if pieces:
        values = values * steps_of(rng, shape, pieces, -0.22, 0.18)
    return jnp.clip(values, -most, most).astype(kind)


def setup_inputs(seed: int = 0) -> dict:
    arg_keys = jax.random.split(jax.random.key(seed), 11)
    cam_jac = scatter_about(arg_keys[0], (18, CAMERAS, OBS_CAM), OBS_CAM ** -0.5, 0.25, ((1, 256),))
    point_jac = scatter_about(arg_keys[1], (6, CAMERAS, OBS_CAM), 1.0, 6.0, ((1, 256),))
    obs_point = draw_obs_point(jax.random.fold_in(arg_keys[10], 71), 0)
    obs_count = draw_obs_count(jax.random.fold_in(arg_keys[10], 71), 0)
    back_list = draw_back_list(jax.random.fold_in(arg_keys[10], 71), 0)
    front_list = draw_front_list(jax.random.fold_in(arg_keys[10], 71), 0)
    point_damp = jnp.clip(jnp.exp(math.log(4.0) - 2.0794415 * jax.random.uniform(arg_keys[6], (POINTS,), jnp.float32) ** steps_of(arg_keys[6], (POINTS,), ((0, 256),), -0.2, 0.2)), 0.5, 4.0)
    cam_damp = jnp.clip(jnp.exp(math.log(1.0) - 2.3025851 * jax.random.uniform(arg_keys[7], (CAMERAS,), jnp.float32) ** steps_of(arg_keys[7], (CAMERAS,), ((0, 256),), -0.2, 0.2)), 0.1, 1.0)
    right_side = draw_right_side(jax.random.fold_in(arg_keys[10], 71), 0)
    start_guess = scatter_about(arg_keys[9], (9, CAMERAS), 0.5, 3.0, ((1, 256),), jnp.float32)
    return {"cam_jac": cam_jac, "point_jac": point_jac, "obs_point": obs_point, "obs_count": obs_count, "back_list": back_list, "front_list": front_list, "point_damp": point_damp, "cam_damp": cam_damp, "right_side": right_side, "start_guess": start_guess}


ENTRY_PAIRS = ((0, 0), (0, 1), (0, 2), (1, 1), (1, 2), (2, 2))


def slot_weights(obs_count, slot_total):
    positions = lax.broadcasted_iota(jnp.int32, (obs_count.shape[0], slot_total), 1)
    return (positions < obs_count[:, None]).astype(jnp.float32)


def global_points(obs_point, back_list, front_list):
    segment = (jnp.arange(obs_point.shape[0], dtype=jnp.int32) // CAM_DEV)[:, None]
    prev_seg = jnp.clip(segment - 1, 0, SEGMENTS - 1)
    next_seg = jnp.clip(segment + 1, 0, SEGMENTS - 1)
    back_slot = jnp.clip(obs_point - P_DEV, 0, BORDER - 1)
    front_slot = jnp.clip(obs_point - P_DEV - BORDER, 0, BORDER - 1)
    own_global = segment * P_DEV + obs_point
    from_back = prev_seg * P_DEV + back_list[prev_seg, back_slot]
    from_front = next_seg * P_DEV + front_list[next_seg, front_slot]
    result = jnp.where(obs_point < P_DEV, own_global, jnp.where(obs_point < P_DEV + BORDER, from_back, from_front))
    return result.astype(jnp.int32).reshape(-1)


def symmetric_inverse(entries):
    cofactors = [entries[3] * entries[5] - entries[4] * entries[4],
                 entries[2] * entries[4] - entries[1] * entries[5],
                 entries[1] * entries[4] - entries[2] * entries[3],
                 entries[0] * entries[5] - entries[2] * entries[2],
                 entries[1] * entries[2] - entries[0] * entries[4],
                 entries[0] * entries[3] - entries[1] * entries[1]]
    determinant = entries[0] * cofactors[0] + entries[1] * cofactors[1] + entries[2] * cofactors[2]
    return [member / determinant for member in cofactors]


def apply_inverse(inverse, point_sums):
    return [inverse[0] * point_sums[0] + inverse[1] * point_sums[1] + inverse[2] * point_sums[2],
            inverse[1] * point_sums[0] + inverse[3] * point_sums[1] + inverse[4] * point_sums[2],
            inverse[2] * point_sums[0] + inverse[4] * point_sums[1] + inverse[5] * point_sums[2]]


def camera_rows(cam_jac, vector, weights):
    error_rows = []
    for row_index in range(2):
        running = cam_jac[9 * row_index].astype(jnp.float32) * vector[0][:, None]
        for column in range(1, 9):
            running = running + cam_jac[9 * row_index + column].astype(jnp.float32) * vector[column][:, None]
        error_rows.append(running * weights)
    return error_rows


def schur_apply(vector, cam_jac, point_jac, weights, owners, inverse, cam_damp):
    errors = camera_rows(cam_jac, vector, weights)
    point_sums = []
    for column in range(3):
        product = errors[0] * point_jac[column].astype(jnp.float32) + errors[1] * point_jac[3 + column].astype(jnp.float32)
        point_sums.append(jax.ops.segment_sum(product.reshape(-1), owners, num_segments=POINTS))
    values = apply_inverse(inverse, point_sums)
    picked = [member[owners].reshape(weights.shape) for member in values]
    adjusted = []
    for row_index in range(2):
        back_term = picked[0] * point_jac[3 * row_index].astype(jnp.float32)
        back_term = back_term + picked[1] * point_jac[3 * row_index + 1].astype(jnp.float32)
        back_term = back_term + picked[2] * point_jac[3 * row_index + 2].astype(jnp.float32)
        adjusted.append(errors[row_index] - weights * back_term)
    result = []
    for column in range(9):
        running = jnp.sum(cam_jac[column].astype(jnp.float32) * adjusted[0] + cam_jac[9 + column].astype(jnp.float32) * adjusted[1], axis=1)
        result.append(cam_damp * vector[column] + running)
    return jnp.stack(result)


def reference(cam_jac, point_jac, obs_point, obs_count, back_list, front_list, point_damp, cam_damp, right_side, start_guess):
    weights = slot_weights(obs_count, obs_point.shape[1])
    owners = global_points(obs_point, back_list, front_list)
    entries = []
    for lead_index, tail_index in ENTRY_PAIRS:
        product = point_jac[lead_index].astype(jnp.float32) * point_jac[tail_index].astype(jnp.float32)
        product = product + point_jac[3 + lead_index].astype(jnp.float32) * point_jac[3 + tail_index].astype(jnp.float32)
        running = jax.ops.segment_sum((product * weights).reshape(-1), owners, num_segments=POINTS)
        if lead_index == tail_index:
            running = running + point_damp
        entries.append(running)
    inverse = symmetric_inverse(entries)
    diagonal = []
    for column in range(9):
        first_sq = cam_jac[column].astype(jnp.float32) ** 2 + cam_jac[9 + column].astype(jnp.float32) ** 2
        diagonal.append(jnp.sum(first_sq * weights, axis=1) + cam_damp)
    precond = 1.0 / jnp.stack(diagonal)

    def operator(vector):
        return schur_apply(vector, cam_jac, point_jac, weights, owners, inverse, cam_damp)

    solution = start_guess
    residual = right_side - operator(solution)
    scaled = precond * residual
    direction = scaled
    inner_now = jnp.sum(residual * scaled)
    for iteration in range(ITERS):
        image = operator(direction)
        step_size = inner_now / jnp.sum(direction * image)
        solution = solution + step_size * direction
        residual = residual - step_size * image
        if iteration + 1 < ITERS:
            scaled = precond * residual
            inner_next = jnp.sum(residual * scaled)
            direction = scaled + (inner_next / inner_now) * direction
            inner_now = inner_next
    return solution, residual
```

```python
import functools

import jax
import jax.numpy as jnp
from jax import lax
from jax.experimental import pallas as pl
from jax.experimental.pallas import tpu as pltpu
from jax.sharding import PartitionSpec as P

F32 = jnp.float32
BF16 = jnp.bfloat16
I32 = jnp.int32
LANES = 128
ENTRY_PAIRS = ((0, 0), (0, 1), (0, 2), (1, 1), (1, 2), (2, 2))

SIDE = 6
LIST_ROWS = 3
NEXT_SLOTS = 3
PREV_SLOTS = 6
OWN_FRONT = 9
INTERIOR = 12
ROWS = 14
PAD_ROWS = 16


def row_of(block, index, rows):
    return jnp.broadcast_to(block[index : index + 1, :], (rows, block.shape[1]))


def sub_iota(rows, width):
    return lax.broadcasted_iota(I32, (rows, width), 0)


def lane_iota(rows, width):
    return lax.broadcasted_iota(I32, (rows, width), 1)


def nt(left, right, **kw):
    return lax.dot_general(
        left, right, (((1,), (1,)), ((), ())), preferred_element_type=F32, **kw
    )


def split_two(value):
    high = value.astype(BF16)
    low = (value - high.astype(F32)).astype(BF16)
    return high.astype(F32), low.astype(F32)


def columns(block):
    eye = (sub_iota(16, 16) == lane_iota(16, 16)).astype(F32)
    return nt(eye, block, precision=lax.Precision.HIGHEST)


def one_hot_rows(index_row, rows, width):
    packed = jnp.broadcast_to(index_row, (16, width)).astype(BF16)
    parts = []
    for start in range(0, rows, 16):
        ids = (sub_iota(16, width) + start).astype(F32).astype(BF16)
        parts.append(jnp.where(packed == ids, jnp.ones_like(packed), jnp.zeros_like(packed)))
    return parts[0] if len(parts) == 1 else jnp.concatenate(parts, axis=0)


def scatter_rows(value_refs, high_ref, low_ref, cameras, width):
    total = None
    ids = sub_iota(16, width).astype(F32).astype(BF16)
    for camera in range(cameras):
        pick = slice(camera, camera + 1)
        lanes = one_hot_rows(low_ref[pick, :], LANES, width)
        mask = jnp.broadcast_to(high_ref[pick, :], (16, width)).astype(BF16) == ids
        rows = []
        for ref, index in value_refs:
            spread = jnp.broadcast_to(ref[index, pick, :], (16, width)).astype(BF16)
            rows.append(jnp.where(mask, spread, jnp.zeros_like(spread)))
        piece = nt(jnp.concatenate(rows, axis=0), lanes)
        total = piece if total is None else total + piece
    return total


def fold_parts(total, index):
    start = 2 * PAD_ROWS * index
    return total[start : start + PAD_ROWS] + total[start + PAD_ROWS : start + 2 * PAD_ROWS]


def gather_rows(table, row_index, lane_index, rows):
    pieces = []
    for start in range(0, row_index.shape[1], LANES):
        row_part = row_index[:, start : start + LANES]
        lane_part = lane_index[:, start : start + LANES]
        out = None
        for row in range(rows):
            spread = jnp.broadcast_to(table[row : row + 1, :], lane_part.shape)
            got = jnp.take_along_axis(spread, lane_part, axis=1, mode="promise_in_bounds")
            out = got if out is None else jnp.where(row_part == row, got, out)
        pieces.append(out)
    return jnp.concatenate(pieces, axis=1)


def errors_of(cam_ref, vector, weights):
    rows = []
    for row in range(2):
        running = None
        for column in range(9):
            term = cam_ref[9 * row + column].astype(F32) * vector[:, column : column + 1]
            running = term if running is None else running + term
        rows.append(running * weights)
    return rows


def weights_of(count_ref, cameras, width):
    counts = jnp.zeros((cameras, width), I32)
    rows = sub_iota(cameras, width)
    for camera in range(cameras):
        counts = jnp.where(rows == camera, count_ref[camera], counts)
    return (lane_iota(cameras, width) < counts).astype(F32)


def send_rows(out_next, out_prev, index, block):
    out_next[SIDE * index : SIDE * (index + 1), :] = block[:SIDE]
    out_prev[SIDE * index : SIDE * (index + 1), :] = block[SIDE : 2 * SIDE]


def point_table(back, front):
    border = back.shape[1]
    eight = sub_iota(8, border)
    lanes = lane_iota(8, border)
    lefts, rights = [], []
    for listed, base in ((back, 0), (front, OWN_FRONT)):
        high = listed >> 7
        low = listed & 127
        hit = jnp.broadcast_to(high, (8, border)) == eight
        row_value = ((lanes >> 7) + (base + 1)).astype(F32)
        lane_value = (lanes & 127).astype(F32)
        zero = jnp.zeros((8, border), F32)
        lefts.append(
            jnp.concatenate(
                [jnp.where(hit, row_value, zero), jnp.where(hit, lane_value, zero)], axis=0
            ).astype(BF16)
        )
        rights.append(one_hot_rows(low.astype(F32), LANES, border))
    table = nt(lefts[0], rights[0]) + nt(lefts[1], rights[1])
    row_plus = table[:8]
    lane = table[8:]
    free = jnp.where(row_plus == 0.0, 1.0, 0.0)
    upper = jnp.where(sub_iota(LANES, LANES) <= lane_iota(LANES, LANES), 1.0, 0.0).astype(BF16)
    seen = lax.dot_general(
        free.astype(BF16), upper, (((1,), (0,)), ((), ())), preferred_element_type=F32
    )
    total = jnp.broadcast_to(seen[:, LANES - 1 : LANES], (8, LANES))
    before = jnp.zeros((8, LANES), F32)
    rows = sub_iota(8, LANES)
    for row in range(7):
        before = before + jnp.where(rows > row, row_of(total, row, 8), 0.0)
    rank = before + seen - free
    return jnp.where(
        free > 0.0, rank + float(INTERIOR * LANES), (row_plus - 1.0) * float(LANES) + lane
    ).astype(I32)


def first_kernel(
    cam_ref, point_ref, obs_ref, count_ref, back_ref, front_ref, damp_ref, guess_ref,
    next_ref, prev_ref, own_ref, index_ref, errors_ref, value_ref, high_ref, low_ref,
):
    cameras, width = obs_ref.shape
    border = back_ref.shape[1]
    points = damp_ref.shape[0] * damp_ref.shape[1]
    table = point_table(back_ref[...], front_ref[...])
    observed = obs_ref[...]
    own_place = gather_rows(table, observed >> 7, observed & 127, points // LANES)
    place = jnp.where(
        observed < points,
        own_place,
        jnp.where(
            observed < points + border,
            observed + (PREV_SLOTS * LANES - points),
            observed + (NEXT_SLOTS * LANES - points - border),
        ),
    )
    index_ref[...] = place
    high_ref[...] = (place >> 7).astype(F32)
    low_ref[...] = (place & 127).astype(F32)
    weights = weights_of(count_ref, cameras, width)
    jac = [point_ref[entry].astype(F32) * weights for entry in range(6)]
    errors = errors_of(cam_ref, columns(guess_ref[...]), weights)
    errors_ref[0] = errors[0]
    errors_ref[1] = errors[1]
    products = [jac[a] * jac[b] + jac[3 + a] * jac[3 + b] for a, b in ENTRY_PAIRS]
    products += [errors[0] * jac[j] + errors[1] * jac[3 + j] for j in range(3)]
    for number, product in enumerate(products):
        value_ref[2 * number], value_ref[2 * number + 1] = split_two(product)
    total = scatter_rows(
        [(value_ref, number) for number in range(18)], high_ref, low_ref, cameras, width
    )
    ids = sub_iota(16, LANES).astype(F32).astype(BF16)
    damping = None
    new_high = (table >> 7).astype(F32)
    new_low = (table & 127).astype(F32)
    first, rest = split_two(damp_ref[...])
    last = damp_ref[...] - first - rest
    for row in range(points // LANES):
        lanes = one_hot_rows(new_low[row : row + 1, :], LANES, LANES)
        mask = row_of(new_high, row, 16).astype(BF16) == ids
        parts = []
        for part in (first, rest, last):
            spread = row_of(part, row, 16).astype(BF16)
            parts.append(jnp.where(mask, spread, jnp.zeros_like(spread)))
        piece = nt(jnp.concatenate(parts, axis=0), lanes)
        damping = piece if damping is None else damping + piece
    damping = damping[:16] + damping[16:32] + damping[32:]
    for number in range(9):
        block = fold_parts(total, number)
        if number in (0, 3, 5):
            block = block + damping
        own_ref[number] = block
        send_rows(next_ref, prev_ref, number, block)


def complete(own_ref, next_ref, prev_ref, number, place):
    block = own_ref[number]
    after = next_ref[SIDE * place : SIDE * (place + 1), :]
    before = prev_ref[SIDE * place : SIDE * (place + 1), :]
    tail = jnp.zeros((PAD_ROWS - 2 * SIDE, LANES), F32)
    return block + jnp.concatenate([after, before, tail], axis=0)


def symmetric_inverse(entries):
    cofactors = [
        entries[3] * entries[5] - entries[4] * entries[4],
        entries[2] * entries[4] - entries[1] * entries[5],
        entries[1] * entries[4] - entries[2] * entries[3],
        entries[0] * entries[5] - entries[2] * entries[2],
        entries[1] * entries[2] - entries[0] * entries[4],
        entries[0] * entries[3] - entries[1] * entries[1],
    ]
    determinant = entries[0] * cofactors[0] + entries[1] * cofactors[1] + entries[2] * cofactors[2]
    determinant = jnp.where(determinant == 0.0, 1.0, determinant)
    return [member / determinant for member in cofactors]


def apply_inverse(inverse, sums):
    return [
        inverse[0] * sums[0] + inverse[1] * sums[1] + inverse[2] * sums[2],
        inverse[1] * sums[0] + inverse[3] * sums[1] + inverse[4] * sums[2],
        inverse[2] * sums[0] + inverse[4] * sums[1] + inverse[5] * sums[2],
    ]


def pack_columns(cols):
    lanes = lane_iota(16, LANES)
    out = jnp.zeros((16, LANES), F32)
    for number, col in enumerate(cols):
        out = jnp.where(lanes == number, col, out)
    return out


def project(cam_ref, jac, errors, inverse, sums, place):
    values = apply_inverse(inverse, sums)
    high = place >> 7
    low = place & 127
    picked = [gather_rows(value, high, low, ROWS) for value in values]
    adjusted = [
        errors[row]
        - (picked[0] * jac[3 * row] + picked[1] * jac[3 * row + 1] + picked[2] * jac[3 * row + 2])
        for row in range(2)
    ]
    cols = []
    for column in range(9):
        term = (
            cam_ref[column].astype(F32) * adjusted[0]
            + cam_ref[9 + column].astype(F32) * adjusted[1]
        )
        cols.append(jnp.sum(term, axis=1, keepdims=True))
    return pack_columns(cols)


def next_scatter(
    cam_ref, jac, vector, weights, place, value_ref, high_ref, low_ref,
    next_ref, prev_ref, own_ref, errors_ref,
):
    cameras, width = place.shape
    errors = errors_of(cam_ref, vector, weights)
    errors_ref[0] = errors[0]
    errors_ref[1] = errors[1]
    for j in range(3):
        product = errors[0] * jac[j] + errors[1] * jac[3 + j]
        value_ref[2 * j], value_ref[2 * j + 1] = split_two(product)
    high_ref[...] = (place >> 7).astype(F32)
    low_ref[...] = (place & 127).astype(F32)
    total = scatter_rows(
        [(value_ref, number) for number in range(6)], high_ref, low_ref, cameras, width
    )
    for number in range(3):
        block = fold_parts(total, number)
        own_ref[number] = block
        send_rows(next_ref, prev_ref, number, block)


def second_kernel(
    cam_ref, point_ref, count_ref, index_ref, errors_in, own_in, after_in, before_in,
    cam_damp_ref, right_ref, guess_ref,
    next_ref, prev_ref, own_ref, errors_ref, inverse_ref, state_ref,
    value_ref, high_ref, low_ref,
):
    cameras, width = index_ref.shape
    weights = weights_of(count_ref, cameras, width)
    jac = [point_ref[entry].astype(F32) * weights for entry in range(6)]
    blocks = [complete(own_in, after_in, before_in, number, number) for number in range(9)]
    inverse = symmetric_inverse(blocks[:6])
    for number in range(6):
        inverse_ref[number] = inverse[number]
    place = index_ref[...]
    image = project(cam_ref, jac, [errors_in[0], errors_in[1]], inverse, blocks[6:], place)
    guess = pack_nine(columns(guess_ref[...]))
    right = pack_nine(columns(right_ref[...]))
    damp = spread_damp(cam_damp_ref, cameras)
    cols = []
    for column in range(9):
        squared = cam_ref[column].astype(F32) ** 2 + cam_ref[9 + column].astype(F32) ** 2
        cols.append(jnp.sum(squared * weights, axis=1, keepdims=True))
    valid = lane_iota(16, LANES) < 9
    precond = jnp.where(valid, 1.0 / (pack_columns(cols) + damp), 0.0)
    residual = right - (damp * guess + image)
    scaled = precond * residual
    state_ref[0] = guess
    state_ref[1] = residual
    state_ref[2] = scaled
    state_ref[3] = precond
    state_ref[4] = damp
    next_scatter(
        cam_ref, jac, scaled, weights, place, value_ref, high_ref, low_ref,
        next_ref, prev_ref, own_ref, errors_ref,
    )


def pack_nine(cols):
    return pack_columns([cols[:, number : number + 1] for number in range(9)])


def spread_damp(cam_damp_ref, cameras):
    rows = sub_iota(16, LANES)
    out = jnp.zeros((16, LANES), F32)
    for camera in range(cameras):
        out = jnp.where(rows == camera, cam_damp_ref[camera], out)
    return out


def third_kernel(
    cam_ref, point_ref, count_ref, index_ref, errors_in, own_in, after_in, before_in,
    inverse_in, state_in,
    next_ref, prev_ref, own_ref, errors_ref, state_ref,
    value_ref, high_ref, low_ref,
):
    cameras, width = index_ref.shape
    weights = weights_of(count_ref, cameras, width)
    jac = [point_ref[entry].astype(F32) * weights for entry in range(6)]
    sums = [complete(own_in, after_in, before_in, number, number) for number in range(3)]
    inverse = [inverse_in[number] for number in range(6)]
    place = index_ref[...]
    image = project(cam_ref, jac, [errors_in[0], errors_in[1]], inverse, sums, place)
    image = state_in[4] * state_in[2] + image
    residual = state_in[1] - image
    scaled = state_in[3] * residual
    state_ref[0] = image
    state_ref[1] = residual
    state_ref[2] = scaled
    next_scatter(
        cam_ref, jac, scaled, weights, place, value_ref, high_ref, low_ref,
        next_ref, prev_ref, own_ref, errors_ref,
    )


def last_kernel(
    cam_ref, point_ref, count_ref, index_ref, errors_in, own_in, after_in, before_in,
    inverse_in, state_in, tilde_in,
    image_ref, dots_ref,
):
    cameras, width = index_ref.shape
    weights = weights_of(count_ref, cameras, width)
    jac = [point_ref[entry].astype(F32) * weights for entry in range(6)]
    sums = [complete(own_in, after_in, before_in, number, number) for number in range(3)]
    inverse = [inverse_in[number] for number in range(6)]
    image = project(
        cam_ref, jac, [errors_in[0], errors_in[1]], inverse, sums, index_ref[...]
    )
    image = state_in[4] * tilde_in[2] + image
    image_ref[...] = image
    residual, scaled, precond = state_in[1], state_in[2], state_in[3]
    first, tilde_residual, tilde = tilde_in[0], tilde_in[1], tilde_in[2]
    back = precond * first
    pairs = (
        (residual, scaled),
        (first, scaled),
        (tilde_residual, tilde),
        (first, tilde),
        (first, back),
        (image, tilde),
        (image, back),
        (first - image, back),
    )
    rows = sub_iota(8, LANES)
    out = jnp.zeros((8, LANES), F32)
    for number, (left, right) in enumerate(pairs):
        out = jnp.where(rows == number, jnp.sum(left * right), out)
    dots_ref[...] = out


def finish_kernel(dots_ref, state_in, tilde_in, image_in, step_ref, residual_ref):
    dots = [row_of(dots_ref[...], number, 16) for number in range(8)]
    inner, curve, tilde_inner, cross, back_inner, tilde_curve, mixed, back_curve = dots
    first_step = inner / curve
    shift = first_step - 1.0
    inner_next = tilde_inner - 2.0 * shift * cross + shift * shift * back_inner
    curve_next = tilde_curve - 2.0 * shift * mixed + shift * shift * back_curve
    ratio = inner_next / inner
    against = cross - shift * back_inner
    second_step = inner_next / (curve_next + 2.0 * ratio * against + ratio * ratio * curve)
    guess, residual, scaled, precond = (state_in[number] for number in range(4))
    first, tilde_residual, tilde = (tilde_in[number] for number in range(3))
    image = image_in[...]
    direction = tilde - shift * (precond * first) + ratio * scaled
    moved = image - shift * (first - image) + ratio * first
    step = guess + first_step * scaled + second_step * direction
    left = tilde_residual - shift * first - second_step * moved
    eye = (sub_iota(16, 16) == lane_iota(16, 16)).astype(F32)
    flip = functools.partial(
        lax.dot_general,
        dimension_numbers=(((0,), (0,)), ((), ())),
        precision=lax.Precision.HIGHEST,
        preferred_element_type=F32,
    )
    step_ref[...] = flip(step, eye)[:9]
    residual_ref[...] = flip(left, eye)[:9]


def vmem(count):
    return [pl.BlockSpec(memory_space=pltpu.VMEM) for _ in range(count)]


def smem():
    return pl.BlockSpec(memory_space=pltpu.SMEM)


def out_f32(*shape):
    return jax.ShapeDtypeStruct(shape, F32)


def shards(
    cam_jac, point_jac, obs_point, obs_count, back_list, front_list, point_damp, cam_damp,
    right_side, start_guess,
):
    cameras, width = obs_point.shape
    count = lax.axis_size("seg")
    forward = [(i, i + 1) for i in range(count - 1)]
    backward = [(i + 1, i) for i in range(count - 1)]

    def scratch(values):
        return [
            pltpu.VMEM((values, cameras, width), F32),
            pltpu.VMEM((cameras, width), F32),
            pltpu.VMEM((cameras, width), F32),
        ]

    def exchange(to_next, to_prev):
        before = lax.ppermute(to_next, "seg", forward)
        after = lax.ppermute(to_prev, "seg", backward)
        return after, before

    plane = out_f32(2, cameras, width)
    to_next, to_prev, own, place, errors = pl.pallas_call(
        first_kernel,
        out_shape=(
            out_f32(9 * SIDE, LANES),
            out_f32(9 * SIDE, LANES),
            out_f32(9, PAD_ROWS, LANES),
            jax.ShapeDtypeStruct((cameras, width), I32),
            plane,
        ),
        in_specs=vmem(3) + [smem()] + vmem(4),
        out_specs=tuple(vmem(5)),
        scratch_shapes=scratch(18),
        name="first",
    )(
        cam_jac, point_jac, obs_point, obs_count, back_list, front_list,
        point_damp.reshape(-1, LANES), start_guess,
    )
    after, before = exchange(to_next, to_prev)
    sent = (out_f32(3 * SIDE, LANES), out_f32(3 * SIDE, LANES), out_f32(3, PAD_ROWS, LANES), plane)
    to_next, to_prev, own, errors, inverse, state = pl.pallas_call(
        second_kernel,
        out_shape=sent + (out_f32(6, PAD_ROWS, LANES), out_f32(5, 16, LANES)),
        in_specs=vmem(2) + [smem()] + vmem(5) + [smem()] + vmem(2),
        out_specs=tuple(vmem(6)),
        scratch_shapes=scratch(6),
        name="second",
    )(
        cam_jac, point_jac, obs_count, place, errors, own, after, before, cam_damp,
        right_side, start_guess,
    )
    after, before = exchange(to_next, to_prev)
    to_next, to_prev, own, errors, tilde = pl.pallas_call(
        third_kernel,
        out_shape=sent + (out_f32(3, 16, LANES),),
        in_specs=vmem(2) + [smem()] + vmem(7),
        out_specs=tuple(vmem(5)),
        scratch_shapes=scratch(6),
        name="third",
    )(cam_jac, point_jac, obs_count, place, errors, own, after, before, inverse, state)
    after, before = exchange(to_next, to_prev)
    image, dots = pl.pallas_call(
        last_kernel,
        out_shape=(out_f32(16, LANES), out_f32(8, LANES)),
        in_specs=vmem(2) + [smem()] + vmem(8),
        out_specs=tuple(vmem(2)),
        name="last",
    )(cam_jac, point_jac, obs_count, place, errors, own, after, before, inverse, state, tilde)
    span = 1
    while span < count:
        dots = dots + lax.ppermute(dots, "seg", [(i, i ^ span) for i in range(count)])
        span *= 2
    return pl.pallas_call(
        finish_kernel,
        out_shape=(out_f32(9, 16), out_f32(9, 16)),
        in_specs=vmem(4),
        out_specs=tuple(vmem(2)),
        name="finish",
    )(dots, state, tilde, image)


def solution(mesh):
    return jax.shard_map(
        shards,
        mesh=mesh,
        in_specs=(
            P(None, "seg", None),
            P(None, "seg", None),
            P("seg", None),
            P("seg"),
            P("seg", None),
            P("seg", None),
            P("seg"),
            P("seg"),
            P(None, "seg"),
            P(None, "seg"),
        ),
        out_specs=(P(None, "seg"), P(None, "seg")),
        check_vma=False,
    )
```

```python
import functools

import jax
import jax.numpy as jnp
from jax import lax
from jax.experimental import pallas as pl
from jax.experimental.pallas import tpu as pltpu
from jax.sharding import PartitionSpec as P

F32 = jnp.float32
BF16 = jnp.bfloat16
I32 = jnp.int32
LANES = 128
ENTRY_PAIRS = ((0, 0), (0, 1), (0, 2), (1, 1), (1, 2), (2, 2))

SIDE = 6
LIST_ROWS = 3
NEXT_SLOTS = 3
PREV_SLOTS = 6
OWN_FRONT = 9
INTERIOR = 12
ROWS = 14
PAD_ROWS = 16


def row_of(block, index, rows):
    return jnp.broadcast_to(block[index : index + 1, :], (rows, block.shape[1]))


def sub_iota(rows, width):
    return lax.broadcasted_iota(I32, (rows, width), 0)


def lane_iota(rows, width):
    return lax.broadcasted_iota(I32, (rows, width), 1)


def nt(left, right, **kw):
    return lax.dot_general(
        left, right, (((1,), (1,)), ((), ())), preferred_element_type=F32, **kw
    )


def split_two(value):
    high = value.astype(BF16)
    low = (value - high.astype(F32)).astype(BF16)
    return high.astype(F32), low.astype(F32)


def columns(block):
    eye = (sub_iota(16, 16) == lane_iota(16, 16)).astype(F32)
    return nt(eye, block, precision=lax.Precision.HIGHEST)


def one_hot_rows(index_row, rows, width):
    packed = jnp.broadcast_to(index_row, (16, width)).astype(BF16)
    parts = []
    for start in range(0, rows, 16):
        ids = (sub_iota(16, width) + start).astype(F32).astype(BF16)
        parts.append(jnp.where(packed == ids, jnp.ones_like(packed), jnp.zeros_like(packed)))
    return parts[0] if len(parts) == 1 else jnp.concatenate(parts, axis=0)


def scatter_rows(value_refs, high_ref, low_ref, cameras, width):
    total = None
    ids = sub_iota(16, width).astype(F32).astype(BF16)
    for camera in range(cameras):
        pick = slice(camera, camera + 1)
        lanes = one_hot_rows(low_ref[pick, :], LANES, width)
        mask = jnp.broadcast_to(high_ref[pick, :], (16, width)).astype(BF16) == ids
        rows = []
        for ref, index in value_refs:
            spread = jnp.broadcast_to(ref[index, pick, :], (16, width)).astype(BF16)
            rows.append(jnp.where(mask, spread, jnp.zeros_like(spread)))
        piece = nt(jnp.concatenate(rows, axis=0), lanes)
        total = piece if total is None else total + piece
    return total


def fold_parts(total, index):
    start = 2 * PAD_ROWS * index
    return total[start : start + PAD_ROWS] + total[start + PAD_ROWS : start + 2 * PAD_ROWS]


def gather_rows(table, row_index, lane_index, rows):
    pieces = []
    for start in range(0, row_index.shape[1], LANES):
        row_part = row_index[:, start : start + LANES]
        lane_part = lane_index[:, start : start + LANES]
        out = None
        for row in range(rows):
            spread = jnp.broadcast_to(table[row : row + 1, :], lane_part.shape)
            got = jnp.take_along_axis(spread, lane_part, axis=1, mode="promise_in_bounds")
            out = got if out is None else jnp.where(row_part == row, got, out)
        pieces.append(out)
    return jnp.concatenate(pieces, axis=1)


def errors_of(cam_ref, vector, weights):
    rows = []
    for row in range(2):
        running = None
        for column in range(9):
            term = cam_ref[9 * row + column].astype(F32) * vector[:, column : column + 1]
            running = term if running is None else running + term
        rows.append(running * weights)
    return rows


def weights_of(count_ref, cameras, width):
    counts = jnp.zeros((cameras, width), I32)
    rows = sub_iota(cameras, width)
    for camera in range(cameras):
        counts = jnp.where(rows == camera, count_ref[camera], counts)
    return (lane_iota(cameras, width) < counts).astype(F32)


def send_rows(odd, mate_ref, other_ref, index, block):
    to_next = block[:SIDE]
    to_prev = block[SIDE : 2 * SIDE]
    mate_ref[SIDE * index : SIDE * (index + 1), :] = jnp.where(odd, to_prev, to_next)
    other_ref[SIDE * index : SIDE * (index + 1), :] = jnp.where(odd, to_next, to_prev)


def point_table(back, front):
    border = back.shape[1]
    eight = sub_iota(8, border)
    lanes = lane_iota(8, border)
    lefts, rights = [], []
    for listed, base in ((back, 0), (front, OWN_FRONT)):
        high = listed >> 7
        low = listed & 127
        hit = jnp.broadcast_to(high, (8, border)) == eight
        row_value = ((lanes >> 7) + (base + 1)).astype(F32)
        lane_value = (lanes & 127).astype(F32)
        zero = jnp.zeros((8, border), F32)
        lefts.append(
            jnp.concatenate(
                [jnp.where(hit, row_value, zero), jnp.where(hit, lane_value, zero)], axis=0
            ).astype(BF16)
        )
        rights.append(one_hot_rows(low.astype(F32), LANES, border))
    table = nt(lefts[0], rights[0]) + nt(lefts[1], rights[1])
    row_plus = table[:8]
    lane = table[8:]
    free = jnp.where(row_plus == 0.0, 1.0, 0.0)
    upper = jnp.where(sub_iota(LANES, LANES) <= lane_iota(LANES, LANES), 1.0, 0.0).astype(BF16)
    seen = lax.dot_general(
        free.astype(BF16), upper, (((1,), (0,)), ((), ())), preferred_element_type=F32
    )
    total = jnp.broadcast_to(seen[:, LANES - 1 : LANES], (8, LANES))
    before = jnp.zeros((8, LANES), F32)
    rows = sub_iota(8, LANES)
    for row in range(7):
        before = before + jnp.where(rows > row, row_of(total, row, 8), 0.0)
    rank = before + seen - free
    return jnp.where(
        free > 0.0, rank + float(INTERIOR * LANES), (row_plus - 1.0) * float(LANES) + lane
    ).astype(I32)


def first_kernel(
    cam_ref, point_ref, obs_ref, count_ref, back_ref, front_ref, damp_ref, guess_ref, odd_ref,
    mate_ref, other_ref, own_ref, index_ref, errors_ref, value_ref, high_ref, low_ref,
):
    odd = odd_ref[0] == 1
    cameras, width = obs_ref.shape
    border = back_ref.shape[1]
    points = damp_ref.shape[0] * damp_ref.shape[1]
    table = point_table(back_ref[...], front_ref[...])
    observed = obs_ref[...]
    own_place = gather_rows(table, observed >> 7, observed & 127, points // LANES)
    place = jnp.where(
        observed < points,
        own_place,
        jnp.where(
            observed < points + border,
            observed + (PREV_SLOTS * LANES - points),
            observed + (NEXT_SLOTS * LANES - points - border),
        ),
    )
    index_ref[...] = place
    high_ref[...] = (place >> 7).astype(F32)
    low_ref[...] = (place & 127).astype(F32)
    weights = weights_of(count_ref, cameras, width)
    jac = [point_ref[entry].astype(F32) * weights for entry in range(6)]
    errors = errors_of(cam_ref, columns(guess_ref[...]), weights)
    errors_ref[0] = errors[0]
    errors_ref[1] = errors[1]
    products = [jac[a] * jac[b] + jac[3 + a] * jac[3 + b] for a, b in ENTRY_PAIRS]
    products += [errors[0] * jac[j] + errors[1] * jac[3 + j] for j in range(3)]
    for number, product in enumerate(products):
        value_ref[2 * number], value_ref[2 * number + 1] = split_two(product)
    total = scatter_rows(
        [(value_ref, number) for number in range(18)], high_ref, low_ref, cameras, width
    )
    ids = sub_iota(16, LANES).astype(F32).astype(BF16)
    damping = None
    new_high = (table >> 7).astype(F32)
    new_low = (table & 127).astype(F32)
    first, rest = split_two(damp_ref[...])
    last = damp_ref[...] - first - rest
    for row in range(points // LANES):
        lanes = one_hot_rows(new_low[row : row + 1, :], LANES, LANES)
        mask = row_of(new_high, row, 16).astype(BF16) == ids
        parts = []
        for part in (first, rest, last):
            spread = row_of(part, row, 16).astype(BF16)
            parts.append(jnp.where(mask, spread, jnp.zeros_like(spread)))
        piece = nt(jnp.concatenate(parts, axis=0), lanes)
        damping = piece if damping is None else damping + piece
    damping = damping[:16] + damping[16:32] + damping[32:]
    for number in range(9):
        block = fold_parts(total, number)
        if number in (0, 3, 5):
            block = block + damping
        own_ref[number] = block
        send_rows(odd, mate_ref, other_ref, number, block)


def complete(odd, own_ref, mate_ref, other_ref, number):
    block = own_ref[number]
    mate = mate_ref[SIDE * number : SIDE * (number + 1), :]
    other = other_ref[SIDE * number : SIDE * (number + 1), :]
    after = jnp.where(odd, other, mate)
    before = jnp.where(odd, mate, other)
    tail = jnp.zeros((PAD_ROWS - 2 * SIDE, LANES), F32)
    return block + jnp.concatenate([after, before, tail], axis=0)


def symmetric_inverse(entries):
    cofactors = [
        entries[3] * entries[5] - entries[4] * entries[4],
        entries[2] * entries[4] - entries[1] * entries[5],
        entries[1] * entries[4] - entries[2] * entries[3],
        entries[0] * entries[5] - entries[2] * entries[2],
        entries[1] * entries[2] - entries[0] * entries[4],
        entries[0] * entries[3] - entries[1] * entries[1],
    ]
    determinant = entries[0] * cofactors[0] + entries[1] * cofactors[1] + entries[2] * cofactors[2]
    determinant = jnp.where(determinant == 0.0, 1.0, determinant)
    return [member / determinant for member in cofactors]


def apply_inverse(inverse, sums):
    return [
        inverse[0] * sums[0] + inverse[1] * sums[1] + inverse[2] * sums[2],
        inverse[1] * sums[0] + inverse[3] * sums[1] + inverse[4] * sums[2],
        inverse[2] * sums[0] + inverse[4] * sums[1] + inverse[5] * sums[2],
    ]


def pack_columns(cols):
    lanes = lane_iota(16, LANES)
    out = jnp.zeros((16, LANES), F32)
    for number, col in enumerate(cols):
        out = jnp.where(lanes == number, col, out)
    return out


def project(cam_ref, jac, errors, inverse, sums, place):
    values = apply_inverse(inverse, sums)
    high = place >> 7
    low = place & 127
    picked = [gather_rows(value, high, low, ROWS) for value in values]
    adjusted = [
        errors[row]
        - (picked[0] * jac[3 * row] + picked[1] * jac[3 * row + 1] + picked[2] * jac[3 * row + 2])
        for row in range(2)
    ]
    cols = []
    for column in range(9):
        term = (
            cam_ref[column].astype(F32) * adjusted[0]
            + cam_ref[9 + column].astype(F32) * adjusted[1]
        )
        cols.append(jnp.sum(term, axis=1, keepdims=True))
    return pack_columns(cols)


def next_scatter(
    odd, cam_ref, jac, vector, weights, place, value_ref, high_ref, low_ref,
    mate_ref, other_ref, own_ref, errors_ref,
):
    cameras, width = place.shape
    errors = errors_of(cam_ref, vector, weights)
    errors_ref[0] = errors[0]
    errors_ref[1] = errors[1]
    for j in range(3):
        product = errors[0] * jac[j] + errors[1] * jac[3 + j]
        value_ref[2 * j], value_ref[2 * j + 1] = split_two(product)
    high_ref[...] = (place >> 7).astype(F32)
    low_ref[...] = (place & 127).astype(F32)
    total = scatter_rows(
        [(value_ref, number) for number in range(6)], high_ref, low_ref, cameras, width
    )
    for number in range(3):
        block = fold_parts(total, number)
        own_ref[number] = block
        send_rows(odd, mate_ref, other_ref, number, block)


def second_kernel(
    cam_ref, point_ref, count_ref, index_ref, errors_in, own_in, mate_in, other_in, odd_ref,
    cam_damp_ref, right_ref, guess_ref,
    mate_ref, other_ref, own_ref, errors_ref, inverse_ref, state_ref,
    value_ref, high_ref, low_ref,
):
    cameras, width = index_ref.shape
    odd = odd_ref[0] == 1
    weights = weights_of(count_ref, cameras, width)
    jac = [point_ref[entry].astype(F32) * weights for entry in range(6)]
    blocks = [complete(odd, own_in, mate_in, other_in, number) for number in range(9)]
    inverse = symmetric_inverse(blocks[:6])
    for number in range(6):
        inverse_ref[number] = inverse[number]
    place = index_ref[...]
    image = project(cam_ref, jac, [errors_in[0], errors_in[1]], inverse, blocks[6:], place)
    guess = pack_nine(columns(guess_ref[...]))
    right = pack_nine(columns(right_ref[...]))
    damp = spread_damp(cam_damp_ref, cameras)
    cols = []
    for column in range(9):
        squared = cam_ref[column].astype(F32) ** 2 + cam_ref[9 + column].astype(F32) ** 2
        cols.append(jnp.sum(squared * weights, axis=1, keepdims=True))
    valid = lane_iota(16, LANES) < 9
    precond = jnp.where(valid, 1.0 / (pack_columns(cols) + damp), 0.0)
    residual = right - (damp * guess + image)
    scaled = precond * residual
    state_ref[0] = guess
    state_ref[1] = residual
    state_ref[2] = scaled
    state_ref[3] = precond
    state_ref[4] = damp
    next_scatter(
        odd, cam_ref, jac, scaled, weights, place, value_ref, high_ref, low_ref,
        mate_ref, other_ref, own_ref, errors_ref,
    )


def pack_nine(cols):
    return pack_columns([cols[:, number : number + 1] for number in range(9)])


def spread_damp(cam_damp_ref, cameras):
    rows = sub_iota(16, LANES)
    out = jnp.zeros((16, LANES), F32)
    for camera in range(cameras):
        out = jnp.where(rows == camera, cam_damp_ref[camera], out)
    return out


def third_kernel(
    cam_ref, point_ref, count_ref, index_ref, errors_in, own_in, mate_in, other_in, odd_ref,
    inverse_in, state_in,
    mate_ref, other_ref, own_ref, errors_ref, state_ref,
    value_ref, high_ref, low_ref,
):
    cameras, width = index_ref.shape
    odd = odd_ref[0] == 1
    weights = weights_of(count_ref, cameras, width)
    jac = [point_ref[entry].astype(F32) * weights for entry in range(6)]
    sums = [complete(odd, own_in, mate_in, other_in, number) for number in range(3)]
    inverse = [inverse_in[number] for number in range(6)]
    place = index_ref[...]
    image = project(cam_ref, jac, [errors_in[0], errors_in[1]], inverse, sums, place)
    image = state_in[4] * state_in[2] + image
    residual = state_in[1] - image
    scaled = state_in[3] * residual
    state_ref[0] = image
    state_ref[1] = residual
    state_ref[2] = scaled
    next_scatter(
        odd, cam_ref, jac, scaled, weights, place, value_ref, high_ref, low_ref,
        mate_ref, other_ref, own_ref, errors_ref,
    )


def last_kernel(
    cam_ref, point_ref, count_ref, index_ref, errors_in, own_in, mate_in, other_in, odd_ref,
    inverse_in, state_in, tilde_in,
    image_ref, dots_ref,
):
    cameras, width = index_ref.shape
    odd = odd_ref[0] == 1
    weights = weights_of(count_ref, cameras, width)
    jac = [point_ref[entry].astype(F32) * weights for entry in range(6)]
    sums = [complete(odd, own_in, mate_in, other_in, number) for number in range(3)]
    inverse = [inverse_in[number] for number in range(6)]
    image = project(
        cam_ref, jac, [errors_in[0], errors_in[1]], inverse, sums, index_ref[...]
    )
    image = state_in[4] * tilde_in[2] + image
    image_ref[...] = image
    residual, scaled, precond = state_in[1], state_in[2], state_in[3]
    first, tilde_residual, tilde = tilde_in[0], tilde_in[1], tilde_in[2]
    back = precond * first
    pairs = (
        (residual, scaled),
        (first, scaled),
        (tilde_residual, tilde),
        (first, tilde),
        (first, back),
        (image, tilde),
        (image, back),
        (first - image, back),
    )
    lanes = lane_iota(8, LANES)
    out = jnp.zeros((8, LANES), F32)
    for number, (left, right) in enumerate(pairs):
        out = jnp.where(lanes == number, jnp.sum(left * right), out)
    for start in range(0, dots_ref.shape[0], 8):
        dots_ref[start : start + 8, :] = out


def finish_kernel(dots_ref, state_in, tilde_in, image_in, step_ref, residual_ref):
    total = jnp.sum(dots_ref[...], axis=0, keepdims=True)
    dots = [total[:, number : number + 1] for number in range(8)]
    inner, curve, tilde_inner, cross, back_inner, tilde_curve, mixed, back_curve = dots
    first_step = inner / curve
    shift = first_step - 1.0
    inner_next = tilde_inner - 2.0 * shift * cross + shift * shift * back_inner
    curve_next = tilde_curve - 2.0 * shift * mixed + shift * shift * back_curve
    ratio = inner_next / inner
    against = cross - shift * back_inner
    second_step = inner_next / (curve_next + 2.0 * ratio * against + ratio * ratio * curve)
    guess, residual, scaled, precond = (state_in[number] for number in range(4))
    first, tilde_residual, tilde = (tilde_in[number] for number in range(3))
    image = image_in[...]
    direction = tilde - shift * (precond * first) + ratio * scaled
    moved = image - shift * (first - image) + ratio * first
    step = guess + first_step * scaled + second_step * direction
    left = tilde_residual - shift * first - second_step * moved
    eye = (sub_iota(16, 16) == lane_iota(16, 16)).astype(F32)
    flip = functools.partial(
        lax.dot_general,
        dimension_numbers=(((0,), (0,)), ((), ())),
        precision=lax.Precision.HIGHEST,
        preferred_element_type=F32,
    )
    step_ref[...] = flip(step, eye)[:9]
    residual_ref[...] = flip(left, eye)[:9]


def vmem(count):
    return [pl.BlockSpec(memory_space=pltpu.VMEM) for _ in range(count)]


def smem():
    return pl.BlockSpec(memory_space=pltpu.SMEM)


def out_f32(*shape):
    return jax.ShapeDtypeStruct(shape, F32)


def shards(
    cam_jac, point_jac, obs_point, obs_count, back_list, front_list, point_damp, cam_damp,
    right_side, start_guess,
):
    cameras, width = obs_point.shape
    count = lax.axis_size("seg")
    odd = (lax.axis_index("seg") % 2).astype(I32).reshape(1)
    mates = [(i, i ^ 1) for i in range(count)]
    others = []
    for i in range(1, count - 1, 2):
        others += [(i, i + 1), (i + 1, i)]
    params = pltpu.CompilerParams(vmem_limit_bytes=16 * 2**20)

    def scratch(values):
        return [
            pltpu.VMEM((values, cameras, width), F32),
            pltpu.VMEM((cameras, width), F32),
            pltpu.VMEM((cameras, width), F32),
        ]

    def exchange(to_mate, to_other):
        other = lax.ppermute(to_other, "seg", others)
        mate = lax.ppermute(to_mate, "seg", mates)
        return mate, other

    plane = out_f32(2, cameras, width)
    to_mate, to_other, own, place, errors = pl.pallas_call(
        first_kernel,
        out_shape=(
            out_f32(9 * SIDE, LANES),
            out_f32(9 * SIDE, LANES),
            out_f32(9, PAD_ROWS, LANES),
            jax.ShapeDtypeStruct((cameras, width), I32),
            plane,
        ),
        in_specs=vmem(3) + [smem()] + vmem(4) + [smem()],
        out_specs=tuple(vmem(5)),
        scratch_shapes=scratch(18),
        compiler_params=params,
        name="first",
    )(
        cam_jac, point_jac, obs_point, obs_count, back_list, front_list,
        point_damp.reshape(-1, LANES), start_guess, odd,
    )
    mate, other = exchange(to_mate, to_other)
    sent = (out_f32(3 * SIDE, LANES), out_f32(3 * SIDE, LANES), out_f32(3, PAD_ROWS, LANES), plane)
    to_mate, to_other, own, errors, inverse, state = pl.pallas_call(
        second_kernel,
        out_shape=sent + (out_f32(6, PAD_ROWS, LANES), out_f32(5, 16, LANES)),
        in_specs=vmem(2) + [smem()] + vmem(5) + [smem(), smem()] + vmem(2),
        out_specs=tuple(vmem(6)),
        scratch_shapes=scratch(6),
        compiler_params=params,
        name="second",
    )(
        cam_jac, point_jac, obs_count, place, errors, own, mate, other, odd, cam_damp,
        right_side, start_guess,
    )
    mate, other = exchange(to_mate, to_other)
    to_mate, to_other, own, errors, tilde = pl.pallas_call(
        third_kernel,
        out_shape=sent + (out_f32(3, 16, LANES),),
        in_specs=vmem(2) + [smem()] + vmem(5) + [smem()] + vmem(2),
        out_specs=tuple(vmem(5)),
        scratch_shapes=scratch(6),
        compiler_params=params,
        name="third",
    )(cam_jac, point_jac, obs_count, place, errors, own, mate, other, odd, inverse, state)
    mate, other = exchange(to_mate, to_other)
    image, dots = pl.pallas_call(
        last_kernel,
        out_shape=(out_f32(16, LANES), out_f32(count, LANES)),
        in_specs=vmem(2) + [smem()] + vmem(5) + [smem()] + vmem(3),
        out_specs=tuple(vmem(2)),
        compiler_params=params,
        name="last",
    )(cam_jac, point_jac, obs_count, place, errors, own, mate, other, odd, inverse, state, tilde)
    dots = lax.all_to_all(dots, "seg", 0, 0, tiled=True)
    return pl.pallas_call(
        finish_kernel,
        out_shape=(out_f32(9, 16), out_f32(9, 16)),
        in_specs=vmem(4),
        out_specs=tuple(vmem(2)),
        compiler_params=params,
        name="finish",
    )(dots, state, tilde, image)


def solution(mesh):
    return jax.shard_map(
        shards,
        mesh=mesh,
        in_specs=(
            P(None, "seg", None),
            P(None, "seg", None),
            P("seg", None),
            P("seg"),
            P("seg", None),
            P("seg", None),
            P("seg"),
            P("seg"),
            P(None, "seg"),
            P(None, "seg"),
        ),
        out_specs=(P(None, "seg"), P(None, "seg")),
        check_vma=False,
    )
```

```python
import jax
import jax.numpy as jnp
from jax import lax
from jax.experimental import pallas as pl
from jax.experimental.pallas import tpu as pltpu
from jax.sharding import Mesh
from jax.sharding import PartitionSpec as P

F32 = jnp.float32
BF16 = jnp.bfloat16
I32 = jnp.int32
LANES = 128
ENTRY_PAIRS = ((0, 0), (0, 1), (0, 2), (1, 1), (1, 2), (2, 2))

SIDE = 6
LIST_ROWS = 3
NEXT_SLOTS = 3
PREV_SLOTS = 6
OWN_FRONT = 9
INTERIOR = 12
ROWS = 14
PAD_ROWS = 16


def row_of(block, index, rows):
    return jnp.broadcast_to(block[index : index + 1, :], (rows, block.shape[1]))


def sub_iota(rows, width):
    return lax.broadcasted_iota(I32, (rows, width), 0)


def lane_iota(rows, width):
    return lax.broadcasted_iota(I32, (rows, width), 1)


def nt(left, right, **kw):
    return lax.dot_general(
        left, right, (((1,), (1,)), ((), ())), preferred_element_type=F32, **kw
    )


def split_two(value):
    high = value.astype(BF16)
    low = (value - high.astype(F32)).astype(BF16)
    return high.astype(F32), low.astype(F32)


def flip_block(block_ref):
    return jnp.transpose(block_ref[...])[:16]


def one_hot_rows(index_row, rows, width):
    packed = jnp.broadcast_to(index_row, (16, width)).astype(BF16)
    parts = []
    for start in range(0, rows, 16):
        ids = (sub_iota(16, width) + start).astype(F32).astype(BF16)
        parts.append(jnp.where(packed == ids, jnp.ones_like(packed), jnp.zeros_like(packed)))
    return parts[0] if len(parts) == 1 else jnp.concatenate(parts, axis=0)


def scatter_rows(value_refs, high_ref, low_ref, cameras, width):
    total = None
    ids = sub_iota(16, width).astype(F32).astype(BF16)
    for camera in range(cameras):
        pick = slice(camera, camera + 1)
        lanes = one_hot_rows(low_ref[pick, :], LANES, width)
        mask = jnp.broadcast_to(high_ref[pick, :], (16, width)).astype(BF16) == ids
        rows = []
        for ref, index in value_refs:
            spread = jnp.broadcast_to(ref[index, pick, :], (16, width)).astype(BF16)
            rows.append(jnp.where(mask, spread, jnp.zeros_like(spread)))
        piece = nt(jnp.concatenate(rows, axis=0), lanes)
        total = piece if total is None else total + piece
    return total


def fold_parts(total, index):
    start = 2 * PAD_ROWS * index
    return total[start : start + PAD_ROWS] + total[start + PAD_ROWS : start + 2 * PAD_ROWS]


def gather_rows(table, row_index, lane_index, rows):
    pieces = []
    for start in range(0, row_index.shape[1], LANES):
        row_part = row_index[:, start : start + LANES]
        lane_part = lane_index[:, start : start + LANES]
        out = None
        for row in range(rows):
            spread = jnp.broadcast_to(table[row : row + 1, :], lane_part.shape)
            got = jnp.take_along_axis(spread, lane_part, axis=1, mode="promise_in_bounds")
            out = got if out is None else jnp.where(row_part == row, got, out)
        pieces.append(out)
    return jnp.concatenate(pieces, axis=1)


def errors_of(cam_ref, vector, weights):
    rows = []
    for row in range(2):
        running = None
        for column in range(9):
            term = cam_ref[9 * row + column].astype(F32) * vector[:, column : column + 1]
            running = term if running is None else running + term
        rows.append(running * weights)
    return rows


def send_rows(mate_ref, other_ref, index, block):
    odd = lax.axis_index("core") == 1
    to_next = block[:SIDE]
    to_prev = block[SIDE : 2 * SIDE]
    mate_ref[SIDE * index : SIDE * (index + 1), :] = jnp.where(odd, to_prev, to_next)
    other_ref[SIDE * index : SIDE * (index + 1), :] = jnp.where(odd, to_next, to_prev)


def point_table(back, front):
    border = back.shape[1]
    eight = sub_iota(8, border)
    lanes = lane_iota(8, border)
    lefts, rights = [], []
    for listed, base in ((back, 0), (front, OWN_FRONT)):
        high = listed >> 7
        low = listed & 127
        hit = jnp.broadcast_to(high, (8, border)) == eight
        row_value = ((lanes >> 7) + (base + 1)).astype(F32)
        lane_value = (lanes & 127).astype(F32)
        zero = jnp.zeros((8, border), F32)
        lefts.append(
            jnp.concatenate(
                [jnp.where(hit, row_value, zero), jnp.where(hit, lane_value, zero)], axis=0
            ).astype(BF16)
        )
        rights.append(one_hot_rows(low.astype(F32), LANES, border))
    table = nt(lefts[0], rights[0]) + nt(lefts[1], rights[1])
    row_plus = table[:8]
    lane = table[8:]
    free = jnp.where(row_plus == 0.0, 1.0, 0.0)
    upper = jnp.where(sub_iota(LANES, LANES) <= lane_iota(LANES, LANES), 1.0, 0.0).astype(BF16)
    seen = lax.dot_general(
        free.astype(BF16), upper, (((1,), (0,)), ((), ())), preferred_element_type=F32
    )
    total = jnp.broadcast_to(seen[:, LANES - 1 : LANES], (8, LANES))
    before = jnp.zeros((8, LANES), F32)
    rows = sub_iota(8, LANES)
    for row in range(7):
        before = before + jnp.where(rows > row, row_of(total, row, 8), 0.0)
    rank = before + seen - free
    return jnp.where(
        free > 0.0, rank + float(INTERIOR * LANES), (row_plus - 1.0) * float(LANES) + lane
    ).astype(I32)


def first_kernel(
    cam_hbm, point_hbm, obs_hbm, count_hbm, back_hbm, front_hbm, damp_hbm, cam_damp_hbm,
    right_hbm, guess_hbm,
    mate_ref, other_ref, own_ref, index_ref, errors_ref, jac_ref, state_ref,
    value_ref, high_ref, low_ref,
    cam_ref, point_ref, obs_ref, count_ref, back_ref, front_ref, damp_ref, cam_damp_ref,
    right_ref, guess_ref, flip_ref, sems,
):
    sources = (
        back_hbm, front_hbm, obs_hbm, guess_hbm, right_hbm, cam_damp_hbm, count_hbm, point_hbm,
        cam_hbm, damp_hbm,
    )
    targets = (
        back_ref, front_ref, obs_ref, guess_ref, right_ref, cam_damp_ref, count_ref, point_ref,
        cam_ref, damp_ref,
    )
    copies = [
        pltpu.make_async_copy(source, target, sems.at[number])
        for number, (source, target) in enumerate(zip(sources, targets))
    ]
    for copy in copies:
        copy.start()
    cameras, width = obs_ref.shape
    border = back_ref.shape[1]
    points = damp_ref.shape[0] * damp_ref.shape[1]
    for copy in copies[:2]:
        copy.wait()
    table = point_table(back_ref[...], front_ref[...])
    for copy in copies[2:7]:
        copy.wait()
    observed = obs_ref[...]
    own_place = gather_rows(table, observed >> 7, observed & 127, points // LANES)
    place = jnp.where(
        observed < points,
        own_place,
        jnp.where(
            observed < points + border,
            observed + (PREV_SLOTS * LANES - points),
            observed + (NEXT_SLOTS * LANES - points - border),
        ),
    )
    index_ref[...] = place
    high_ref[...] = (place >> 7).astype(F32)
    low_ref[...] = (place & 127).astype(F32)
    valid = lane_iota(16, LANES) < 9
    flip_ref[0, :9, :16] = guess_ref[...]
    flip_ref[1, :9, :16] = right_ref[...]
    flip_ref[2, 0:1, :16] = cam_damp_ref[...]
    flip_ref[2, 1:2, :16] = count_ref[...].astype(F32)
    guess = jnp.where(valid, flip_block(flip_ref.at[0]), 0.0)
    right = jnp.where(valid, flip_block(flip_ref.at[1]), 0.0)
    sides = flip_block(flip_ref.at[2])
    damp = jnp.where(valid, sides[:, 0:1], 0.0)
    weights = (lane_iota(cameras, width).astype(F32) < sides[:, 1:2]).astype(F32)
    state_ref[0] = guess
    state_ref[1] = right
    state_ref[2] = damp
    copies[7].wait()
    jac = [point_ref[entry].astype(F32) * weights for entry in range(6)]
    for entry in range(6):
        jac_ref[entry] = jac[entry]
    jac_ref[6] = weights
    products = [jac[a] * jac[b] + jac[3 + a] * jac[3 + b] for a, b in ENTRY_PAIRS]
    copies[8].wait()
    copies[9].wait()
    errors = errors_of(cam_ref, guess, weights)
    errors_ref[0] = errors[0]
    errors_ref[1] = errors[1]
    products += [errors[0] * jac[j] + errors[1] * jac[3 + j] for j in range(3)]
    for number, product in enumerate(products):
        value_ref[2 * number], value_ref[2 * number + 1] = split_two(product)
    total = scatter_rows(
        [(value_ref, number) for number in range(18)], high_ref, low_ref, cameras, width
    )
    ids = sub_iota(16, LANES).astype(F32).astype(BF16)
    damping = None
    new_high = (table >> 7).astype(F32)
    new_low = (table & 127).astype(F32)
    first, rest = split_two(damp_ref[...])
    last = damp_ref[...] - first - rest
    for row in range(points // LANES):
        lanes = one_hot_rows(new_low[row : row + 1, :], LANES, LANES)
        mask = row_of(new_high, row, 16).astype(BF16) == ids
        parts = []
        for part in (first, rest, last):
            spread = row_of(part, row, 16).astype(BF16)
            parts.append(jnp.where(mask, spread, jnp.zeros_like(spread)))
        piece = nt(jnp.concatenate(parts, axis=0), lanes)
        damping = piece if damping is None else damping + piece
    damping = damping[:16] + damping[16:32] + damping[32:]
    for number in range(9):
        block = fold_parts(total, number)
        if number in (0, 3, 5):
            block = block + damping
        own_ref[number] = block
        send_rows(mate_ref, other_ref, number, block)


def complete(own_ref, mate_ref, other_ref, number):
    odd = lax.axis_index("core") == 1
    block = own_ref[number]
    mate = mate_ref[SIDE * number : SIDE * (number + 1), :]
    other = other_ref[SIDE * number : SIDE * (number + 1), :]
    after = jnp.where(odd, other, mate)
    before = jnp.where(odd, mate, other)
    tail = jnp.zeros((PAD_ROWS - 2 * SIDE, LANES), F32)
    return block + jnp.concatenate([after, before, tail], axis=0)


def symmetric_inverse(entries):
    cofactors = [
        entries[3] * entries[5] - entries[4] * entries[4],
        entries[2] * entries[4] - entries[1] * entries[5],
        entries[1] * entries[4] - entries[2] * entries[3],
        entries[0] * entries[5] - entries[2] * entries[2],
        entries[1] * entries[2] - entries[0] * entries[4],
        entries[0] * entries[3] - entries[1] * entries[1],
    ]
    determinant = entries[0] * cofactors[0] + entries[1] * cofactors[1] + entries[2] * cofactors[2]
    determinant = jnp.where(determinant == 0.0, 1.0, determinant)
    return [member / determinant for member in cofactors]


def apply_inverse(inverse, sums):
    return [
        inverse[0] * sums[0] + inverse[1] * sums[1] + inverse[2] * sums[2],
        inverse[1] * sums[0] + inverse[3] * sums[1] + inverse[4] * sums[2],
        inverse[2] * sums[0] + inverse[4] * sums[1] + inverse[5] * sums[2],
    ]


def pack_columns(cols):
    lanes = lane_iota(16, LANES)
    out = jnp.zeros((16, LANES), F32)
    for number, col in enumerate(cols):
        out = jnp.where(lanes == number, col, out)
    return out


def project(cam_ref, jac_ref, errors_ref, values, place):
    high = place >> 7
    low = place & 127
    picked = [gather_rows(value, high, low, ROWS) for value in values]
    adjusted = []
    for row in range(2):
        back = (
            picked[0] * jac_ref[3 * row]
            + picked[1] * jac_ref[3 * row + 1]
            + picked[2] * jac_ref[3 * row + 2]
        )
        adjusted.append(errors_ref[row] - back)
    cols = []
    for column in range(9):
        term = (
            cam_ref[column].astype(F32) * adjusted[0]
            + cam_ref[9 + column].astype(F32) * adjusted[1]
        )
        cols.append(jnp.sum(term, axis=1, keepdims=True))
    return pack_columns(cols)


def next_scatter(
    cam_ref, jac_ref, vector, place, value_ref, high_ref, low_ref,
    mate_ref, other_ref, own_ref, errors_ref,
):
    cameras, width = place.shape
    errors = errors_of(cam_ref, vector, jac_ref[6])
    errors_ref[0] = errors[0]
    errors_ref[1] = errors[1]
    for j in range(3):
        product = errors[0] * jac_ref[j] + errors[1] * jac_ref[3 + j]
        value_ref[2 * j], value_ref[2 * j + 1] = split_two(product)
    high_ref[...] = (place >> 7).astype(F32)
    low_ref[...] = (place & 127).astype(F32)
    total = scatter_rows(
        [(value_ref, number) for number in range(6)], high_ref, low_ref, cameras, width
    )
    blocks = []
    for number in range(3):
        block = fold_parts(total, number)
        own_ref[number] = block
        send_rows(mate_ref, other_ref, number, block)
        blocks.append(block)
    return errors, blocks


def second_kernel(
    cam_ref, jac_ref, index_ref, errors_in, own_in, mate_in, other_in, state_in,
    mate_ref, other_ref, own_ref, errors_ref, inverse_ref, state_ref,
    value_ref, high_ref, low_ref,
):
    blocks = [complete(own_in, mate_in, other_in, number) for number in range(9)]
    inverse = symmetric_inverse(blocks[:6])
    for number in range(6):
        inverse_ref[number] = inverse[number]
    place = index_ref[...]
    values = apply_inverse(inverse, blocks[6:])
    image = project(cam_ref, jac_ref, errors_in, values, place)
    guess, right, damp = state_in[0], state_in[1], state_in[2]
    cols = []
    for column in range(9):
        squared = cam_ref[column].astype(F32) ** 2 + cam_ref[9 + column].astype(F32) ** 2
        cols.append(jnp.sum(squared * jac_ref[6], axis=1, keepdims=True))
    valid = lane_iota(16, LANES) < 9
    precond = jnp.where(valid, 1.0 / (pack_columns(cols) + damp), 0.0)
    residual = right - (damp * guess + image)
    scaled = precond * residual
    state_ref[0] = residual
    state_ref[1] = scaled
    state_ref[2] = precond
    next_scatter(
        cam_ref, jac_ref, scaled, place, value_ref, high_ref, low_ref,
        mate_ref, other_ref, own_ref, errors_ref,
    )


def unshared_rows():
    chip = lax.axis_index("chip")
    core = lax.axis_index("core")
    first = jnp.logical_and(chip == 0, core == 0)
    last = jnp.logical_and(chip == lax.axis_size("chip") - 1, core == 1)
    start = jnp.where(first, SIDE, INTERIOR)
    stop = jnp.where(last, SIDE, 0)
    rows = sub_iota(PAD_ROWS, LANES)
    return jnp.logical_or(rows >= start, rows < stop)


def column_sums(block):
    return jnp.sum(block, axis=0, keepdims=True)


def third_kernel(
    cam_ref, jac_ref, index_ref, errors_in, own_in, mate_in, other_in, inverse_in, given, state_in,
    mate_ref, other_ref, own_ref, errors_ref, state_ref, rows_ref,
    value_ref, high_ref, low_ref,
):
    sums = [complete(own_in, mate_in, other_in, number) for number in range(3)]
    inverse = [inverse_in[number] for number in range(6)]
    values = apply_inverse(inverse, sums)
    image = project(cam_ref, jac_ref, errors_in, values, index_ref[...])
    damp = given[2]
    residual, scaled, precond = state_in[0], state_in[1], state_in[2]
    image = damp * scaled + image
    tilde_residual = residual - image
    tilde = precond * tilde_residual
    state_ref[0] = image
    state_ref[1] = tilde_residual
    state_ref[2] = tilde
    errors, blocks = next_scatter(
        cam_ref, jac_ref, tilde, index_ref[...], value_ref, high_ref, low_ref,
        mate_ref, other_ref, own_ref, errors_ref,
    )
    energy = column_sums(damp * tilde * tilde)
    squares = column_sums(errors[0] * errors[0] + errors[1] * errors[1])
    for start in range(0, squares.shape[1], LANES):
        energy = energy + squares[:, start : start + LANES]
    lone = unshared_rows()
    for value, point in zip(apply_inverse(inverse, blocks), blocks):
        energy = energy - column_sums(jnp.where(lone, value * point, 0.0))
    rows = [
        column_sums(residual * scaled),
        column_sums(image * scaled),
        column_sums(tilde_residual * tilde),
        column_sums(image * tilde),
        column_sums(image * (precond * image)),
        energy,
    ]
    for number, row in enumerate(rows):
        rows_ref[number : number + 1, :] = row
        mate_ref[3 * SIDE + number : 3 * SIDE + number + 1, :] = row


def sum_kernel(own_in, mate_in, other_in, inverse_in, rows_in, values_ref, dots_ref):
    sums = [complete(own_in, mate_in, other_in, number) for number in range(3)]
    inverse = [inverse_in[number] for number in range(6)]
    values = apply_inverse(inverse, sums)
    shared = None
    for number in range(3):
        values_ref[number] = values[number]
        term = values[number] * sums[number]
        shared = term if shared is None else shared + term
    border = column_sums(jnp.where(unshared_rows(), 0.0, shared))
    rows = rows_in[...] + mate_in[3 * SIDE : 3 * SIDE + 6, :]
    rows = rows - jnp.where(sub_iota(6, LANES) == 5, border, 0.0)
    totals = jnp.sum(rows, axis=1, keepdims=True)
    line = column_sums(jnp.where(sub_iota(6, LANES) == lane_iota(6, LANES), totals, 0.0))
    dots_ref[...] = jnp.broadcast_to(line, dots_ref.shape)


def finish_kernel(
    cam_ref, jac_ref, index_ref, errors_in, values_in, given, state_in, tilde_in, dots_ref,
    step_ref, residual_ref, flip_ref,
):
    values = [values_in[number] for number in range(3)]
    image = project(cam_ref, jac_ref, errors_in, values, index_ref[...])
    guess, damp = given[0], given[2]
    scaled, precond = state_in[1], state_in[2]
    first, tilde_residual, tilde = (tilde_in[number] for number in range(3))
    image = damp * tilde + image
    total = column_sums(dots_ref[...])
    inner, curve, tilde_inner, cross, back_inner, tilde_curve = (
        total[:, number : number + 1] for number in range(6)
    )
    mixed = cross - tilde_curve
    back_curve = back_inner - mixed
    first_step = inner / curve
    shift = first_step - 1.0
    inner_next = tilde_inner - 2.0 * shift * cross + shift * shift * back_inner
    curve_next = tilde_curve - 2.0 * shift * mixed + shift * shift * back_curve
    ratio = inner_next / inner
    against = cross - shift * back_inner
    second_step = inner_next / (curve_next + 2.0 * ratio * against + ratio * ratio * curve)
    direction = tilde - shift * (precond * first) + ratio * scaled
    moved = image - shift * (first - image) + ratio * first
    flip_ref[0, :16, :] = guess + first_step * scaled + second_step * direction
    flip_ref[1, :16, :] = tilde_residual - shift * first - second_step * moved
    step_ref[...] = jnp.transpose(flip_ref[0])[:9, :16]
    residual_ref[...] = jnp.transpose(flip_ref[1])[:9, :16]


def vmem(count):
    return [pl.BlockSpec(memory_space=pltpu.VMEM) for _ in range(count)]


def out_f32(*shape):
    return jax.ShapeDtypeStruct(shape, F32)


SEG = ("chip", "core")


def shards(
    cam_jac, point_jac, obs_point, obs_count, back_list, front_list, point_damp, cam_damp,
    right_side, start_guess,
):
    cameras, width = obs_point.shape
    chips = lax.axis_size("chip")
    count = 2 * chips
    mates = [(i, i ^ 1) for i in range(count)]
    others = []
    for i in range(1, count - 1, 2):
        others += [(i, i + 1), (i + 1, i)]
    params = pltpu.CompilerParams(vmem_limit_bytes=16 * 2**20)
    inputs = (
        cam_jac, point_jac, obs_point, obs_count.reshape(1, -1), back_list, front_list,
        point_damp.reshape(-1, LANES), cam_damp.reshape(1, -1), right_side, start_guess,
    )

    def scratch(values):
        return [
            pltpu.VMEM((values, cameras, width), F32),
            pltpu.VMEM((cameras, width), F32),
            pltpu.VMEM((cameras, width), F32),
        ]

    def exchange(to_mate, to_other):
        other = lax.ppermute(to_other, SEG, others)
        mate = lax.ppermute(to_mate, SEG, mates)
        return mate, other

    def call(kernel, name, outs, operands, scratches=(), spaces=None):
        return pl.pallas_call(
            kernel,
            out_shape=outs,
            in_specs=spaces or vmem(len(operands)),
            out_specs=tuple(vmem(len(outs))),
            scratch_shapes=list(scratches),
            compiler_params=params,
            name=name,
        )(*operands)

    plane = out_f32(2, cameras, width)
    to_mate, to_other, own, place, errors, jac, given = call(
        first_kernel,
        "first",
        (
            out_f32(9 * SIDE, LANES),
            out_f32(9 * SIDE, LANES),
            out_f32(9, PAD_ROWS, LANES),
            jax.ShapeDtypeStruct((cameras, width), I32),
            plane,
            out_f32(7, cameras, width),
            out_f32(3, 16, LANES),
        ),
        tuple(pltpu.with_memory_space_constraint(value, pltpu.HBM) for value in inputs),
        scratch(18)
        + [pltpu.VMEM(value.shape, value.dtype) for value in inputs]
        + [pltpu.VMEM((3, LANES, LANES), F32), pltpu.SemaphoreType.DMA((len(inputs),))],
        [pl.BlockSpec(memory_space=pltpu.HBM) for _ in inputs],
    )
    mate, other = exchange(to_mate, to_other)
    own_shape = out_f32(3, PAD_ROWS, LANES)
    to_mate, to_other, own, errors, inverse, state = call(
        second_kernel,
        "second",
        (
            out_f32(3 * SIDE, LANES),
            out_f32(3 * SIDE, LANES),
            own_shape,
            plane,
            out_f32(6, PAD_ROWS, LANES),
            out_f32(3, 16, LANES),
        ),
        (cam_jac, jac, place, errors, own, mate, other, given),
        scratch(6),
    )
    mate, other = exchange(to_mate, to_other)
    to_mate, to_other, own, errors, tilde, rows = call(
        third_kernel,
        "third",
        (
            out_f32(3 * SIDE + 6, LANES),
            out_f32(3 * SIDE, LANES),
            own_shape,
            plane,
            out_f32(3, 16, LANES),
            out_f32(6, LANES),
        ),
        (cam_jac, jac, place, errors, own, mate, other, inverse, given, state),
        scratch(6),
    )
    mate, other = exchange(to_mate, to_other)
    values, dots = call(
        sum_kernel,
        "sum",
        (own_shape, out_f32(chips, LANES)),
        (own, mate, other, inverse, rows),
    )
    dots = lax.all_to_all(dots, "chip", 0, 0, tiled=True)
    return call(
        finish_kernel,
        "finish",
        (out_f32(9, 16), out_f32(9, 16)),
        (cam_jac, jac, place, errors, values, given, state, tilde, dots),
        [pltpu.VMEM((2, LANES, LANES), F32)],
    )


def solution(mesh):
    finer = Mesh(mesh.devices.reshape(-1, 2), SEG)
    return jax.shard_map(
        shards,
        mesh=finer,
        in_specs=(
            P(None, SEG, None),
            P(None, SEG, None),
            P(SEG, None),
            P(SEG),
            P(SEG, None),
            P(SEG, None),
            P(SEG),
            P(SEG),
            P(None, SEG),
            P(None, SEG),
        ),
        out_specs=(P(None, SEG), P(None, SEG)),
        check_vma=False,
    )
```

```python
import jax
import jax.numpy as jnp
from jax import lax
from jax.experimental import pallas as pl
from jax.experimental.pallas import tpu as pltpu
from jax.sharding import Mesh
from jax.sharding import PartitionSpec as P

F32 = jnp.float32
BF16 = jnp.bfloat16
I32 = jnp.int32
LANES = 128
ENTRY_PAIRS = ((0, 0), (0, 1), (0, 2), (1, 1), (1, 2), (2, 2))

SIDE = 6
LIST_ROWS = 3
NEXT_SLOTS = 3
PREV_SLOTS = 6
OWN_FRONT = 9
INTERIOR = 12
ROWS = 14
PAD_ROWS = 16


def row_of(block, index, rows):
    return jnp.broadcast_to(block[index : index + 1, :], (rows, block.shape[1]))


def sub_iota(rows, width):
    return lax.broadcasted_iota(I32, (rows, width), 0)


def lane_iota(rows, width):
    return lax.broadcasted_iota(I32, (rows, width), 1)


def nt(left, right, **kw):
    return lax.dot_general(
        left, right, (((1,), (1,)), ((), ())), preferred_element_type=F32, **kw
    )


def split_two(value):
    high = value.astype(BF16)
    low = (value - high.astype(F32)).astype(BF16)
    return high.astype(F32), low.astype(F32)


def flip_block(block_ref):
    return jnp.transpose(block_ref[...])[:16]


def one_hot_rows(index_row, rows, width):
    packed = jnp.broadcast_to(index_row, (16, width)).astype(BF16)
    parts = []
    for start in range(0, rows, 16):
        ids = (sub_iota(16, width) + start).astype(F32).astype(BF16)
        parts.append(jnp.where(packed == ids, jnp.ones_like(packed), jnp.zeros_like(packed)))
    return parts[0] if len(parts) == 1 else jnp.concatenate(parts, axis=0)


def scatter_rows(value_refs, high_ref, low_ref, cameras, width):
    total = None
    ids = sub_iota(16, width).astype(F32).astype(BF16)
    for camera in range(cameras):
        pick = slice(camera, camera + 1)
        lanes = one_hot_rows(low_ref[pick, :], LANES, width).astype(jnp.float8_e4m3fn)
        mask = jnp.broadcast_to(high_ref[pick, :], (16, width)).astype(BF16) == ids
        rows = []
        for ref, index in value_refs:
            spread = jnp.broadcast_to(ref[index, pick, :], (16, width)).astype(BF16)
            rows.append(jnp.where(mask, spread, jnp.zeros_like(spread)))
        piece = nt(jnp.concatenate(rows, axis=0), lanes)
        total = piece if total is None else total + piece
    return total


def fold_parts(total, index):
    start = 2 * PAD_ROWS * index
    return total[start : start + PAD_ROWS] + total[start + PAD_ROWS : start + 2 * PAD_ROWS]


def gather_rows(tables, row_index, lane_index, rows):
    halves = []
    for top in range(0, row_index.shape[0], 8):
        pieces = []
        for start in range(0, row_index.shape[1], LANES):
            row_part = row_index[top : top + 8, start : start + LANES]
            lane_part = lane_index[top : top + 8, start : start + LANES]
            outs = [None] * len(tables)
            for row in range(rows):
                here = row_part == row
                for number, table in enumerate(tables):
                    spread = jnp.broadcast_to(table[row : row + 1, :], (8, LANES))
                    got = jnp.take_along_axis(spread, lane_part, axis=1, mode="promise_in_bounds")
                    outs[number] = got if row == 0 else jnp.where(here, got, outs[number])
            pieces.append(outs)
        halves.append([jnp.concatenate([p[n] for p in pieces], axis=1) for n in range(len(tables))])
    return [jnp.concatenate([h[n] for h in halves], axis=0) for n in range(len(tables))]


def errors_of(cam_ref, vector, weights):
    rows = []
    for row in range(2):
        running = None
        for column in range(9):
            term = cam_ref[9 * row + column].astype(F32) * vector[:, column : column + 1]
            running = term if running is None else running + term
        rows.append(running * weights)
    return rows


def send_rows(mate_ref, other_ref, index, block):
    odd = lax.axis_index("core") == 1
    to_next = block[:SIDE]
    to_prev = block[SIDE : 2 * SIDE]
    mate_ref[SIDE * index : SIDE * (index + 1), :] = jnp.where(odd, to_prev, to_next)
    other_ref[SIDE * index : SIDE * (index + 1), :] = jnp.where(odd, to_next, to_prev)


def point_table(back, front):
    border = back.shape[1]
    eight = sub_iota(8, border)
    lanes = lane_iota(8, border)
    lefts, rights = [], []
    for listed, base in ((back, 0), (front, OWN_FRONT)):
        high = listed >> 7
        low = listed & 127
        hit = jnp.broadcast_to(high, (8, border)) == eight
        row_value = ((lanes >> 7) + (base + 1)).astype(F32)
        lane_value = (lanes & 127).astype(F32)
        zero = jnp.zeros((8, border), F32)
        lefts.append(
            jnp.concatenate(
                [jnp.where(hit, row_value, zero), jnp.where(hit, lane_value, zero)], axis=0
            ).astype(BF16)
        )
        rights.append(one_hot_rows(low.astype(F32), LANES, border))
    table = nt(lefts[0], rights[0]) + nt(lefts[1], rights[1])
    row_plus = table[:8]
    lane = table[8:]
    free = jnp.where(row_plus == 0.0, 1.0, 0.0)
    upper = jnp.where(sub_iota(LANES, LANES) <= lane_iota(LANES, LANES), 1.0, 0.0).astype(BF16)
    seen = lax.dot_general(
        free.astype(BF16), upper, (((1,), (0,)), ((), ())), preferred_element_type=F32
    )
    total = jnp.broadcast_to(seen[:, LANES - 1 : LANES], (8, LANES))
    before = jnp.zeros((8, LANES), F32)
    rows = sub_iota(8, LANES)
    for row in range(7):
        before = before + jnp.where(rows > row, row_of(total, row, 8), 0.0)
    rank = before + seen - free
    return jnp.where(
        free > 0.0, rank + float(INTERIOR * LANES), (row_plus - 1.0) * float(LANES) + lane
    ).astype(I32)


def first_kernel(
    cam_hbm, point_hbm, obs_hbm, count_hbm, back_hbm, front_hbm, damp_hbm, cam_damp_hbm,
    right_hbm, guess_hbm,
    mate_ref, other_ref, own_ref, index_ref, errors_ref, jac_ref, state_ref,
    value_ref, high_ref, low_ref,
    cam_ref, point_ref, obs_ref, count_ref, back_ref, front_ref, damp_ref, cam_damp_ref,
    right_ref, guess_ref, flip_ref, sems,
):
    sources = (
        back_hbm, front_hbm, obs_hbm, guess_hbm, right_hbm, cam_damp_hbm, count_hbm, point_hbm,
        cam_hbm, damp_hbm,
    )
    targets = (
        back_ref, front_ref, obs_ref, guess_ref, right_ref, cam_damp_ref, count_ref, point_ref,
        cam_ref, damp_ref,
    )
    copies = [
        pltpu.make_async_copy(source, target, sems.at[number])
        for number, (source, target) in enumerate(zip(sources, targets))
    ]
    for copy in copies:
        copy.start()
    cameras, width = obs_ref.shape
    border = back_ref.shape[1]
    points = damp_ref.shape[0] * damp_ref.shape[1]
    for copy in copies:
        copy.wait()
    table = point_table(back_ref[...], front_ref[...])
    observed = obs_ref[...]
    own_place = gather_rows([table], observed >> 7, observed & 127, points // LANES)[0]
    place = jnp.where(
        observed < points,
        own_place,
        jnp.where(
            observed < points + border,
            observed + (PREV_SLOTS * LANES - points),
            observed + (NEXT_SLOTS * LANES - points - border),
        ),
    )
    index_ref[...] = place
    high_ref[...] = (place >> 7).astype(F32)
    low_ref[...] = (place & 127).astype(F32)
    valid = lane_iota(16, LANES) < 9
    flip_ref[0, :9, :16] = guess_ref[...]
    flip_ref[1, :9, :16] = right_ref[...]
    flip_ref[2, 0:1, :16] = cam_damp_ref[...]
    flip_ref[2, 1:2, :16] = count_ref[...].astype(F32)
    guess = jnp.where(valid, flip_block(flip_ref.at[0]), 0.0)
    right = jnp.where(valid, flip_block(flip_ref.at[1]), 0.0)
    sides = flip_block(flip_ref.at[2])
    damp = jnp.where(valid, sides[:, 0:1], 0.0)
    weights = (lane_iota(cameras, width).astype(F32) < sides[:, 1:2]).astype(F32)
    state_ref[0] = guess
    state_ref[1] = right
    state_ref[2] = damp
    jac = [point_ref[entry].astype(F32) * weights for entry in range(6)]
    for entry in range(6):
        jac_ref[entry] = jac[entry]
    jac_ref[6] = weights
    products = [jac[a] * jac[b] + jac[3 + a] * jac[3 + b] for a, b in ENTRY_PAIRS]
    errors = errors_of(cam_ref, guess, weights)
    errors_ref[0] = errors[0]
    errors_ref[1] = errors[1]
    products += [errors[0] * jac[j] + errors[1] * jac[3 + j] for j in range(3)]
    for number, product in enumerate(products):
        value_ref[2 * number], value_ref[2 * number + 1] = split_two(product)
    total = scatter_rows(
        [(value_ref, number) for number in range(18)], high_ref, low_ref, cameras, width
    )
    ids = sub_iota(16, LANES).astype(F32).astype(BF16)
    damping = None
    new_high = (table >> 7).astype(F32)
    new_low = (table & 127).astype(F32)
    first, rest = split_two(damp_ref[...])
    last = damp_ref[...] - first - rest
    for row in range(points // LANES):
        lanes = one_hot_rows(new_low[row : row + 1, :], LANES, LANES)
        mask = row_of(new_high, row, 16).astype(BF16) == ids
        parts = []
        for part in (first, rest, last):
            spread = row_of(part, row, 16).astype(BF16)
            parts.append(jnp.where(mask, spread, jnp.zeros_like(spread)))
        piece = nt(jnp.concatenate(parts, axis=0), lanes)
        damping = piece if damping is None else damping + piece
    damping = damping[:16] + damping[16:32] + damping[32:]
    for number in range(9):
        block = fold_parts(total, number)
        if number in (0, 3, 5):
            block = block + damping
        own_ref[number] = block
        send_rows(mate_ref, other_ref, number, block)


def complete(own_ref, mate_ref, other_ref, number):
    odd = lax.axis_index("core") == 1
    block = own_ref[number]
    mate = mate_ref[SIDE * number : SIDE * (number + 1), :]
    other = other_ref[SIDE * number : SIDE * (number + 1), :]
    after = jnp.where(odd, other, mate)
    before = jnp.where(odd, mate, other)
    tail = jnp.zeros((PAD_ROWS - 2 * SIDE, LANES), F32)
    return block + jnp.concatenate([after, before, tail], axis=0)


def symmetric_inverse(entries):
    cofactors = [
        entries[3] * entries[5] - entries[4] * entries[4],
        entries[2] * entries[4] - entries[1] * entries[5],
        entries[1] * entries[4] - entries[2] * entries[3],
        entries[0] * entries[5] - entries[2] * entries[2],
        entries[1] * entries[2] - entries[0] * entries[4],
        entries[0] * entries[3] - entries[1] * entries[1],
    ]
    determinant = entries[0] * cofactors[0] + entries[1] * cofactors[1] + entries[2] * cofactors[2]
    determinant = jnp.where(determinant == 0.0, 1.0, determinant)
    return [member / determinant for member in cofactors]


def apply_inverse(inverse, sums):
    return [
        inverse[0] * sums[0] + inverse[1] * sums[1] + inverse[2] * sums[2],
        inverse[1] * sums[0] + inverse[3] * sums[1] + inverse[4] * sums[2],
        inverse[2] * sums[0] + inverse[4] * sums[1] + inverse[5] * sums[2],
    ]


def pack_columns(cols):
    lanes = lane_iota(16, LANES)
    out = jnp.zeros((16, LANES), F32)
    for number, col in enumerate(cols):
        out = jnp.where(lanes == number, col, out)
    return out


def project(cam_ref, jac_ref, errors_ref, values, place):
    high = place >> 7
    low = place & 127
    picked = gather_rows(values, high, low, ROWS)
    adjusted = []
    for row in range(2):
        back = (
            picked[0] * jac_ref[3 * row]
            + picked[1] * jac_ref[3 * row + 1]
            + picked[2] * jac_ref[3 * row + 2]
        )
        adjusted.append(errors_ref[row] - back)
    cols = []
    for column in range(9):
        term = (
            cam_ref[column].astype(F32) * adjusted[0]
            + cam_ref[9 + column].astype(F32) * adjusted[1]
        )
        cols.append(jnp.sum(term, axis=1, keepdims=True))
    return pack_columns(cols)


def next_scatter(
    cam_ref, jac_ref, vector, place, value_ref, high_ref, low_ref,
    mate_ref, other_ref, own_ref, errors_ref,
):
    cameras, width = place.shape
    errors = errors_of(cam_ref, vector, jac_ref[6])
    errors_ref[0] = errors[0]
    errors_ref[1] = errors[1]
    for j in range(3):
        product = errors[0] * jac_ref[j] + errors[1] * jac_ref[3 + j]
        value_ref[2 * j], value_ref[2 * j + 1] = split_two(product)
    high_ref[...] = (place >> 7).astype(F32)
    low_ref[...] = (place & 127).astype(F32)
    total = scatter_rows(
        [(value_ref, number) for number in range(6)], high_ref, low_ref, cameras, width
    )
    blocks = []
    for number in range(3):
        block = fold_parts(total, number)
        own_ref[number] = block
        send_rows(mate_ref, other_ref, number, block)
        blocks.append(block)
    return errors, blocks


def side_kernel(cam_ref, jac_ref, given, precond_ref):
    cols = []
    for column in range(9):
        squared = cam_ref[column].astype(F32) ** 2 + cam_ref[9 + column].astype(F32) ** 2
        cols.append(jnp.sum(squared * jac_ref[6], axis=1, keepdims=True))
    valid = lane_iota(16, LANES) < 9
    precond_ref[...] = jnp.where(valid, 1.0 / (pack_columns(cols) + given[2]), 0.0)


def second_kernel(
    cam_ref, jac_ref, index_ref, errors_in, own_in, mate_in, other_in, state_in, precond_in,
    mate_ref, other_ref, own_ref, errors_ref, inverse_ref, state_ref,
    value_ref, high_ref, low_ref,
):
    blocks = [complete(own_in, mate_in, other_in, number) for number in range(9)]
    inverse = symmetric_inverse(blocks[:6])
    for number in range(6):
        inverse_ref[number] = inverse[number]
    place = index_ref[...]
    values = apply_inverse(inverse, blocks[6:])
    image = project(cam_ref, jac_ref, errors_in, values, place)
    guess, right, damp = state_in[0], state_in[1], state_in[2]
    precond = precond_in[...]
    residual = right - (damp * guess + image)
    scaled = precond * residual
    state_ref[0] = residual
    state_ref[1] = scaled
    state_ref[2] = precond
    next_scatter(
        cam_ref, jac_ref, scaled, place, value_ref, high_ref, low_ref,
        mate_ref, other_ref, own_ref, errors_ref,
    )


def unshared_rows():
    chip = lax.axis_index("chip")
    core = lax.axis_index("core")
    first = jnp.logical_and(chip == 0, core == 0)
    last = jnp.logical_and(chip == lax.axis_size("chip") - 1, core == 1)
    start = jnp.where(first, SIDE, INTERIOR)
    stop = jnp.where(last, SIDE, 0)
    rows = sub_iota(PAD_ROWS, LANES)
    return jnp.logical_or(rows >= start, rows < stop)


def column_sums(block):
    return jnp.sum(block, axis=0, keepdims=True)


def third_kernel(
    cam_ref, jac_ref, index_ref, errors_in, own_in, mate_in, other_in, inverse_in, given, state_in,
    mate_ref, other_ref, own_ref, errors_ref, state_ref, rows_ref,
    value_ref, high_ref, low_ref,
):
    sums = [complete(own_in, mate_in, other_in, number) for number in range(3)]
    inverse = [inverse_in[number] for number in range(6)]
    values = apply_inverse(inverse, sums)
    place = index_ref[...]
    image = project(cam_ref, jac_ref, errors_in, values, place)
    damp = given[2]
    residual, scaled, precond = state_in[0], state_in[1], state_in[2]
    image = damp * scaled + image
    tilde_residual = residual - image
    tilde = precond * tilde_residual
    state_ref[0] = image
    state_ref[1] = tilde_residual
    state_ref[2] = tilde
    errors, blocks = next_scatter(
        cam_ref, jac_ref, tilde, place, value_ref, high_ref, low_ref,
        mate_ref, other_ref, own_ref, errors_ref,
    )
    energy = column_sums(damp * tilde * tilde)
    squares = column_sums(errors[0] * errors[0] + errors[1] * errors[1])
    for start in range(0, squares.shape[1], LANES):
        energy = energy + squares[:, start : start + LANES]
    lone = unshared_rows()
    for value, point in zip(apply_inverse(inverse, blocks), blocks):
        energy = energy - column_sums(jnp.where(lone, value * point, 0.0))
    rows = [
        column_sums(residual * scaled),
        column_sums(image * scaled),
        column_sums(tilde_residual * tilde),
        column_sums(image * tilde),
        column_sums(image * (precond * image)),
        energy,
    ]
    for number, row in enumerate(rows):
        rows_ref[number : number + 1, :] = row
        mate_ref[3 * SIDE + number : 3 * SIDE + number + 1, :] = row


def sum_kernel(own_in, mate_in, other_in, inverse_in, rows_in, values_ref, dots_ref):
    sums = [complete(own_in, mate_in, other_in, number) for number in range(3)]
    inverse = [inverse_in[number] for number in range(6)]
    values = apply_inverse(inverse, sums)
    shared = None
    for number in range(3):
        values_ref[number] = values[number]
        term = values[number] * sums[number]
        shared = term if shared is None else shared + term
    border = column_sums(jnp.where(unshared_rows(), 0.0, shared))
    rows = rows_in[...] + mate_in[3 * SIDE : 3 * SIDE + 6, :]
    rows = rows - jnp.where(sub_iota(6, LANES) == 5, border, 0.0)
    totals = jnp.sum(rows, axis=1, keepdims=True)
    line = column_sums(jnp.where(sub_iota(6, LANES) == lane_iota(6, LANES), totals, 0.0))
    dots_ref[...] = jnp.broadcast_to(line, dots_ref.shape)


def finish_kernel(
    cam_ref, jac_ref, index_ref, errors_in, values_in, given, state_in, tilde_in, dots_ref,
    step_ref, residual_ref, flip_ref,
):
    values = [values_in[number] for number in range(3)]
    image = project(cam_ref, jac_ref, errors_in, values, index_ref[...])
    guess, damp = given[0], given[2]
    scaled, precond = state_in[1], state_in[2]
    first, tilde_residual, tilde = (tilde_in[number] for number in range(3))
    image = damp * tilde + image
    total = column_sums(dots_ref[...])
    inner, curve, tilde_inner, cross, back_inner, tilde_curve = (
        total[:, number : number + 1] for number in range(6)
    )
    mixed = cross - tilde_curve
    back_curve = back_inner - mixed
    first_step = inner / curve
    shift = first_step - 1.0
    inner_next = tilde_inner - 2.0 * shift * cross + shift * shift * back_inner
    curve_next = tilde_curve - 2.0 * shift * mixed + shift * shift * back_curve
    ratio = inner_next / inner
    against = cross - shift * back_inner
    second_step = inner_next / (curve_next + 2.0 * ratio * against + ratio * ratio * curve)
    direction = tilde - shift * (precond * first) + ratio * scaled
    moved = image - shift * (first - image) + ratio * first
    flip_ref[0, :16, :] = guess + first_step * scaled + second_step * direction
    flip_ref[1, :16, :] = tilde_residual - shift * first - second_step * moved
    step_ref[...] = jnp.transpose(flip_ref[0])[:9, :16]
    residual_ref[...] = jnp.transpose(flip_ref[1])[:9, :16]


def vmem(count):
    return [pl.BlockSpec(memory_space=pltpu.VMEM) for _ in range(count)]


def out_f32(*shape):
    return jax.ShapeDtypeStruct(shape, F32)


SEG = ("chip", "core")


def shards(
    cam_jac, point_jac, obs_point, obs_count, back_list, front_list, point_damp, cam_damp,
    right_side, start_guess,
):
    cameras, width = obs_point.shape
    chips = lax.axis_size("chip")
    count = 2 * chips
    mates = [(i, i ^ 1) for i in range(count)]
    others = []
    for i in range(1, count - 1, 2):
        others += [(i, i + 1), (i + 1, i)]
    params = pltpu.CompilerParams(vmem_limit_bytes=16 * 2**20)
    inputs = (
        cam_jac, point_jac, obs_point, obs_count.reshape(1, -1), back_list, front_list,
        point_damp.reshape(-1, LANES), cam_damp.reshape(1, -1), right_side, start_guess,
    )

    def scratch(values):
        return [
            pltpu.VMEM((values, cameras, width), F32),
            pltpu.VMEM((cameras, width), F32),
            pltpu.VMEM((cameras, width), F32),
        ]

    def exchange(to_mate, to_other):
        other = lax.ppermute(to_other, SEG, others)
        mate = lax.ppermute(to_mate, SEG, mates)
        return mate, other

    def call(kernel, name, outs, operands, scratches=(), spaces=None):
        return pl.pallas_call(
            kernel,
            out_shape=outs,
            in_specs=spaces or vmem(len(operands)),
            out_specs=tuple(vmem(len(outs))),
            scratch_shapes=list(scratches),
            compiler_params=params,
            name=name,
        )(*operands)

    plane = out_f32(2, cameras, width)
    to_mate, to_other, own, place, errors, jac, given = call(
        first_kernel,
        "first",
        (
            out_f32(9 * SIDE, LANES),
            out_f32(9 * SIDE, LANES),
            out_f32(9, PAD_ROWS, LANES),
            jax.ShapeDtypeStruct((cameras, width), I32),
            plane,
            out_f32(7, cameras, width),
            out_f32(3, 16, LANES),
        ),
        tuple(pltpu.with_memory_space_constraint(value, pltpu.HBM) for value in inputs),
        scratch(18)
        + [pltpu.VMEM(value.shape, value.dtype) for value in inputs]
        + [pltpu.VMEM((3, LANES, LANES), F32), pltpu.SemaphoreType.DMA((len(inputs),))],
        [pl.BlockSpec(memory_space=pltpu.HBM) for _ in inputs],
    )
    mate, other = exchange(to_mate, to_other)
    (precond,) = call(side_kernel, "side", (out_f32(16, LANES),), (cam_jac, jac, given))
    own_shape = out_f32(3, PAD_ROWS, LANES)
    to_mate, to_other, own, errors, inverse, state = call(
        second_kernel,
        "second",
        (
            out_f32(3 * SIDE, LANES),
            out_f32(3 * SIDE, LANES),
            own_shape,
            plane,
            out_f32(6, PAD_ROWS, LANES),
            out_f32(3, 16, LANES),
        ),
        (cam_jac, jac, place, errors, own, mate, other, given, precond),
        scratch(6),
    )
    mate, other = exchange(to_mate, to_other)
    to_mate, to_other, own, errors, tilde, rows = call(
        third_kernel,
        "third",
        (
            out_f32(3 * SIDE + 6, LANES),
            out_f32(3 * SIDE, LANES),
            own_shape,
            plane,
            out_f32(3, 16, LANES),
            out_f32(6, LANES),
        ),
        (cam_jac, jac, place, errors, own, mate, other, inverse, given, state),
        scratch(6),
    )
    mate, other = exchange(to_mate, to_other)
    values, dots = call(
        sum_kernel,
        "sum",
        (own_shape, out_f32(chips, LANES)),
        (own, mate, other, inverse, rows),
    )
    dots = lax.all_to_all(dots, "chip", 0, 0, tiled=True)
    return call(
        finish_kernel,
        "finish",
        (out_f32(9, 16), out_f32(9, 16)),
        (cam_jac, jac, place, errors, values, given, state, tilde, dots),
        [pltpu.VMEM((2, LANES, LANES), F32)],
    )


def solution(mesh):
    finer = Mesh(mesh.devices.reshape(-1, 2), SEG)
    return jax.shard_map(
        shards,
        mesh=finer,
        in_specs=(
            P(None, SEG, None),
            P(None, SEG, None),
            P(SEG, None),
            P(SEG),
            P(SEG, None),
            P(SEG, None),
            P(SEG),
            P(SEG),
            P(None, SEG),
            P(None, SEG),
        ),
        out_specs=(P(None, SEG), P(None, SEG)),
        check_vma=False,
    )
```

```python
import jax
import jax.numpy as jnp
from jax import lax
from jax.experimental import pallas as pl
from jax.experimental.pallas import tpu as pltpu
from jax.sharding import Mesh
from jax.sharding import PartitionSpec as P

F32 = jnp.float32
BF16 = jnp.bfloat16
I32 = jnp.int32
LANES = 128
ENTRY_PAIRS = ((0, 0), (0, 1), (0, 2), (1, 1), (1, 2), (2, 2))

SIDE = 6
LIST_ROWS = 3
NEXT_SLOTS = 3
PREV_SLOTS = 6
OWN_FRONT = 9
INTERIOR = 12
ROWS = 14
PAD_ROWS = 16


def row_of(block, index, rows):
    return jnp.broadcast_to(block[index : index + 1, :], (rows, block.shape[1]))


def sub_iota(rows, width):
    return lax.broadcasted_iota(I32, (rows, width), 0)


def lane_iota(rows, width):
    return lax.broadcasted_iota(I32, (rows, width), 1)


def nt(left, right, **kw):
    return lax.dot_general(
        left, right, (((1,), (1,)), ((), ())), preferred_element_type=F32, **kw
    )


def split_two(value):
    high = value.astype(BF16)
    low = (value - high.astype(F32)).astype(BF16)
    return high.astype(F32), low.astype(F32)


def flip_block(block_ref):
    return jnp.transpose(block_ref[...])[:16]


def one_hot_rows(index_row, rows, width):
    packed = jnp.broadcast_to(index_row, (16, width)).astype(BF16)
    parts = []
    for start in range(0, rows, 16):
        ids = (sub_iota(16, width) + start).astype(F32).astype(BF16)
        parts.append(jnp.where(packed == ids, jnp.ones_like(packed), jnp.zeros_like(packed)))
    return parts[0] if len(parts) == 1 else jnp.concatenate(parts, axis=0)


def scatter_rows(value_refs, high_ref, low_ref, cameras, width, group):
    ids = sub_iota(16, width).astype(F32).astype(BF16)

    def step(number, total):
        for inner in range(group):
            pick = pl.ds(number * group + inner, 1)
            lanes = one_hot_rows(low_ref[pick, :], LANES, width).astype(jnp.float8_e4m3fn)
            mask = jnp.broadcast_to(high_ref[pick, :], (16, width)).astype(BF16) == ids
            rows = []
            for ref, index in value_refs:
                spread = jnp.broadcast_to(ref[index, pick, :], (16, width)).astype(BF16)
                rows.append(jnp.where(mask, spread, jnp.zeros_like(spread)))
            piece = nt(jnp.concatenate(rows, axis=0), lanes)
            total = piece if total is None else total + piece
        return total

    if group == cameras:
        return step(0, None)
    start = jnp.zeros((16 * len(value_refs), LANES), F32)
    return lax.fori_loop(0, cameras // group, step, start)


def fold_parts(total, index):
    start = 2 * PAD_ROWS * index
    return total[start : start + PAD_ROWS] + total[start + PAD_ROWS : start + 2 * PAD_ROWS]


def gather_rows(tables, row_index, lane_index, rows):
    halves = []
    for top in range(0, row_index.shape[0], 8):
        pieces = []
        for start in range(0, row_index.shape[1], LANES):
            row_part = row_index[top : top + 8, start : start + LANES]
            lane_part = lane_index[top : top + 8, start : start + LANES]
            outs = [None] * len(tables)
            for row in range(rows):
                here = row_part == row
                for number, table in enumerate(tables):
                    spread = jnp.broadcast_to(table[row : row + 1, :], (8, LANES))
                    got = jnp.take_along_axis(spread, lane_part, axis=1, mode="promise_in_bounds")
                    outs[number] = got if row == 0 else jnp.where(here, got, outs[number])
            pieces.append(outs)
        halves.append([jnp.concatenate([p[n] for p in pieces], axis=1) for n in range(len(tables))])
    return [jnp.concatenate([h[n] for h in halves], axis=0) for n in range(len(tables))]


def errors_of(cam_ref, vector, weights):
    rows = []
    for row in range(2):
        running = None
        for column in range(9):
            term = cam_ref[9 * row + column].astype(F32) * vector[:, column : column + 1]
            running = term if running is None else running + term
        rows.append(running * weights)
    return rows


def send_rows(mate_ref, other_ref, index, block):
    odd = lax.axis_index("core") == 1
    to_next = block[:SIDE]
    to_prev = block[SIDE : 2 * SIDE]
    mate_ref[SIDE * index : SIDE * (index + 1), :] = jnp.where(odd, to_prev, to_next)
    other_ref[SIDE * index : SIDE * (index + 1), :] = jnp.where(odd, to_next, to_prev)


def point_table(back, front):
    border = back.shape[1]
    eight = sub_iota(8, border)
    lanes = lane_iota(8, border)
    lefts, rights = [], []
    for listed, base in ((back, 0), (front, OWN_FRONT)):
        high = listed >> 7
        low = listed & 127
        hit = jnp.broadcast_to(high, (8, border)) == eight
        row_value = ((lanes >> 7) + (base + 1)).astype(F32)
        lane_value = (lanes & 127).astype(F32)
        zero = jnp.zeros((8, border), F32)
        lefts.append(
            jnp.concatenate(
                [jnp.where(hit, row_value, zero), jnp.where(hit, lane_value, zero)], axis=0
            ).astype(BF16)
        )
        rights.append(one_hot_rows(low.astype(F32), LANES, border))
    table = nt(lefts[0], rights[0]) + nt(lefts[1], rights[1])
    row_plus = table[:8]
    lane = table[8:]
    free = jnp.where(row_plus == 0.0, 1.0, 0.0)
    upper = jnp.where(sub_iota(LANES, LANES) <= lane_iota(LANES, LANES), 1.0, 0.0).astype(BF16)
    seen = lax.dot_general(
        free.astype(BF16), upper, (((1,), (0,)), ((), ())), preferred_element_type=F32
    )
    total = jnp.broadcast_to(seen[:, LANES - 1 : LANES], (8, LANES))
    before = jnp.zeros((8, LANES), F32)
    rows = sub_iota(8, LANES)
    for row in range(7):
        before = before + jnp.where(rows > row, row_of(total, row, 8), 0.0)
    rank = before + seen - free
    return jnp.where(
        free > 0.0, rank + float(INTERIOR * LANES), (row_plus - 1.0) * float(LANES) + lane
    ).astype(I32)


def first_kernel(
    cam_hbm, point_hbm, obs_hbm, count_hbm, back_hbm, front_hbm, damp_hbm, cam_damp_hbm,
    right_hbm, guess_hbm,
    mate_ref, other_ref, own_ref, index_ref, errors_ref, jac_ref, state_ref,
    value_ref, high_ref, low_ref,
    cam_ref, point_ref, obs_ref, count_ref, back_ref, front_ref, damp_ref, cam_damp_ref,
    right_ref, guess_ref, flip_ref, sems,
):
    sources = (
        back_hbm, front_hbm, obs_hbm, guess_hbm, right_hbm, cam_damp_hbm, count_hbm, point_hbm,
        cam_hbm, damp_hbm,
    )
    targets = (
        back_ref, front_ref, obs_ref, guess_ref, right_ref, cam_damp_ref, count_ref, point_ref,
        cam_ref, damp_ref,
    )
    copies = [
        pltpu.make_async_copy(source, target, sems.at[number])
        for number, (source, target) in enumerate(zip(sources, targets))
    ]
    for copy in copies:
        copy.start()
    cameras, width = obs_ref.shape
    border = back_ref.shape[1]
    points = damp_ref.shape[0] * damp_ref.shape[1]
    for copy in copies[:2]:
        copy.wait()
    table = point_table(back_ref[...], front_ref[...])
    for copy in copies[2:7]:
        copy.wait()
    observed = obs_ref[...]
    own_place = gather_rows([table], observed >> 7, observed & 127, points // LANES)[0]
    place = jnp.where(
        observed < points,
        own_place,
        jnp.where(
            observed < points + border,
            observed + (PREV_SLOTS * LANES - points),
            observed + (NEXT_SLOTS * LANES - points - border),
        ),
    )
    index_ref[...] = place
    high_ref[...] = (place >> 7).astype(F32)
    low_ref[...] = (place & 127).astype(F32)
    valid = lane_iota(16, LANES) < 9
    flip_ref[0, :9, :16] = guess_ref[...]
    flip_ref[1, :9, :16] = right_ref[...]
    flip_ref[2, 0:1, :16] = cam_damp_ref[...]
    flip_ref[2, 1:2, :16] = count_ref[...].astype(F32)
    guess = jnp.where(valid, flip_block(flip_ref.at[0]), 0.0)
    right = jnp.where(valid, flip_block(flip_ref.at[1]), 0.0)
    sides = flip_block(flip_ref.at[2])
    damp = jnp.where(valid, sides[:, 0:1], 0.0)
    weights = (lane_iota(cameras, width).astype(F32) < sides[:, 1:2]).astype(F32)
    state_ref[0] = guess
    state_ref[1] = right
    state_ref[2] = damp
    copies[7].wait()
    jac = [point_ref[entry].astype(F32) * weights for entry in range(6)]
    for entry in range(6):
        jac_ref[entry] = jac[entry]
    jac_ref[6] = weights
    products = [jac[a] * jac[b] + jac[3 + a] * jac[3 + b] for a, b in ENTRY_PAIRS]
    copies[8].wait()
    copies[9].wait()
    errors = errors_of(cam_ref, guess, weights)
    errors_ref[0] = errors[0]
    errors_ref[1] = errors[1]
    products += [errors[0] * jac[j] + errors[1] * jac[3 + j] for j in range(3)]
    for number, product in enumerate(products):
        value_ref[2 * number], value_ref[2 * number + 1] = split_two(product)
    total = scatter_rows(
        [(value_ref, number) for number in range(18)], high_ref, low_ref, cameras, width, cameras
    )
    ids = sub_iota(16, LANES).astype(F32).astype(BF16)
    damping = None
    new_high = (table >> 7).astype(F32)
    new_low = (table & 127).astype(F32)
    first, rest = split_two(damp_ref[...])
    last = damp_ref[...] - first - rest
    for row in range(points // LANES):
        lanes = one_hot_rows(new_low[row : row + 1, :], LANES, LANES)
        mask = row_of(new_high, row, 16).astype(BF16) == ids
        parts = []
        for part in (first, rest, last):
            spread = row_of(part, row, 16).astype(BF16)
            parts.append(jnp.where(mask, spread, jnp.zeros_like(spread)))
        piece = nt(jnp.concatenate(parts, axis=0), lanes)
        damping = piece if damping is None else damping + piece
    damping = damping[:16] + damping[16:32] + damping[32:]
    for number in range(9):
        block = fold_parts(total, number)
        if number in (0, 3, 5):
            block = block + damping
        own_ref[number] = block
        send_rows(mate_ref, other_ref, number, block)


def complete(own_ref, mate_ref, other_ref, number):
    odd = lax.axis_index("core") == 1
    block = own_ref[number]
    mate = mate_ref[SIDE * number : SIDE * (number + 1), :]
    other = other_ref[SIDE * number : SIDE * (number + 1), :]
    after = jnp.where(odd, other, mate)
    before = jnp.where(odd, mate, other)
    tail = jnp.zeros((PAD_ROWS - 2 * SIDE, LANES), F32)
    return block + jnp.concatenate([after, before, tail], axis=0)


def symmetric_inverse(entries):
    cofactors = [
        entries[3] * entries[5] - entries[4] * entries[4],
        entries[2] * entries[4] - entries[1] * entries[5],
        entries[1] * entries[4] - entries[2] * entries[3],
        entries[0] * entries[5] - entries[2] * entries[2],
        entries[1] * entries[2] - entries[0] * entries[4],
        entries[0] * entries[3] - entries[1] * entries[1],
    ]
    determinant = entries[0] * cofactors[0] + entries[1] * cofactors[1] + entries[2] * cofactors[2]
    determinant = jnp.where(determinant == 0.0, 1.0, determinant)
    return [member / determinant for member in cofactors]


def apply_inverse(inverse, sums):
    return [
        inverse[0] * sums[0] + inverse[1] * sums[1] + inverse[2] * sums[2],
        inverse[1] * sums[0] + inverse[3] * sums[1] + inverse[4] * sums[2],
        inverse[2] * sums[0] + inverse[4] * sums[1] + inverse[5] * sums[2],
    ]


def pack_columns(cols):
    lanes = lane_iota(16, LANES)
    out = jnp.zeros((16, LANES), F32)
    for number, col in enumerate(cols):
        out = jnp.where(lanes == number, col, out)
    return out


def project(cam_ref, jac_ref, errors_ref, values, place):
    high = place >> 7
    low = place & 127
    picked = gather_rows(values, high, low, ROWS)
    adjusted = []
    for row in range(2):
        back = (
            picked[0] * jac_ref[3 * row]
            + picked[1] * jac_ref[3 * row + 1]
            + picked[2] * jac_ref[3 * row + 2]
        )
        adjusted.append(errors_ref[row] - back)
    cols = []
    for column in range(9):
        term = (
            cam_ref[column].astype(F32) * adjusted[0]
            + cam_ref[9 + column].astype(F32) * adjusted[1]
        )
        cols.append(jnp.sum(term, axis=1, keepdims=True))
    return pack_columns(cols)


def next_scatter(
    cam_ref, jac_ref, vector, place, value_ref, high_ref, low_ref,
    mate_ref, other_ref, own_ref, errors_ref,
):
    cameras, width = place.shape
    errors = errors_of(cam_ref, vector, jac_ref[6])
    errors_ref[0] = errors[0]
    errors_ref[1] = errors[1]
    for j in range(3):
        product = errors[0] * jac_ref[j] + errors[1] * jac_ref[3 + j]
        value_ref[2 * j], value_ref[2 * j + 1] = split_two(product)
    high_ref[...] = (place >> 7).astype(F32)
    low_ref[...] = (place & 127).astype(F32)
    total = scatter_rows(
        [(value_ref, number) for number in range(6)], high_ref, low_ref, cameras, width, 8
    )
    blocks = []
    for number in range(3):
        block = fold_parts(total, number)
        own_ref[number] = block
        send_rows(mate_ref, other_ref, number, block)
        blocks.append(block)
    return errors, blocks


def side_kernel(cam_ref, jac_ref, given, precond_ref):
    cols = []
    for column in range(9):
        squared = cam_ref[column].astype(F32) ** 2 + cam_ref[9 + column].astype(F32) ** 2
        cols.append(jnp.sum(squared * jac_ref[6], axis=1, keepdims=True))
    valid = lane_iota(16, LANES) < 9
    precond_ref[...] = jnp.where(valid, 1.0 / (pack_columns(cols) + given[2]), 0.0)


def second_kernel(
    cam_ref, jac_ref, index_ref, errors_in, own_in, mate_in, other_in, state_in, precond_in,
    mate_ref, other_ref, own_ref, errors_ref, inverse_ref, state_ref,
    value_ref, high_ref, low_ref,
):
    blocks = [complete(own_in, mate_in, other_in, number) for number in range(9)]
    inverse = symmetric_inverse(blocks[:6])
    for number in range(6):
        inverse_ref[number] = inverse[number]
    place = index_ref[...]
    values = apply_inverse(inverse, blocks[6:])
    image = project(cam_ref, jac_ref, errors_in, values, place)
    guess, right, damp = state_in[0], state_in[1], state_in[2]
    precond = precond_in[...]
    residual = right - (damp * guess + image)
    scaled = precond * residual
    state_ref[0] = residual
    state_ref[1] = scaled
    state_ref[2] = precond
    next_scatter(
        cam_ref, jac_ref, scaled, place, value_ref, high_ref, low_ref,
        mate_ref, other_ref, own_ref, errors_ref,
    )


def unshared_rows():
    chip = lax.axis_index("chip")
    core = lax.axis_index("core")
    first = jnp.logical_and(chip == 0, core == 0)
    last = jnp.logical_and(chip == lax.axis_size("chip") - 1, core == 1)
    start = jnp.where(first, SIDE, INTERIOR)
    stop = jnp.where(last, SIDE, 0)
    rows = sub_iota(PAD_ROWS, LANES)
    return jnp.logical_or(rows >= start, rows < stop)


def column_sums(block):
    return jnp.sum(block, axis=0, keepdims=True)


def third_kernel(
    cam_ref, jac_ref, index_ref, errors_in, own_in, mate_in, other_in, inverse_in, given, state_in,
    mate_ref, other_ref, own_ref, errors_ref, state_ref, rows_ref,
    value_ref, high_ref, low_ref,
):
    sums = [complete(own_in, mate_in, other_in, number) for number in range(3)]
    inverse = [inverse_in[number] for number in range(6)]
    values = apply_inverse(inverse, sums)
    place = index_ref[...]
    image = project(cam_ref, jac_ref, errors_in, values, place)
    damp = given[2]
    residual, scaled, precond = state_in[0], state_in[1], state_in[2]
    image = damp * scaled + image
    tilde_residual = residual - image
    tilde = precond * tilde_residual
    state_ref[0] = image
    state_ref[1] = tilde_residual
    state_ref[2] = tilde
    errors, blocks = next_scatter(
        cam_ref, jac_ref, tilde, place, value_ref, high_ref, low_ref,
        mate_ref, other_ref, own_ref, errors_ref,
    )
    energy = column_sums(damp * tilde * tilde)
    squares = column_sums(errors[0] * errors[0] + errors[1] * errors[1])
    for start in range(0, squares.shape[1], LANES):
        energy = energy + squares[:, start : start + LANES]
    lone = unshared_rows()
    for value, point in zip(apply_inverse(inverse, blocks), blocks):
        energy = energy - column_sums(jnp.where(lone, value * point, 0.0))
    rows = [
        column_sums(residual * scaled),
        column_sums(image * scaled),
        column_sums(tilde_residual * tilde),
        column_sums(image * tilde),
        column_sums(image * (precond * image)),
        energy,
    ]
    for number, row in enumerate(rows):
        rows_ref[number : number + 1, :] = row
        mate_ref[3 * SIDE + number : 3 * SIDE + number + 1, :] = row


def sum_kernel(own_in, mate_in, other_in, inverse_in, rows_in, values_ref, dots_ref):
    sums = [complete(own_in, mate_in, other_in, number) for number in range(3)]
    inverse = [inverse_in[number] for number in range(6)]
    values = apply_inverse(inverse, sums)
    shared = None
    for number in range(3):
        values_ref[number] = values[number]
        term = values[number] * sums[number]
        shared = term if shared is None else shared + term
    border = column_sums(jnp.where(unshared_rows(), 0.0, shared))
    rows = rows_in[...] + mate_in[3 * SIDE : 3 * SIDE + 6, :]
    rows = rows - jnp.where(sub_iota(6, LANES) == 5, border, 0.0)
    totals = jnp.sum(rows, axis=1, keepdims=True)
    line = column_sums(jnp.where(sub_iota(6, LANES) == lane_iota(6, LANES), totals, 0.0))
    dots_ref[...] = jnp.broadcast_to(line, dots_ref.shape)


def finish_kernel(
    cam_ref, jac_ref, index_ref, errors_in, values_in, given, state_in, tilde_in, dots_ref,
    step_ref, residual_ref, flip_ref,
):
    values = [values_in[number] for number in range(3)]
    image = project(cam_ref, jac_ref, errors_in, values, index_ref[...])
    guess, damp = given[0], given[2]
    scaled, precond = state_in[1], state_in[2]
    first, tilde_residual, tilde = (tilde_in[number] for number in range(3))
    image = damp * tilde + image
    total = column_sums(dots_ref[...])
    inner, curve, tilde_inner, cross, back_inner, tilde_curve = (
        total[:, number : number + 1] for number in range(6)
    )
    mixed = cross - tilde_curve
    back_curve = back_inner - mixed
    first_step = inner / curve
    shift = first_step - 1.0
    inner_next = tilde_inner - 2.0 * shift * cross + shift * shift * back_inner
    curve_next = tilde_curve - 2.0 * shift * mixed + shift * shift * back_curve
    ratio = inner_next / inner
    against = cross - shift * back_inner
    second_step = inner_next / (curve_next + 2.0 * ratio * against + ratio * ratio * curve)
    direction = tilde - shift * (precond * first) + ratio * scaled
    moved = image - shift * (first - image) + ratio * first
    flip_ref[0, :16, :] = guess + first_step * scaled + second_step * direction
    flip_ref[1, :16, :] = tilde_residual - shift * first - second_step * moved
    step_ref[...] = jnp.transpose(flip_ref[0])[:9, :16]
    residual_ref[...] = jnp.transpose(flip_ref[1])[:9, :16]


def vmem(count):
    return [pl.BlockSpec(memory_space=pltpu.VMEM) for _ in range(count)]


def out_f32(*shape):
    return jax.ShapeDtypeStruct(shape, F32)


SEG = ("chip", "core")


def shards(
    cam_jac, point_jac, obs_point, obs_count, back_list, front_list, point_damp, cam_damp,
    right_side, start_guess,
):
    cameras, width = obs_point.shape
    chips = lax.axis_size("chip")
    count = 2 * chips
    mates = [(i, i ^ 1) for i in range(count)]
    others = []
    for i in range(1, count - 1, 2):
        others += [(i, i + 1), (i + 1, i)]
    params = pltpu.CompilerParams(vmem_limit_bytes=16 * 2**20)
    inputs = (
        cam_jac, point_jac, obs_point, obs_count.reshape(1, -1), back_list, front_list,
        point_damp.reshape(-1, LANES), cam_damp.reshape(1, -1), right_side, start_guess,
    )

    def scratch(values):
        return [
            pltpu.VMEM((values, cameras, width), F32),
            pltpu.VMEM((cameras, width), F32),
            pltpu.VMEM((cameras, width), F32),
        ]

    def exchange(to_mate, to_other):
        other = lax.ppermute(to_other, SEG, others)
        mate = lax.ppermute(to_mate, SEG, mates)
        return mate, other

    def call(kernel, name, outs, operands, scratches=(), spaces=None):
        return pl.pallas_call(
            kernel,
            out_shape=outs,
            in_specs=spaces or vmem(len(operands)),
            out_specs=tuple(vmem(len(outs))),
            scratch_shapes=list(scratches),
            compiler_params=params,
            name=name,
        )(*operands)

    plane = out_f32(2, cameras, width)
    to_mate, to_other, own, place, errors, jac, given = call(
        first_kernel,
        "first",
        (
            out_f32(9 * SIDE, LANES),
            out_f32(9 * SIDE, LANES),
            out_f32(9, PAD_ROWS, LANES),
            jax.ShapeDtypeStruct((cameras, width), I32),
            plane,
            out_f32(7, cameras, width),
            out_f32(3, 16, LANES),
        ),
        tuple(pltpu.with_memory_space_constraint(value, pltpu.HBM) for value in inputs),
        scratch(18)
        + [pltpu.VMEM(value.shape, value.dtype) for value in inputs]
        + [pltpu.VMEM((3, LANES, LANES), F32), pltpu.SemaphoreType.DMA((len(inputs),))],
        [pl.BlockSpec(memory_space=pltpu.HBM) for _ in inputs],
    )
    mate, other = exchange(to_mate, to_other)
    (precond,) = call(side_kernel, "side", (out_f32(16, LANES),), (cam_jac, jac, given))
    own_shape = out_f32(3, PAD_ROWS, LANES)
    to_mate, to_other, own, errors, inverse, state = call(
        second_kernel,
        "second",
        (
            out_f32(3 * SIDE, LANES),
            out_f32(3 * SIDE, LANES),
            own_shape,
            plane,
            out_f32(6, PAD_ROWS, LANES),
            out_f32(3, 16, LANES),
        ),
        (cam_jac, jac, place, errors, own, mate, other, given, precond),
        scratch(6),
    )
    mate, other = exchange(to_mate, to_other)
    to_mate, to_other, own, errors, tilde, rows = call(
        third_kernel,
        "third",
        (
            out_f32(3 * SIDE + 6, LANES),
            out_f32(3 * SIDE, LANES),
            own_shape,
            plane,
            out_f32(3, 16, LANES),
            out_f32(6, LANES),
        ),
        (cam_jac, jac, place, errors, own, mate, other, inverse, given, state),
        scratch(6),
    )
    mate, other = exchange(to_mate, to_other)
    values, dots = call(
        sum_kernel,
        "sum",
        (own_shape, out_f32(chips, LANES)),
        (own, mate, other, inverse, rows),
    )
    dots = lax.all_to_all(dots, "chip", 0, 0, tiled=True)
    return call(
        finish_kernel,
        "finish",
        (out_f32(9, 16), out_f32(9, 16)),
        (cam_jac, jac, place, errors, values, given, state, tilde, dots),
        [pltpu.VMEM((2, LANES, LANES), F32)],
    )


def solution(mesh):
    finer = Mesh(mesh.devices.reshape(-1, 2), SEG)
    return jax.shard_map(
        shards,
        mesh=finer,
        in_specs=(
            P(None, SEG, None),
            P(None, SEG, None),
            P(SEG, None),
            P(SEG),
            P(SEG, None),
            P(SEG, None),
            P(SEG),
            P(SEG),
            P(None, SEG),
            P(None, SEG),
        ),
        out_specs=(P(None, SEG), P(None, SEG)),
        check_vma=False,
    )
```

```python
import jax
import jax.numpy as jnp
from jax import lax
from jax.experimental import pallas as pl
from jax.experimental.pallas import tpu as pltpu
from jax.sharding import Mesh
from jax.sharding import PartitionSpec as P

F32 = jnp.float32
BF16 = jnp.bfloat16
I32 = jnp.int32
LANES = 128
ENTRY_PAIRS = ((0, 0), (0, 1), (0, 2), (1, 1), (1, 2), (2, 2))

SIDE = 6
LIST_ROWS = 3
NEXT_SLOTS = 3
PREV_SLOTS = 6
OWN_FRONT = 9
INTERIOR = 12
ROWS = 14
PAD_ROWS = 16


def row_of(block, index, rows):
    return jnp.broadcast_to(block[index : index + 1, :], (rows, block.shape[1]))


def sub_iota(rows, width):
    return lax.broadcasted_iota(I32, (rows, width), 0)


def lane_iota(rows, width):
    return lax.broadcasted_iota(I32, (rows, width), 1)


def nt(left, right, **kw):
    return lax.dot_general(
        left, right, (((1,), (1,)), ((), ())), preferred_element_type=F32, **kw
    )


def split_two(value):
    high = value.astype(BF16)
    low = (value - high.astype(F32)).astype(BF16)
    return high.astype(F32), low.astype(F32)


def flip_block(block_ref):
    return jnp.transpose(block_ref[...])[:16]


def one_hot_rows(index_row, rows, width):
    packed = jnp.broadcast_to(index_row, (16, width)).astype(BF16)
    parts = []
    for start in range(0, rows, 16):
        ids = (sub_iota(16, width) + start).astype(F32).astype(BF16)
        parts.append(jnp.where(packed == ids, jnp.ones_like(packed), jnp.zeros_like(packed)))
    return parts[0] if len(parts) == 1 else jnp.concatenate(parts, axis=0)


def scatter_rows(value_refs, high_ref, low_ref, cameras, width, group):
    ids = sub_iota(16, width).astype(F32).astype(BF16)

    def step(number, total):
        for inner in range(group):
            pick = pl.ds(number * group + inner, 1)
            lanes = one_hot_rows(low_ref[pick, :], LANES, width).astype(jnp.float8_e4m3fn)
            mask = jnp.broadcast_to(high_ref[pick, :], (16, width)).astype(BF16) == ids
            rows = []
            for ref, index in value_refs:
                spread = jnp.broadcast_to(ref[index, pick, :], (16, width)).astype(BF16)
                rows.append(jnp.where(mask, spread, jnp.zeros_like(spread)))
            piece = nt(jnp.concatenate(rows, axis=0), lanes)
            total = piece if total is None else total + piece
        return total

    if group == cameras:
        return step(0, None)
    start = jnp.zeros((16 * len(value_refs), LANES), F32)
    return lax.fori_loop(0, cameras // group, step, start)


def fold_parts(total, index):
    start = 2 * PAD_ROWS * index
    return total[start : start + PAD_ROWS] + total[start + PAD_ROWS : start + 2 * PAD_ROWS]


def gather_rows(tables, row_index, lane_index, rows):
    halves = []
    for top in range(0, row_index.shape[0], 8):
        pieces = []
        for start in range(0, row_index.shape[1], LANES):
            row_part = row_index[top : top + 8, start : start + LANES]
            lane_part = lane_index[top : top + 8, start : start + LANES]
            outs = [None] * len(tables)
            for row in range(rows):
                here = row_part == row
                for number, table in enumerate(tables):
                    spread = jnp.broadcast_to(table[row : row + 1, :], (8, LANES))
                    got = jnp.take_along_axis(spread, lane_part, axis=1, mode="promise_in_bounds")
                    outs[number] = got if row == 0 else jnp.where(here, got, outs[number])
            pieces.append(outs)
        halves.append([jnp.concatenate([p[n] for p in pieces], axis=1) for n in range(len(tables))])
    return [jnp.concatenate([h[n] for h in halves], axis=0) for n in range(len(tables))]


def errors_of(cam_ref, vector, weights):
    rows = []
    for row in range(2):
        running = None
        for column in range(9):
            term = cam_ref[9 * row + column].astype(F32) * vector[:, column : column + 1]
            running = term if running is None else running + term
        rows.append(running * weights)
    return rows


def send_rows(mate_ref, other_ref, index, block):
    odd = lax.axis_index("core") == 1
    to_next = block[:SIDE]
    to_prev = block[SIDE : 2 * SIDE]
    mate_ref[SIDE * index : SIDE * (index + 1), :] = jnp.where(odd, to_prev, to_next)
    other_ref[SIDE * index : SIDE * (index + 1), :] = jnp.where(odd, to_next, to_prev)


def point_table(back, front):
    border = back.shape[1]
    eight = sub_iota(8, border)
    lanes = lane_iota(8, border)
    lefts, rights = [], []
    for listed, base in ((back, 0), (front, OWN_FRONT)):
        high = listed >> 7
        low = listed & 127
        hit = jnp.broadcast_to(high, (8, border)) == eight
        row_value = ((lanes >> 7) + (base + 1)).astype(F32)
        lane_value = (lanes & 127).astype(F32)
        zero = jnp.zeros((8, border), F32)
        lefts.append(
            jnp.concatenate(
                [jnp.where(hit, row_value, zero), jnp.where(hit, lane_value, zero)], axis=0
            ).astype(BF16)
        )
        rights.append(one_hot_rows(low.astype(F32), LANES, border))
    table = nt(lefts[0], rights[0]) + nt(lefts[1], rights[1])
    row_plus = table[:8]
    lane = table[8:]
    free = jnp.where(row_plus == 0.0, 1.0, 0.0)
    upper = jnp.where(sub_iota(LANES, LANES) <= lane_iota(LANES, LANES), 1.0, 0.0).astype(BF16)
    seen = lax.dot_general(
        free.astype(BF16), upper, (((1,), (0,)), ((), ())), preferred_element_type=F32
    )
    total = jnp.broadcast_to(seen[:, LANES - 1 : LANES], (8, LANES))
    before = jnp.zeros((8, LANES), F32)
    rows = sub_iota(8, LANES)
    for row in range(7):
        before = before + jnp.where(rows > row, row_of(total, row, 8), 0.0)
    rank = before + seen - free
    return jnp.where(
        free > 0.0, rank + float(INTERIOR * LANES), (row_plus - 1.0) * float(LANES) + lane
    ).astype(I32)


def first_kernel(
    cam_hbm, point_hbm, obs_hbm, count_hbm, back_hbm, front_hbm, damp_hbm, cam_damp_hbm,
    right_hbm, guess_hbm,
    mate_ref, other_ref, own_ref, index_ref, errors_ref, jac_ref, state_ref,
    value_ref, high_ref, low_ref,
    cam_ref, point_ref, obs_ref, count_ref, back_ref, front_ref, damp_ref, cam_damp_ref,
    right_ref, guess_ref, flip_ref, sems,
):
    sources = (
        back_hbm, front_hbm, obs_hbm, guess_hbm, right_hbm, cam_damp_hbm, count_hbm, point_hbm,
        cam_hbm, damp_hbm,
    )
    targets = (
        back_ref, front_ref, obs_ref, guess_ref, right_ref, cam_damp_ref, count_ref, point_ref,
        cam_ref, damp_ref,
    )
    copies = [
        pltpu.make_async_copy(source, target, sems.at[number])
        for number, (source, target) in enumerate(zip(sources, targets))
    ]
    for copy in copies:
        copy.start()
    cameras, width = obs_ref.shape
    border = back_ref.shape[1]
    points = damp_ref.shape[0] * damp_ref.shape[1]
    for copy in copies[:2]:
        copy.wait()
    table = point_table(back_ref[...], front_ref[...])
    for copy in copies[2:7]:
        copy.wait()
    observed = obs_ref[...]
    own_place = gather_rows([table], observed >> 7, observed & 127, points // LANES)[0]
    place = jnp.where(
        observed < points,
        own_place,
        jnp.where(
            observed < points + border,
            observed + (PREV_SLOTS * LANES - points),
            observed + (NEXT_SLOTS * LANES - points - border),
        ),
    )
    index_ref[...] = place
    high_ref[...] = (place >> 7).astype(F32)
    low_ref[...] = (place & 127).astype(F32)
    valid = lane_iota(16, LANES) < 9
    flip_ref[0, :9, :16] = guess_ref[...]
    flip_ref[1, :9, :16] = right_ref[...]
    flip_ref[2, 0:1, :16] = cam_damp_ref[...]
    flip_ref[2, 1:2, :16] = count_ref[...].astype(F32)
    guess = jnp.where(valid, flip_block(flip_ref.at[0]), 0.0)
    right = jnp.where(valid, flip_block(flip_ref.at[1]), 0.0)
    sides = flip_block(flip_ref.at[2])
    damp = jnp.where(valid, sides[:, 0:1], 0.0)
    weights = (lane_iota(cameras, width).astype(F32) < sides[:, 1:2]).astype(F32)
    state_ref[0] = guess
    state_ref[1] = right
    state_ref[2] = damp
    copies[7].wait()
    jac = [point_ref[entry].astype(F32) * weights for entry in range(6)]
    for entry in range(6):
        jac_ref[entry] = jac[entry]
    jac_ref[6] = weights
    products = [jac[a] * jac[b] + jac[3 + a] * jac[3 + b] for a, b in ENTRY_PAIRS]
    copies[8].wait()
    copies[9].wait()
    errors = errors_of(cam_ref, guess, weights)
    errors_ref[0] = errors[0]
    errors_ref[1] = errors[1]
    products += [errors[0] * jac[j] + errors[1] * jac[3 + j] for j in range(3)]
    for number, product in enumerate(products):
        value_ref[2 * number], value_ref[2 * number + 1] = split_two(product)
    total = scatter_rows(
        [(value_ref, number) for number in range(18)], high_ref, low_ref, cameras, width, 8
    )
    ids = sub_iota(16, LANES).astype(F32).astype(BF16)
    damping = None
    new_high = (table >> 7).astype(F32)
    new_low = (table & 127).astype(F32)
    first, rest = split_two(damp_ref[...])
    last = damp_ref[...] - first - rest
    for row in range(points // LANES):
        lanes = one_hot_rows(new_low[row : row + 1, :], LANES, LANES)
        mask = row_of(new_high, row, 16).astype(BF16) == ids
        parts = []
        for part in (first, rest, last):
            spread = row_of(part, row, 16).astype(BF16)
            parts.append(jnp.where(mask, spread, jnp.zeros_like(spread)))
        piece = nt(jnp.concatenate(parts, axis=0), lanes)
        damping = piece if damping is None else damping + piece
    damping = damping[:16] + damping[16:32] + damping[32:]
    for number in range(9):
        block = fold_parts(total, number)
        if number in (0, 3, 5):
            block = block + damping
        own_ref[number] = block
        send_rows(mate_ref, other_ref, number, block)


def complete(own_ref, mate_ref, other_ref, number):
    odd = lax.axis_index("core") == 1
    block = own_ref[number]
    mate = mate_ref[SIDE * number : SIDE * (number + 1), :]
    other = other_ref[SIDE * number : SIDE * (number + 1), :]
    after = jnp.where(odd, other, mate)
    before = jnp.where(odd, mate, other)
    tail = jnp.zeros((PAD_ROWS - 2 * SIDE, LANES), F32)
    return block + jnp.concatenate([after, before, tail], axis=0)


def symmetric_inverse(entries):
    cofactors = [
        entries[3] * entries[5] - entries[4] * entries[4],
        entries[2] * entries[4] - entries[1] * entries[5],
        entries[1] * entries[4] - entries[2] * entries[3],
        entries[0] * entries[5] - entries[2] * entries[2],
        entries[1] * entries[2] - entries[0] * entries[4],
        entries[0] * entries[3] - entries[1] * entries[1],
    ]
    determinant = entries[0] * cofactors[0] + entries[1] * cofactors[1] + entries[2] * cofactors[2]
    determinant = jnp.where(determinant == 0.0, 1.0, determinant)
    return [member / determinant for member in cofactors]


def apply_inverse(inverse, sums):
    return [
        inverse[0] * sums[0] + inverse[1] * sums[1] + inverse[2] * sums[2],
        inverse[1] * sums[0] + inverse[3] * sums[1] + inverse[4] * sums[2],
        inverse[2] * sums[0] + inverse[4] * sums[1] + inverse[5] * sums[2],
    ]


def pack_columns(cols):
    lanes = lane_iota(16, LANES)
    out = jnp.zeros((16, LANES), F32)
    for number, col in enumerate(cols):
        out = jnp.where(lanes == number, col, out)
    return out


def project(cam_ref, jac_ref, errors_ref, values, place):
    high = place >> 7
    low = place & 127
    picked = gather_rows(values, high, low, ROWS)
    adjusted = []
    for row in range(2):
        back = (
            picked[0] * jac_ref[3 * row]
            + picked[1] * jac_ref[3 * row + 1]
            + picked[2] * jac_ref[3 * row + 2]
        )
        adjusted.append(errors_ref[row] - back)
    cols = []
    for column in range(9):
        term = (
            cam_ref[column].astype(F32) * adjusted[0]
            + cam_ref[9 + column].astype(F32) * adjusted[1]
        )
        cols.append(jnp.sum(term, axis=1, keepdims=True))
    return pack_columns(cols)


def next_scatter(
    cam_ref, jac_ref, vector, place, value_ref, high_ref, low_ref,
    mate_ref, other_ref, own_ref, errors_ref,
):
    cameras, width = place.shape
    errors = errors_of(cam_ref, vector, jac_ref[6])
    errors_ref[0] = errors[0]
    errors_ref[1] = errors[1]
    for j in range(3):
        product = errors[0] * jac_ref[j] + errors[1] * jac_ref[3 + j]
        value_ref[2 * j], value_ref[2 * j + 1] = split_two(product)
    high_ref[...] = (place >> 7).astype(F32)
    low_ref[...] = (place & 127).astype(F32)
    total = scatter_rows(
        [(value_ref, number) for number in range(6)], high_ref, low_ref, cameras, width, 8
    )
    blocks = []
    for number in range(3):
        block = fold_parts(total, number)
        own_ref[number] = block
        send_rows(mate_ref, other_ref, number, block)
        blocks.append(block)
    return errors, blocks


def side_kernel(cam_ref, jac_ref, given, precond_ref):
    cols = []
    for column in range(9):
        squared = cam_ref[column].astype(F32) ** 2 + cam_ref[9 + column].astype(F32) ** 2
        cols.append(jnp.sum(squared * jac_ref[6], axis=1, keepdims=True))
    valid = lane_iota(16, LANES) < 9
    precond_ref[...] = jnp.where(valid, 1.0 / (pack_columns(cols) + given[2]), 0.0)


def second_kernel(
    cam_ref, jac_ref, index_ref, errors_in, own_in, mate_in, other_in, state_in, precond_in,
    mate_ref, other_ref, own_ref, errors_ref, inverse_ref, state_ref,
    value_ref, high_ref, low_ref,
):
    blocks = [complete(own_in, mate_in, other_in, number) for number in range(9)]
    inverse = symmetric_inverse(blocks[:6])
    for number in range(6):
        inverse_ref[number] = inverse[number]
    place = index_ref[...]
    values = apply_inverse(inverse, blocks[6:])
    image = project(cam_ref, jac_ref, errors_in, values, place)
    guess, right, damp = state_in[0], state_in[1], state_in[2]
    precond = precond_in[...]
    residual = right - (damp * guess + image)
    scaled = precond * residual
    state_ref[0] = residual
    state_ref[1] = scaled
    state_ref[2] = precond
    next_scatter(
        cam_ref, jac_ref, scaled, place, value_ref, high_ref, low_ref,
        mate_ref, other_ref, own_ref, errors_ref,
    )


def unshared_rows():
    chip = lax.axis_index("chip")
    core = lax.axis_index("core")
    first = jnp.logical_and(chip == 0, core == 0)
    last = jnp.logical_and(chip == lax.axis_size("chip") - 1, core == 1)
    start = jnp.where(first, SIDE, INTERIOR)
    stop = jnp.where(last, SIDE, 0)
    rows = sub_iota(PAD_ROWS, LANES)
    return jnp.logical_or(rows >= start, rows < stop)


def column_sums(block):
    return jnp.sum(block, axis=0, keepdims=True)


def third_kernel(
    cam_ref, jac_ref, index_ref, errors_in, own_in, mate_in, other_in, inverse_in, given, state_in,
    mate_ref, other_ref, own_ref, errors_ref, state_ref, rows_ref,
    value_ref, high_ref, low_ref,
):
    sums = [complete(own_in, mate_in, other_in, number) for number in range(3)]
    inverse = [inverse_in[number] for number in range(6)]
    values = apply_inverse(inverse, sums)
    place = index_ref[...]
    image = project(cam_ref, jac_ref, errors_in, values, place)
    damp = given[2]
    residual, scaled, precond = state_in[0], state_in[1], state_in[2]
    image = damp * scaled + image
    tilde_residual = residual - image
    tilde = precond * tilde_residual
    state_ref[0] = image
    state_ref[1] = tilde_residual
    state_ref[2] = tilde
    errors, blocks = next_scatter(
        cam_ref, jac_ref, tilde, place, value_ref, high_ref, low_ref,
        mate_ref, other_ref, own_ref, errors_ref,
    )
    energy = column_sums(damp * tilde * tilde)
    squares = column_sums(errors[0] * errors[0] + errors[1] * errors[1])
    for start in range(0, squares.shape[1], LANES):
        energy = energy + squares[:, start : start + LANES]
    lone = unshared_rows()
    for value, point in zip(apply_inverse(inverse, blocks), blocks):
        energy = energy - column_sums(jnp.where(lone, value * point, 0.0))
    rows = [
        column_sums(residual * scaled),
        column_sums(image * scaled),
        column_sums(tilde_residual * tilde),
        column_sums(image * tilde),
        column_sums(image * (precond * image)),
        energy,
    ]
    for number, row in enumerate(rows):
        rows_ref[number : number + 1, :] = row
        mate_ref[3 * SIDE + number : 3 * SIDE + number + 1, :] = row


def sum_kernel(own_in, mate_in, other_in, inverse_in, rows_in, values_ref, dots_ref):
    sums = [complete(own_in, mate_in, other_in, number) for number in range(3)]
    inverse = [inverse_in[number] for number in range(6)]
    values = apply_inverse(inverse, sums)
    shared = None
    for number in range(3):
        values_ref[number] = values[number]
        term = values[number] * sums[number]
        shared = term if shared is None else shared + term
    border = column_sums(jnp.where(unshared_rows(), 0.0, shared))
    rows = rows_in[...] + mate_in[3 * SIDE : 3 * SIDE + 6, :]
    rows = rows - jnp.where(sub_iota(6, LANES) == 5, border, 0.0)
    totals = jnp.sum(rows, axis=1, keepdims=True)
    line = column_sums(jnp.where(sub_iota(6, LANES) == lane_iota(6, LANES), totals, 0.0))
    dots_ref[...] = jnp.broadcast_to(line, dots_ref.shape)


def finish_kernel(
    cam_ref, jac_ref, index_ref, errors_in, values_in, given, state_in, tilde_in, dots_ref,
    step_ref, residual_ref, flip_ref,
):
    values = [values_in[number] for number in range(3)]
    image = project(cam_ref, jac_ref, errors_in, values, index_ref[...])
    guess, damp = given[0], given[2]
    scaled, precond = state_in[1], state_in[2]
    first, tilde_residual, tilde = (tilde_in[number] for number in range(3))
    image = damp * tilde + image
    total = column_sums(dots_ref[...])
    inner, curve, tilde_inner, cross, back_inner, tilde_curve = (
        total[:, number : number + 1] for number in range(6)
    )
    mixed = cross - tilde_curve
    back_curve = back_inner - mixed
    first_step = inner / curve
    shift = first_step - 1.0
    inner_next = tilde_inner - 2.0 * shift * cross + shift * shift * back_inner
    curve_next = tilde_curve - 2.0 * shift * mixed + shift * shift * back_curve
    ratio = inner_next / inner
    against = cross - shift * back_inner
    second_step = inner_next / (curve_next + 2.0 * ratio * against + ratio * ratio * curve)
    direction = tilde - shift * (precond * first) + ratio * scaled
    moved = image - shift * (first - image) + ratio * first
    flip_ref[0, :16, :] = guess + first_step * scaled + second_step * direction
    flip_ref[1, :16, :] = tilde_residual - shift * first - second_step * moved
    step_ref[...] = jnp.transpose(flip_ref[0])[:9, :16]
    residual_ref[...] = jnp.transpose(flip_ref[1])[:9, :16]


def vmem(count):
    return [pl.BlockSpec(memory_space=pltpu.VMEM) for _ in range(count)]


def out_f32(*shape):
    return jax.ShapeDtypeStruct(shape, F32)


SEG = ("chip", "core")


def shards(
    cam_jac, point_jac, obs_point, obs_count, back_list, front_list, point_damp, cam_damp,
    right_side, start_guess,
):
    cameras, width = obs_point.shape
    chips = lax.axis_size("chip")
    count = 2 * chips
    mates = [(i, i ^ 1) for i in range(count)]
    others = []
    for i in range(1, count - 1, 2):
        others += [(i, i + 1), (i + 1, i)]
    params = pltpu.CompilerParams(vmem_limit_bytes=16 * 2**20)
    inputs = (
        cam_jac, point_jac, obs_point, obs_count.reshape(1, -1), back_list, front_list,
        point_damp.reshape(-1, LANES), cam_damp.reshape(1, -1), right_side, start_guess,
    )

    def scratch(values):
        return [
            pltpu.VMEM((values, cameras, width), F32),
            pltpu.VMEM((cameras, width), F32),
            pltpu.VMEM((cameras, width), F32),
        ]

    def exchange(to_mate, to_other):
        other = lax.ppermute(to_other, SEG, others)
        mate = lax.ppermute(to_mate, SEG, mates)
        return mate, other

    def call(kernel, name, outs, operands, scratches=(), spaces=None):
        return pl.pallas_call(
            kernel,
            out_shape=outs,
            in_specs=spaces or vmem(len(operands)),
            out_specs=tuple(vmem(len(outs))),
            scratch_shapes=list(scratches),
            compiler_params=params,
            name=name,
        )(*operands)

    plane = out_f32(2, cameras, width)
    to_mate, to_other, own, place, errors, jac, given = call(
        first_kernel,
        "first",
        (
            out_f32(9 * SIDE, LANES),
            out_f32(9 * SIDE, LANES),
            out_f32(9, PAD_ROWS, LANES),
            jax.ShapeDtypeStruct((cameras, width), I32),
            plane,
            out_f32(7, cameras, width),
            out_f32(3, 16, LANES),
        ),
        tuple(pltpu.with_memory_space_constraint(value, pltpu.HBM) for value in inputs),
        scratch(18)
        + [pltpu.VMEM(value.shape, value.dtype) for value in inputs]
        + [pltpu.VMEM((3, LANES, LANES), F32), pltpu.SemaphoreType.DMA((len(inputs),))],
        [pl.BlockSpec(memory_space=pltpu.HBM) for _ in inputs],
    )
    mate, other = exchange(to_mate, to_other)
    (precond,) = call(side_kernel, "side", (out_f32(16, LANES),), (cam_jac, jac, given))
    own_shape = out_f32(3, PAD_ROWS, LANES)
    to_mate, to_other, own, errors, inverse, state = call(
        second_kernel,
        "second",
        (
            out_f32(3 * SIDE, LANES),
            out_f32(3 * SIDE, LANES),
            own_shape,
            plane,
            out_f32(6, PAD_ROWS, LANES),
            out_f32(3, 16, LANES),
        ),
        (cam_jac, jac, place, errors, own, mate, other, given, precond),
        scratch(6),
    )
    mate, other = exchange(to_mate, to_other)
    to_mate, to_other, own, errors, tilde, rows = call(
        third_kernel,
        "third",
        (
            out_f32(3 * SIDE + 6, LANES),
            out_f32(3 * SIDE, LANES),
            own_shape,
            plane,
            out_f32(3, 16, LANES),
            out_f32(6, LANES),
        ),
        (cam_jac, jac, place, errors, own, mate, other, inverse, given, state),
        scratch(6),
    )
    mate, other = exchange(to_mate, to_other)
    values, dots = call(
        sum_kernel,
        "sum",
        (own_shape, out_f32(chips, LANES)),
        (own, mate, other, inverse, rows),
    )
    dots = lax.all_to_all(dots, "chip", 0, 0, tiled=True)
    return call(
        finish_kernel,
        "finish",
        (out_f32(9, 16), out_f32(9, 16)),
        (cam_jac, jac, place, errors, values, given, state, tilde, dots),
        [pltpu.VMEM((2, LANES, LANES), F32)],
    )


def solution(mesh):
    finer = Mesh(mesh.devices.reshape(-1, 2), SEG)
    return jax.shard_map(
        shards,
        mesh=finer,
        in_specs=(
            P(None, SEG, None),
            P(None, SEG, None),
            P(SEG, None),
            P(SEG),
            P(SEG, None),
            P(SEG, None),
            P(SEG),
            P(SEG),
            P(None, SEG),
            P(None, SEG),
        ),
        out_specs=(P(None, SEG), P(None, SEG)),
        check_vma=False,
    )
```

```python
import jax
import jax.numpy as jnp
from jax import lax
from jax.experimental import pallas as pl
from jax.experimental.pallas import tpu as pltpu
from jax.sharding import Mesh
from jax.sharding import PartitionSpec as P

F32 = jnp.float32
BF16 = jnp.bfloat16
I32 = jnp.int32
LANES = 128
ENTRY_PAIRS = ((0, 0), (0, 1), (0, 2), (1, 1), (1, 2), (2, 2))

SIDE = 6
LIST_ROWS = 3
NEXT_SLOTS = 3
PREV_SLOTS = 6
OWN_FRONT = 9
INTERIOR = 12
ROWS = 14
PAD_ROWS = 16


def row_of(block, index, rows):
    return jnp.broadcast_to(block[index : index + 1, :], (rows, block.shape[1]))


def sub_iota(rows, width):
    return lax.broadcasted_iota(I32, (rows, width), 0)


def lane_iota(rows, width):
    return lax.broadcasted_iota(I32, (rows, width), 1)


def nt(left, right, **kw):
    return lax.dot_general(
        left, right, (((1,), (1,)), ((), ())), preferred_element_type=F32, **kw
    )


def split_two(value):
    high = value.astype(BF16)
    low = (value - high.astype(F32)).astype(BF16)
    return high.astype(F32), low.astype(F32)


def flip_block(block_ref):
    return jnp.transpose(block_ref[...])[:16]


def one_hot_rows(index_row, rows, width):
    packed = jnp.broadcast_to(index_row, (16, width)).astype(BF16)
    parts = []
    for start in range(0, rows, 16):
        ids = (sub_iota(16, width) + start).astype(F32).astype(BF16)
        parts.append(jnp.where(packed == ids, jnp.ones_like(packed), jnp.zeros_like(packed)))
    return parts[0] if len(parts) == 1 else jnp.concatenate(parts, axis=0)


def scatter_rows(value_refs, high_ref, low_ref, cameras, width, group):
    ids = sub_iota(16, width).astype(F32).astype(BF16)

    def step(number, total):
        for inner in range(group):
            pick = pl.ds(number * group + inner, 1)
            lanes = one_hot_rows(low_ref[pick, :], LANES, width).astype(jnp.float8_e4m3fn)
            mask = jnp.broadcast_to(high_ref[pick, :], (16, width)).astype(BF16) == ids
            rows = []
            for ref, index in value_refs:
                spread = jnp.broadcast_to(ref[index, pick, :], (16, width)).astype(BF16)
                rows.append(jnp.where(mask, spread, jnp.zeros_like(spread)))
            piece = nt(jnp.concatenate(rows, axis=0), lanes)
            total = piece if total is None else total + piece
        return total

    if group == cameras:
        return step(0, None)
    start = jnp.zeros((16 * len(value_refs), LANES), F32)
    return lax.fori_loop(0, cameras // group, step, start)


def fold_parts(total, index):
    start = 2 * PAD_ROWS * index
    return total[start : start + PAD_ROWS] + total[start + PAD_ROWS : start + 2 * PAD_ROWS]


def gather_rows(tables, row_index, lane_index, rows):
    halves = []
    for top in range(0, row_index.shape[0], 8):
        pieces = []
        for start in range(0, row_index.shape[1], LANES):
            row_part = row_index[top : top + 8, start : start + LANES]
            lane_part = lane_index[top : top + 8, start : start + LANES]
            outs = [None] * len(tables)
            for row in range(rows):
                here = row_part == row
                for number, table in enumerate(tables):
                    spread = jnp.broadcast_to(table[row : row + 1, :], (8, LANES))
                    got = jnp.take_along_axis(spread, lane_part, axis=1, mode="promise_in_bounds")
                    outs[number] = got if row == 0 else jnp.where(here, got, outs[number])
            pieces.append(outs)
        halves.append([jnp.concatenate([p[n] for p in pieces], axis=1) for n in range(len(tables))])
    return [jnp.concatenate([h[n] for h in halves], axis=0) for n in range(len(tables))]


def errors_of(cam_ref, vector, weights):
    rows = []
    for row in range(2):
        running = None
        for column in range(9):
            term = cam_ref[9 * row + column].astype(F32) * vector[:, column : column + 1]
            running = term if running is None else running + term
        rows.append(running * weights)
    return rows


def send_rows(mate_ref, other_ref, index, block):
    odd = lax.axis_index("core") == 1
    to_next = block[:SIDE]
    to_prev = block[SIDE : 2 * SIDE]
    mate_ref[SIDE * index : SIDE * (index + 1), :] = jnp.where(odd, to_prev, to_next)
    other_ref[SIDE * index : SIDE * (index + 1), :] = jnp.where(odd, to_next, to_prev)


def point_table(back, front):
    border = back.shape[1]
    eight = sub_iota(8, border)
    lanes = lane_iota(8, border)
    lefts, rights = [], []
    for listed, base in ((back, 0), (front, OWN_FRONT)):
        high = listed >> 7
        low = listed & 127
        hit = jnp.broadcast_to(high, (8, border)) == eight
        row_value = ((lanes >> 7) + (base + 1)).astype(F32)
        lane_value = (lanes & 127).astype(F32)
        zero = jnp.zeros((8, border), F32)
        lefts.append(
            jnp.concatenate(
                [jnp.where(hit, row_value, zero), jnp.where(hit, lane_value, zero)], axis=0
            ).astype(BF16)
        )
        rights.append(one_hot_rows(low.astype(F32), LANES, border))
    table = nt(lefts[0], rights[0]) + nt(lefts[1], rights[1])
    row_plus = table[:8]
    lane = table[8:]
    free = jnp.where(row_plus == 0.0, 1.0, 0.0)
    upper = jnp.where(sub_iota(LANES, LANES) <= lane_iota(LANES, LANES), 1.0, 0.0).astype(BF16)
    seen = lax.dot_general(
        free.astype(BF16), upper, (((1,), (0,)), ((), ())), preferred_element_type=F32
    )
    total = jnp.broadcast_to(seen[:, LANES - 1 : LANES], (8, LANES))
    before = jnp.zeros((8, LANES), F32)
    rows = sub_iota(8, LANES)
    for row in range(7):
        before = before + jnp.where(rows > row, row_of(total, row, 8), 0.0)
    rank = before + seen - free
    return jnp.where(
        free > 0.0, rank + float(INTERIOR * LANES), (row_plus - 1.0) * float(LANES) + lane
    ).astype(I32)


def first_kernel(
    cam_hbm, point_hbm, obs_hbm, count_hbm, back_hbm, front_hbm, damp_hbm, cam_damp_hbm,
    right_hbm, guess_hbm,
    mate_ref, other_ref, own_ref, index_ref, errors_ref, jac_ref, state_ref, cam_ref,
    value_ref, high_ref, low_ref,
    point_ref, obs_ref, count_ref, back_ref, front_ref, damp_ref, cam_damp_ref,
    right_ref, guess_ref, flip_ref, sems,
):
    sources = (
        back_hbm, front_hbm, obs_hbm, guess_hbm, right_hbm, cam_damp_hbm, count_hbm, point_hbm,
        cam_hbm, damp_hbm,
    )
    targets = (
        back_ref, front_ref, obs_ref, guess_ref, right_ref, cam_damp_ref, count_ref, point_ref,
        cam_ref, damp_ref,
    )
    copies = [
        pltpu.make_async_copy(source, target, sems.at[number])
        for number, (source, target) in enumerate(zip(sources, targets))
    ]
    for copy in copies:
        copy.start()
    cameras, width = obs_ref.shape
    border = back_ref.shape[1]
    points = damp_ref.shape[0] * damp_ref.shape[1]
    for copy in copies[:8]:
        copy.wait()
    table = point_table(back_ref[...], front_ref[...])
    observed = obs_ref[...]
    own_place = gather_rows([table], observed >> 7, observed & 127, points // LANES)[0]
    place = jnp.where(
        observed < points,
        own_place,
        jnp.where(
            observed < points + border,
            observed + (PREV_SLOTS * LANES - points),
            observed + (NEXT_SLOTS * LANES - points - border),
        ),
    )
    index_ref[...] = place
    high_ref[...] = (place >> 7).astype(F32)
    low_ref[...] = (place & 127).astype(F32)
    valid = lane_iota(16, LANES) < 9
    flip_ref[0, :9, :16] = guess_ref[...]
    flip_ref[1, :9, :16] = right_ref[...]
    flip_ref[2, 0:1, :16] = cam_damp_ref[...]
    flip_ref[2, 1:2, :16] = count_ref[...].astype(F32)
    guess = jnp.where(valid, flip_block(flip_ref.at[0]), 0.0)
    right = jnp.where(valid, flip_block(flip_ref.at[1]), 0.0)
    sides = flip_block(flip_ref.at[2])
    damp = jnp.where(valid, sides[:, 0:1], 0.0)
    weights = (lane_iota(cameras, width).astype(F32) < sides[:, 1:2]).astype(F32)
    state_ref[0] = guess
    state_ref[1] = right
    state_ref[2] = damp
    jac = [point_ref[entry].astype(F32) * weights for entry in range(6)]
    for entry in range(6):
        jac_ref[entry] = jac[entry]
    jac_ref[6] = weights
    products = [jac[a] * jac[b] + jac[3 + a] * jac[3 + b] for a, b in ENTRY_PAIRS]
    copies[8].wait()
    copies[9].wait()
    errors = errors_of(cam_ref, guess, weights)
    errors_ref[0] = errors[0]
    errors_ref[1] = errors[1]
    products += [errors[0] * jac[j] + errors[1] * jac[3 + j] for j in range(3)]
    for number, product in enumerate(products):
        value_ref[2 * number], value_ref[2 * number + 1] = split_two(product)
    total = scatter_rows(
        [(value_ref, number) for number in range(18)], high_ref, low_ref, cameras, width, 8
    )
    ids = sub_iota(16, LANES).astype(F32).astype(BF16)
    damping = None
    new_high = (table >> 7).astype(F32)
    new_low = (table & 127).astype(F32)
    first, rest = split_two(damp_ref[...])
    last = damp_ref[...] - first - rest
    for row in range(points // LANES):
        lanes = one_hot_rows(new_low[row : row + 1, :], LANES, LANES)
        mask = row_of(new_high, row, 16).astype(BF16) == ids
        parts = []
        for part in (first, rest, last):
            spread = row_of(part, row, 16).astype(BF16)
            parts.append(jnp.where(mask, spread, jnp.zeros_like(spread)))
        piece = nt(jnp.concatenate(parts, axis=0), lanes)
        damping = piece if damping is None else damping + piece
    damping = damping[:16] + damping[16:32] + damping[32:]
    for number in range(9):
        block = fold_parts(total, number)
        if number in (0, 3, 5):
            block = block + damping
        own_ref[number] = block
        send_rows(mate_ref, other_ref, number, block)


def complete(own_ref, mate_ref, other_ref, number):
    odd = lax.axis_index("core") == 1
    block = own_ref[number]
    mate = mate_ref[SIDE * number : SIDE * (number + 1), :]
    other = other_ref[SIDE * number : SIDE * (number + 1), :]
    after = jnp.where(odd, other, mate)
    before = jnp.where(odd, mate, other)
    tail = jnp.zeros((PAD_ROWS - 2 * SIDE, LANES), F32)
    return block + jnp.concatenate([after, before, tail], axis=0)


def symmetric_inverse(entries):
    cofactors = [
        entries[3] * entries[5] - entries[4] * entries[4],
        entries[2] * entries[4] - entries[1] * entries[5],
        entries[1] * entries[4] - entries[2] * entries[3],
        entries[0] * entries[5] - entries[2] * entries[2],
        entries[1] * entries[2] - entries[0] * entries[4],
        entries[0] * entries[3] - entries[1] * entries[1],
    ]
    determinant = entries[0] * cofactors[0] + entries[1] * cofactors[1] + entries[2] * cofactors[2]
    determinant = jnp.where(determinant == 0.0, 1.0, determinant)
    return [member / determinant for member in cofactors]


def apply_inverse(inverse, sums):
    return [
        inverse[0] * sums[0] + inverse[1] * sums[1] + inverse[2] * sums[2],
        inverse[1] * sums[0] + inverse[3] * sums[1] + inverse[4] * sums[2],
        inverse[2] * sums[0] + inverse[4] * sums[1] + inverse[5] * sums[2],
    ]


def pack_columns(cols):
    lanes = lane_iota(16, LANES)
    out = jnp.zeros((16, LANES), F32)
    for number, col in enumerate(cols):
        out = jnp.where(lanes == number, col, out)
    return out


def project(cam_ref, jac_ref, errors_ref, values, place):
    high = place >> 7
    low = place & 127
    picked = gather_rows(values, high, low, ROWS)
    adjusted = []
    for row in range(2):
        back = (
            picked[0] * jac_ref[3 * row]
            + picked[1] * jac_ref[3 * row + 1]
            + picked[2] * jac_ref[3 * row + 2]
        )
        adjusted.append(errors_ref[row] - back)
    cols = []
    for column in range(9):
        term = (
            cam_ref[column].astype(F32) * adjusted[0]
            + cam_ref[9 + column].astype(F32) * adjusted[1]
        )
        cols.append(jnp.sum(term, axis=1, keepdims=True))
    return pack_columns(cols)


def next_scatter(
    cam_ref, jac_ref, vector, place, value_ref, high_ref, low_ref,
    mate_ref, other_ref, own_ref, errors_ref,
):
    cameras, width = place.shape
    errors = errors_of(cam_ref, vector, jac_ref[6])
    errors_ref[0] = errors[0]
    errors_ref[1] = errors[1]
    for j in range(3):
        product = errors[0] * jac_ref[j] + errors[1] * jac_ref[3 + j]
        value_ref[2 * j], value_ref[2 * j + 1] = split_two(product)
    high_ref[...] = (place >> 7).astype(F32)
    low_ref[...] = (place & 127).astype(F32)
    total = scatter_rows(
        [(value_ref, number) for number in range(6)], high_ref, low_ref, cameras, width, 8
    )
    blocks = []
    for number in range(3):
        block = fold_parts(total, number)
        own_ref[number] = block
        send_rows(mate_ref, other_ref, number, block)
        blocks.append(block)
    return errors, blocks


def side_kernel(cam_ref, jac_ref, given, precond_ref):
    cols = []
    for column in range(9):
        squared = cam_ref[column].astype(F32) ** 2 + cam_ref[9 + column].astype(F32) ** 2
        cols.append(jnp.sum(squared * jac_ref[6], axis=1, keepdims=True))
    valid = lane_iota(16, LANES) < 9
    precond_ref[...] = jnp.where(valid, 1.0 / (pack_columns(cols) + given[2]), 0.0)


def second_kernel(
    cam_ref, jac_ref, index_ref, errors_in, own_in, mate_in, other_in, state_in, precond_in,
    mate_ref, other_ref, own_ref, errors_ref, inverse_ref, state_ref,
    value_ref, high_ref, low_ref,
):
    blocks = [complete(own_in, mate_in, other_in, number) for number in range(9)]
    inverse = symmetric_inverse(blocks[:6])
    for number in range(6):
        inverse_ref[number] = inverse[number]
    place = index_ref[...]
    values = apply_inverse(inverse, blocks[6:])
    image = project(cam_ref, jac_ref, errors_in, values, place)
    guess, right, damp = state_in[0], state_in[1], state_in[2]
    precond = precond_in[...]
    residual = right - (damp * guess + image)
    scaled = precond * residual
    state_ref[0] = residual
    state_ref[1] = scaled
    state_ref[2] = precond
    next_scatter(
        cam_ref, jac_ref, scaled, place, value_ref, high_ref, low_ref,
        mate_ref, other_ref, own_ref, errors_ref,
    )


def unshared_rows():
    chip = lax.axis_index("chip")
    core = lax.axis_index("core")
    first = jnp.logical_and(chip == 0, core == 0)
    last = jnp.logical_and(chip == lax.axis_size("chip") - 1, core == 1)
    start = jnp.where(first, SIDE, INTERIOR)
    stop = jnp.where(last, SIDE, 0)
    rows = sub_iota(PAD_ROWS, LANES)
    return jnp.logical_or(rows >= start, rows < stop)


def column_sums(block):
    return jnp.sum(block, axis=0, keepdims=True)


def third_kernel(
    cam_ref, jac_ref, index_ref, errors_in, own_in, mate_in, other_in, inverse_in, given, state_in,
    mate_ref, other_ref, own_ref, errors_ref, state_ref, rows_ref,
    value_ref, high_ref, low_ref,
):
    sums = [complete(own_in, mate_in, other_in, number) for number in range(3)]
    inverse = [inverse_in[number] for number in range(6)]
    values = apply_inverse(inverse, sums)
    place = index_ref[...]
    image = project(cam_ref, jac_ref, errors_in, values, place)
    damp = given[2]
    residual, scaled, precond = state_in[0], state_in[1], state_in[2]
    image = damp * scaled + image
    tilde_residual = residual - image
    tilde = precond * tilde_residual
    state_ref[0] = image
    state_ref[1] = tilde_residual
    state_ref[2] = tilde
    errors, blocks = next_scatter(
        cam_ref, jac_ref, tilde, place, value_ref, high_ref, low_ref,
        mate_ref, other_ref, own_ref, errors_ref,
    )
    energy = column_sums(damp * tilde * tilde)
    squares = column_sums(errors[0] * errors[0] + errors[1] * errors[1])
    for start in range(0, squares.shape[1], LANES):
        energy = energy + squares[:, start : start + LANES]
    lone = unshared_rows()
    for value, point in zip(apply_inverse(inverse, blocks), blocks):
        energy = energy - column_sums(jnp.where(lone, value * point, 0.0))
    rows = [
        column_sums(residual * scaled),
        column_sums(image * scaled),
        column_sums(tilde_residual * tilde),
        column_sums(image * tilde),
        column_sums(image * (precond * image)),
        energy,
    ]
    for number, row in enumerate(rows):
        rows_ref[number : number + 1, :] = row
        mate_ref[3 * SIDE + number : 3 * SIDE + number + 1, :] = row


def sum_kernel(own_in, mate_in, other_in, inverse_in, rows_in, values_ref, dots_ref):
    sums = [complete(own_in, mate_in, other_in, number) for number in range(3)]
    inverse = [inverse_in[number] for number in range(6)]
    values = apply_inverse(inverse, sums)
    shared = None
    for number in range(3):
        values_ref[number] = values[number]
        term = values[number] * sums[number]
        shared = term if shared is None else shared + term
    border = column_sums(jnp.where(unshared_rows(), 0.0, shared))
    rows = rows_in[...] + mate_in[3 * SIDE : 3 * SIDE + 6, :]
    rows = rows - jnp.where(sub_iota(6, LANES) == 5, border, 0.0)
    totals = jnp.sum(rows, axis=1, keepdims=True)
    line = column_sums(jnp.where(sub_iota(6, LANES) == lane_iota(6, LANES), totals, 0.0))
    dots_ref[...] = jnp.broadcast_to(line, dots_ref.shape)


def finish_kernel(
    cam_ref, jac_ref, index_ref, errors_in, values_in, given, state_in, tilde_in, dots_ref,
    step_ref, residual_ref, flip_ref,
):
    values = [values_in[number] for number in range(3)]
    image = project(cam_ref, jac_ref, errors_in, values, index_ref[...])
    guess, damp = given[0], given[2]
    scaled, precond = state_in[1], state_in[2]
    first, tilde_residual, tilde = (tilde_in[number] for number in range(3))
    image = damp * tilde + image
    total = column_sums(dots_ref[...])
    inner, curve, tilde_inner, cross, back_inner, tilde_curve = (
        total[:, number : number + 1] for number in range(6)
    )
    mixed = cross - tilde_curve
    back_curve = back_inner - mixed
    first_step = inner / curve
    shift = first_step - 1.0
    inner_next = tilde_inner - 2.0 * shift * cross + shift * shift * back_inner
    curve_next = tilde_curve - 2.0 * shift * mixed + shift * shift * back_curve
    ratio = inner_next / inner
    against = cross - shift * back_inner
    second_step = inner_next / (curve_next + 2.0 * ratio * against + ratio * ratio * curve)
    direction = tilde - shift * (precond * first) + ratio * scaled
    moved = image - shift * (first - image) + ratio * first
    flip_ref[0, :16, :] = guess + first_step * scaled + second_step * direction
    flip_ref[1, :16, :] = tilde_residual - shift * first - second_step * moved
    step_ref[...] = jnp.transpose(flip_ref[0])[:9, :16]
    residual_ref[...] = jnp.transpose(flip_ref[1])[:9, :16]


def vmem(count):
    return [pl.BlockSpec(memory_space=pltpu.VMEM) for _ in range(count)]


def out_f32(*shape):
    return jax.ShapeDtypeStruct(shape, F32)


SEG = ("chip", "core")


def shards(
    cam_jac, point_jac, obs_point, obs_count, back_list, front_list, point_damp, cam_damp,
    right_side, start_guess,
):
    cameras, width = obs_point.shape
    chips = lax.axis_size("chip")
    count = 2 * chips
    mates = [(i, i ^ 1) for i in range(count)]
    others = []
    for i in range(1, count - 1, 2):
        others += [(i, i + 1), (i + 1, i)]
    params = pltpu.CompilerParams(vmem_limit_bytes=16 * 2**20)
    inputs = (
        cam_jac, point_jac, obs_point, obs_count.reshape(1, -1), back_list, front_list,
        point_damp.reshape(-1, LANES), cam_damp.reshape(1, -1), right_side, start_guess,
    )

    def scratch(values):
        return [
            pltpu.VMEM((values, cameras, width), F32),
            pltpu.VMEM((cameras, width), F32),
            pltpu.VMEM((cameras, width), F32),
        ]

    def exchange(to_mate, to_other):
        other = lax.ppermute(to_other, SEG, others)
        mate = lax.ppermute(to_mate, SEG, mates)
        return mate, other

    def call(kernel, name, outs, operands, scratches=(), spaces=None):
        return pl.pallas_call(
            kernel,
            out_shape=outs,
            in_specs=spaces or vmem(len(operands)),
            out_specs=tuple(vmem(len(outs))),
            scratch_shapes=list(scratches),
            compiler_params=params,
            name=name,
        )(*operands)

    plane = out_f32(2, cameras, width)
    to_mate, to_other, own, place, errors, jac, given, cam_jac = call(
        first_kernel,
        "first",
        (
            out_f32(9 * SIDE, LANES),
            out_f32(9 * SIDE, LANES),
            out_f32(9, PAD_ROWS, LANES),
            jax.ShapeDtypeStruct((cameras, width), I32),
            plane,
            out_f32(7, cameras, width),
            out_f32(3, 16, LANES),
            jax.ShapeDtypeStruct(cam_jac.shape, cam_jac.dtype),
        ),
        tuple(pltpu.with_memory_space_constraint(value, pltpu.HBM) for value in inputs),
        scratch(18)
        + [pltpu.VMEM(value.shape, value.dtype) for value in inputs[1:]]
        + [pltpu.VMEM((3, LANES, LANES), F32), pltpu.SemaphoreType.DMA((len(inputs),))],
        [pl.BlockSpec(memory_space=pltpu.HBM) for _ in inputs],
    )
    mate, other = exchange(to_mate, to_other)
    (precond,) = call(side_kernel, "side", (out_f32(16, LANES),), (cam_jac, jac, given))
    own_shape = out_f32(3, PAD_ROWS, LANES)
    to_mate, to_other, own, errors, inverse, state = call(
        second_kernel,
        "second",
        (
            out_f32(3 * SIDE, LANES),
            out_f32(3 * SIDE, LANES),
            own_shape,
            plane,
            out_f32(6, PAD_ROWS, LANES),
            out_f32(3, 16, LANES),
        ),
        (cam_jac, jac, place, errors, own, mate, other, given, precond),
        scratch(6),
    )
    mate, other = exchange(to_mate, to_other)
    to_mate, to_other, own, errors, tilde, rows = call(
        third_kernel,
        "third",
        (
            out_f32(3 * SIDE + 6, LANES),
            out_f32(3 * SIDE, LANES),
            own_shape,
            plane,
            out_f32(3, 16, LANES),
            out_f32(6, LANES),
        ),
        (cam_jac, jac, place, errors, own, mate, other, inverse, given, state),
        scratch(6),
    )
    mate, other = exchange(to_mate, to_other)
    values, dots = call(
        sum_kernel,
        "sum",
        (own_shape, out_f32(chips, LANES)),
        (own, mate, other, inverse, rows),
    )
    dots = lax.all_to_all(dots, "chip", 0, 0, tiled=True)
    return call(
        finish_kernel,
        "finish",
        (out_f32(9, 16), out_f32(9, 16)),
        (cam_jac, jac, place, errors, values, given, state, tilde, dots),
        [pltpu.VMEM((2, LANES, LANES), F32)],
    )


def solution(mesh):
    finer = Mesh(mesh.devices.reshape(-1, 2), SEG)
    return jax.shard_map(
        shards,
        mesh=finer,
        in_specs=(
            P(None, SEG, None),
            P(None, SEG, None),
            P(SEG, None),
            P(SEG),
            P(SEG, None),
            P(SEG, None),
            P(SEG),
            P(SEG),
            P(None, SEG),
            P(None, SEG),
        ),
        out_specs=(P(None, SEG), P(None, SEG)),
        check_vma=False,
    )
```

```python
import jax
import jax.numpy as jnp
from jax import lax
from jax.experimental import pallas as pl
from jax.experimental.pallas import tpu as pltpu
from jax.sharding import Mesh
from jax.sharding import PartitionSpec as P

F32 = jnp.float32
BF16 = jnp.bfloat16
I32 = jnp.int32
LANES = 128
ENTRY_PAIRS = ((0, 0), (0, 1), (0, 2), (1, 1), (1, 2), (2, 2))

SIDE = 6
LIST_ROWS = 3
NEXT_SLOTS = 3
PREV_SLOTS = 6
OWN_FRONT = 9
INTERIOR = 12
ROWS = 14
PAD_ROWS = 16


def row_of(block, index, rows):
    return jnp.broadcast_to(block[index : index + 1, :], (rows, block.shape[1]))


def sub_iota(rows, width):
    return lax.broadcasted_iota(I32, (rows, width), 0)


def lane_iota(rows, width):
    return lax.broadcasted_iota(I32, (rows, width), 1)


def nt(left, right, **kw):
    return lax.dot_general(
        left, right, (((1,), (1,)), ((), ())), preferred_element_type=F32, **kw
    )


def split_two(value):
    high = value.astype(BF16)
    low = (value - high.astype(F32)).astype(BF16)
    return high.astype(F32), low.astype(F32)


def flip_block(block_ref):
    return jnp.transpose(block_ref[...])[:16]


def one_hot_rows(index_row, rows, width):
    packed = jnp.broadcast_to(index_row, (16, width)).astype(BF16)
    parts = []
    for start in range(0, rows, 16):
        ids = (sub_iota(16, width) + start).astype(F32).astype(BF16)
        parts.append(jnp.where(packed == ids, jnp.ones_like(packed), jnp.zeros_like(packed)))
    return parts[0] if len(parts) == 1 else jnp.concatenate(parts, axis=0)


def scatter_rows(value_refs, high_ref, low_ref, cameras, width, group):
    ids = sub_iota(16, width).astype(F32).astype(BF16)

    def step(number, total):
        for inner in range(group):
            pick = pl.ds(number * group + inner, 1)
            lanes = one_hot_rows(low_ref[pick, :], LANES, width).astype(jnp.float8_e4m3fn)
            mask = jnp.broadcast_to(high_ref[pick, :], (16, width)).astype(BF16) == ids
            rows = []
            for ref, index in value_refs:
                spread = jnp.broadcast_to(ref[index, pick, :], (16, width)).astype(BF16)
                rows.append(jnp.where(mask, spread, jnp.zeros_like(spread)))
            piece = nt(jnp.concatenate(rows, axis=0), lanes)
            total = piece if total is None else total + piece
        return total

    if group == cameras:
        return step(0, None)
    start = jnp.zeros((16 * len(value_refs), LANES), F32)
    return lax.fori_loop(0, cameras // group, step, start)


def fold_parts(total, index):
    start = 2 * PAD_ROWS * index
    return total[start : start + PAD_ROWS] + total[start + PAD_ROWS : start + 2 * PAD_ROWS]


def gather_rows(tables, row_index, lane_index, rows):
    halves = []
    for top in range(0, row_index.shape[0], 8):
        pieces = []
        for start in range(0, row_index.shape[1], LANES):
            row_part = row_index[top : top + 8, start : start + LANES]
            lane_part = lane_index[top : top + 8, start : start + LANES]
            outs = [None] * len(tables)
            for row in range(rows):
                here = row_part == row
                for number, table in enumerate(tables):
                    spread = jnp.broadcast_to(table[row : row + 1, :], (8, LANES))
                    got = jnp.take_along_axis(spread, lane_part, axis=1, mode="promise_in_bounds")
                    outs[number] = got if row == 0 else jnp.where(here, got, outs[number])
            pieces.append(outs)
        halves.append([jnp.concatenate([p[n] for p in pieces], axis=1) for n in range(len(tables))])
    return [jnp.concatenate([h[n] for h in halves], axis=0) for n in range(len(tables))]


def errors_of(cam_ref, vector, weights):
    rows = []
    for row in range(2):
        running = None
        for column in range(9):
            term = cam_ref[9 * row + column].astype(F32) * vector[:, column : column + 1]
            running = term if running is None else running + term
        rows.append(running * weights)
    return rows


def send_rows(mate_ref, other_ref, index, block):
    odd = lax.axis_index("core") == 1
    to_next = block[:SIDE]
    to_prev = block[SIDE : 2 * SIDE]
    mate_ref[SIDE * index : SIDE * (index + 1), :] = jnp.where(odd, to_prev, to_next)
    other_ref[SIDE * index : SIDE * (index + 1), :] = jnp.where(odd, to_next, to_prev)


def point_table(back, front):
    border = back.shape[1]
    eight = sub_iota(8, border)
    lanes = lane_iota(8, border)
    lefts, rights = [], []
    for listed, base in ((back, 0), (front, OWN_FRONT)):
        high = listed >> 7
        low = listed & 127
        hit = jnp.broadcast_to(high, (8, border)) == eight
        row_value = ((lanes >> 7) + (base + 1)).astype(F32)
        lane_value = (lanes & 127).astype(F32)
        zero = jnp.zeros((8, border), F32)
        lefts.append(
            jnp.concatenate(
                [jnp.where(hit, row_value, zero), jnp.where(hit, lane_value, zero)], axis=0
            ).astype(BF16)
        )
        rights.append(one_hot_rows(low.astype(F32), LANES, border))
    table = nt(lefts[0], rights[0]) + nt(lefts[1], rights[1])
    row_plus = table[:8]
    lane = table[8:]
    free = jnp.where(row_plus == 0.0, 1.0, 0.0)
    upper = jnp.where(sub_iota(LANES, LANES) <= lane_iota(LANES, LANES), 1.0, 0.0).astype(BF16)
    seen = lax.dot_general(
        free.astype(BF16), upper, (((1,), (0,)), ((), ())), preferred_element_type=F32
    )
    total = jnp.broadcast_to(seen[:, LANES - 1 : LANES], (8, LANES))
    before = jnp.zeros((8, LANES), F32)
    rows = sub_iota(8, LANES)
    for row in range(7):
        before = before + jnp.where(rows > row, row_of(total, row, 8), 0.0)
    rank = before + seen - free
    return jnp.where(
        free > 0.0, rank + float(INTERIOR * LANES), (row_plus - 1.0) * float(LANES) + lane
    ).astype(I32)


def first_kernel(
    cam_hbm, point_hbm, obs_hbm, count_hbm, back_hbm, front_hbm, damp_hbm, cam_damp_hbm,
    right_hbm, guess_hbm,
    mate_ref, other_ref, own_ref, index_ref, errors_ref, jac_ref, state_ref, cam_ref,
    value_ref, high_ref, low_ref,
    point_ref, obs_ref, count_ref, back_ref, front_ref, damp_ref, cam_damp_ref,
    right_ref, guess_ref, flip_ref, sems,
):
    sources = (
        back_hbm, front_hbm, obs_hbm, guess_hbm, right_hbm, cam_damp_hbm, count_hbm, point_hbm,
        cam_hbm, damp_hbm,
    )
    targets = (
        back_ref, front_ref, obs_ref, guess_ref, right_ref, cam_damp_ref, count_ref, point_ref,
        cam_ref, damp_ref,
    )
    copies = [
        pltpu.make_async_copy(source, target, sems.at[number])
        for number, (source, target) in enumerate(zip(sources, targets))
    ]
    for copy in copies:
        copy.start()
    cameras, width = obs_ref.shape
    border = back_ref.shape[1]
    points = damp_ref.shape[0] * damp_ref.shape[1]
    for copy in copies[:2]:
        copy.wait()
    table = point_table(back_ref[...], front_ref[...])
    copies[2].wait()
    observed = obs_ref[...]
    own_place = gather_rows([table], observed >> 7, observed & 127, points // LANES)[0]
    place = jnp.where(
        observed < points,
        own_place,
        jnp.where(
            observed < points + border,
            observed + (PREV_SLOTS * LANES - points),
            observed + (NEXT_SLOTS * LANES - points - border),
        ),
    )
    index_ref[...] = place
    high_ref[...] = (place >> 7).astype(F32)
    low_ref[...] = (place & 127).astype(F32)
    valid = lane_iota(16, LANES) < 9
    for copy in copies[3:7]:
        copy.wait()
    flip_ref[0, :9, :16] = guess_ref[...]
    flip_ref[1, :9, :16] = right_ref[...]
    flip_ref[2, 0:1, :16] = cam_damp_ref[...]
    flip_ref[2, 1:2, :16] = count_ref[...].astype(F32)
    guess = jnp.where(valid, flip_block(flip_ref.at[0]), 0.0)
    right = jnp.where(valid, flip_block(flip_ref.at[1]), 0.0)
    sides = flip_block(flip_ref.at[2])
    damp = jnp.where(valid, sides[:, 0:1], 0.0)
    weights = (lane_iota(cameras, width).astype(F32) < sides[:, 1:2]).astype(F32)
    state_ref[0] = guess
    state_ref[1] = right
    state_ref[2] = damp
    copies[7].wait()
    jac = [point_ref[entry].astype(F32) * weights for entry in range(6)]
    for entry in range(6):
        jac_ref[entry] = jac[entry]
    jac_ref[6] = weights
    products = [jac[a] * jac[b] + jac[3 + a] * jac[3 + b] for a, b in ENTRY_PAIRS]
    copies[8].wait()
    copies[9].wait()
    errors = errors_of(cam_ref, guess, weights)
    errors_ref[0] = errors[0]
    errors_ref[1] = errors[1]
    products += [errors[0] * jac[j] + errors[1] * jac[3 + j] for j in range(3)]
    for number, product in enumerate(products):
        value_ref[2 * number], value_ref[2 * number + 1] = split_two(product)
    total = scatter_rows(
        [(value_ref, number) for number in range(18)], high_ref, low_ref, cameras, width, 8
    )
    ids = sub_iota(16, LANES).astype(F32).astype(BF16)
    damping = None
    new_high = (table >> 7).astype(F32)
    new_low = (table & 127).astype(F32)
    first, rest = split_two(damp_ref[...])
    last = damp_ref[...] - first - rest
    for row in range(points // LANES):
        lanes = one_hot_rows(new_low[row : row + 1, :], LANES, LANES)
        mask = row_of(new_high, row, 16).astype(BF16) == ids
        parts = []
        for part in (first, rest, last):
            spread = row_of(part, row, 16).astype(BF16)
            parts.append(jnp.where(mask, spread, jnp.zeros_like(spread)))
        piece = nt(jnp.concatenate(parts, axis=0), lanes)
        damping = piece if damping is None else damping + piece
    damping = damping[:16] + damping[16:32] + damping[32:]
    for number in range(9):
        block = fold_parts(total, number)
        if number in (0, 3, 5):
            block = block + damping
        own_ref[number] = block
        send_rows(mate_ref, other_ref, number, block)


def complete(own_ref, mate_ref, other_ref, number):
    odd = lax.axis_index("core") == 1
    block = own_ref[number]
    mate = mate_ref[SIDE * number : SIDE * (number + 1), :]
    other = other_ref[SIDE * number : SIDE * (number + 1), :]
    after = jnp.where(odd, other, mate)
    before = jnp.where(odd, mate, other)
    tail = jnp.zeros((PAD_ROWS - 2 * SIDE, LANES), F32)
    return block + jnp.concatenate([after, before, tail], axis=0)


def symmetric_inverse(entries):
    cofactors = [
        entries[3] * entries[5] - entries[4] * entries[4],
        entries[2] * entries[4] - entries[1] * entries[5],
        entries[1] * entries[4] - entries[2] * entries[3],
        entries[0] * entries[5] - entries[2] * entries[2],
        entries[1] * entries[2] - entries[0] * entries[4],
        entries[0] * entries[3] - entries[1] * entries[1],
    ]
    determinant = entries[0] * cofactors[0] + entries[1] * cofactors[1] + entries[2] * cofactors[2]
    determinant = jnp.where(determinant == 0.0, 1.0, determinant)
    return [member / determinant for member in cofactors]


def apply_inverse(inverse, sums):
    return [
        inverse[0] * sums[0] + inverse[1] * sums[1] + inverse[2] * sums[2],
        inverse[1] * sums[0] + inverse[3] * sums[1] + inverse[4] * sums[2],
        inverse[2] * sums[0] + inverse[4] * sums[1] + inverse[5] * sums[2],
    ]


def pack_columns(cols):
    lanes = lane_iota(16, LANES)
    out = jnp.zeros((16, LANES), F32)
    for number, col in enumerate(cols):
        out = jnp.where(lanes == number, col, out)
    return out


def project(cam_ref, jac_ref, errors_ref, values, place):
    high = place >> 7
    low = place & 127
    picked = gather_rows(values, high, low, ROWS)
    adjusted = []
    for row in range(2):
        back = (
            picked[0] * jac_ref[3 * row]
            + picked[1] * jac_ref[3 * row + 1]
            + picked[2] * jac_ref[3 * row + 2]
        )
        adjusted.append(errors_ref[row] - back)
    cols = []
    for column in range(9):
        term = (
            cam_ref[column].astype(F32) * adjusted[0]
            + cam_ref[9 + column].astype(F32) * adjusted[1]
        )
        cols.append(jnp.sum(term, axis=1, keepdims=True))
    return pack_columns(cols)


def next_scatter(
    cam_ref, jac_ref, vector, place, value_ref, high_ref, low_ref,
    mate_ref, other_ref, own_ref, errors_ref,
):
    cameras, width = place.shape
    errors = errors_of(cam_ref, vector, jac_ref[6])
    errors_ref[0] = errors[0]
    errors_ref[1] = errors[1]
    for j in range(3):
        product = errors[0] * jac_ref[j] + errors[1] * jac_ref[3 + j]
        value_ref[2 * j], value_ref[2 * j + 1] = split_two(product)
    high_ref[...] = (place >> 7).astype(F32)
    low_ref[...] = (place & 127).astype(F32)
    total = scatter_rows(
        [(value_ref, number) for number in range(6)], high_ref, low_ref, cameras, width, 8
    )
    blocks = []
    for number in range(3):
        block = fold_parts(total, number)
        own_ref[number] = block
        send_rows(mate_ref, other_ref, number, block)
        blocks.append(block)
    return errors, blocks


def side_kernel(cam_ref, jac_ref, given, precond_ref):
    cols = []
    for column in range(9):
        squared = cam_ref[column].astype(F32) ** 2 + cam_ref[9 + column].astype(F32) ** 2
        cols.append(jnp.sum(squared * jac_ref[6], axis=1, keepdims=True))
    valid = lane_iota(16, LANES) < 9
    precond_ref[...] = jnp.where(valid, 1.0 / (pack_columns(cols) + given[2]), 0.0)


def second_kernel(
    cam_ref, jac_ref, index_ref, errors_in, own_in, mate_in, other_in, state_in, precond_in,
    mate_ref, other_ref, own_ref, errors_ref, inverse_ref, state_ref,
    value_ref, high_ref, low_ref,
):
    blocks = [complete(own_in, mate_in, other_in, number) for number in range(9)]
    inverse = symmetric_inverse(blocks[:6])
    for number in range(6):
        inverse_ref[number] = inverse[number]
    place = index_ref[...]
    values = apply_inverse(inverse, blocks[6:])
    image = project(cam_ref, jac_ref, errors_in, values, place)
    guess, right, damp = state_in[0], state_in[1], state_in[2]
    precond = precond_in[...]
    residual = right - (damp * guess + image)
    scaled = precond * residual
    state_ref[0] = residual
    state_ref[1] = scaled
    state_ref[2] = precond
    next_scatter(
        cam_ref, jac_ref, scaled, place, value_ref, high_ref, low_ref,
        mate_ref, other_ref, own_ref, errors_ref,
    )


def unshared_rows():
    chip = lax.axis_index("chip")
    core = lax.axis_index("core")
    first = jnp.logical_and(chip == 0, core == 0)
    last = jnp.logical_and(chip == lax.axis_size("chip") - 1, core == 1)
    start = jnp.where(first, SIDE, INTERIOR)
    stop = jnp.where(last, SIDE, 0)
    rows = sub_iota(PAD_ROWS, LANES)
    return jnp.logical_or(rows >= start, rows < stop)


def column_sums(block):
    return jnp.sum(block, axis=0, keepdims=True)


def third_kernel(
    cam_ref, jac_ref, index_ref, errors_in, own_in, mate_in, other_in, inverse_in, given, state_in,
    mate_ref, other_ref, own_ref, errors_ref, state_ref, rows_ref,
    value_ref, high_ref, low_ref,
):
    sums = [complete(own_in, mate_in, other_in, number) for number in range(3)]
    inverse = [inverse_in[number] for number in range(6)]
    values = apply_inverse(inverse, sums)
    place = index_ref[...]
    image = project(cam_ref, jac_ref, errors_in, values, place)
    damp = given[2]
    residual, scaled, precond = state_in[0], state_in[1], state_in[2]
    image = damp * scaled + image
    tilde_residual = residual - image
    tilde = precond * tilde_residual
    state_ref[0] = image
    state_ref[1] = tilde_residual
    state_ref[2] = tilde
    errors, blocks = next_scatter(
        cam_ref, jac_ref, tilde, place, value_ref, high_ref, low_ref,
        mate_ref, other_ref, own_ref, errors_ref,
    )
    energy = column_sums(damp * tilde * tilde)
    squares = column_sums(errors[0] * errors[0] + errors[1] * errors[1])
    for start in range(0, squares.shape[1], LANES):
        energy = energy + squares[:, start : start + LANES]
    lone = unshared_rows()
    for value, point in zip(apply_inverse(inverse, blocks), blocks):
        energy = energy - column_sums(jnp.where(lone, value * point, 0.0))
    rows = [
        column_sums(residual * scaled),
        column_sums(image * scaled),
        column_sums(tilde_residual * tilde),
        column_sums(image * tilde),
        column_sums(image * (precond * image)),
        energy,
    ]
    for number, row in enumerate(rows):
        rows_ref[number : number + 1, :] = row
        mate_ref[3 * SIDE + number : 3 * SIDE + number + 1, :] = row


def sum_kernel(own_in, mate_in, other_in, inverse_in, rows_in, values_ref, dots_ref):
    sums = [complete(own_in, mate_in, other_in, number) for number in range(3)]
    inverse = [inverse_in[number] for number in range(6)]
    values = apply_inverse(inverse, sums)
    shared = None
    for number in range(3):
        values_ref[number] = values[number]
        term = values[number] * sums[number]
        shared = term if shared is None else shared + term
    border = column_sums(jnp.where(unshared_rows(), 0.0, shared))
    rows = rows_in[...] + mate_in[3 * SIDE : 3 * SIDE + 6, :]
    rows = rows - jnp.where(sub_iota(6, LANES) == 5, border, 0.0)
    totals = jnp.sum(rows, axis=1, keepdims=True)
    line = column_sums(jnp.where(sub_iota(6, LANES) == lane_iota(6, LANES), totals, 0.0))
    dots_ref[...] = jnp.broadcast_to(line, dots_ref.shape)


def finish_kernel(
    cam_ref, jac_ref, index_ref, errors_in, values_in, given, state_in, tilde_in, dots_ref,
    step_ref, residual_ref, flip_ref,
):
    values = [values_in[number] for number in range(3)]
    image = project(cam_ref, jac_ref, errors_in, values, index_ref[...])
    guess, damp = given[0], given[2]
    scaled, precond = state_in[1], state_in[2]
    first, tilde_residual, tilde = (tilde_in[number] for number in range(3))
    image = damp * tilde + image
    total = column_sums(dots_ref[...])
    inner, curve, tilde_inner, cross, back_inner, tilde_curve = (
        total[:, number : number + 1] for number in range(6)
    )
    mixed = cross - tilde_curve
    back_curve = back_inner - mixed
    first_step = inner / curve
    shift = first_step - 1.0
    inner_next = tilde_inner - 2.0 * shift * cross + shift * shift * back_inner
    curve_next = tilde_curve - 2.0 * shift * mixed + shift * shift * back_curve
    ratio = inner_next / inner
    against = cross - shift * back_inner
    second_step = inner_next / (curve_next + 2.0 * ratio * against + ratio * ratio * curve)
    direction = tilde - shift * (precond * first) + ratio * scaled
    moved = image - shift * (first - image) + ratio * first
    flip_ref[0, :16, :] = guess + first_step * scaled + second_step * direction
    flip_ref[1, :16, :] = tilde_residual - shift * first - second_step * moved
    step_ref[...] = jnp.transpose(flip_ref[0])[:9, :16]
    residual_ref[...] = jnp.transpose(flip_ref[1])[:9, :16]


def vmem(count):
    return [pl.BlockSpec(memory_space=pltpu.VMEM) for _ in range(count)]


def out_f32(*shape):
    return jax.ShapeDtypeStruct(shape, F32)


SEG = ("chip", "core")


def shards(
    cam_jac, point_jac, obs_point, obs_count, back_list, front_list, point_damp, cam_damp,
    right_side, start_guess,
):
    cameras, width = obs_point.shape
    chips = lax.axis_size("chip")
    count = 2 * chips
    mates = [(i, i ^ 1) for i in range(count)]
    others = []
    for i in range(1, count - 1, 2):
        others += [(i, i + 1), (i + 1, i)]
    params = pltpu.CompilerParams(vmem_limit_bytes=16 * 2**20)
    inputs = (
        cam_jac, point_jac, obs_point, obs_count.reshape(1, -1), back_list, front_list,
        point_damp.reshape(-1, LANES), cam_damp.reshape(1, -1), right_side, start_guess,
    )

    def scratch(values):
        return [
            pltpu.VMEM((values, cameras, width), F32),
            pltpu.VMEM((cameras, width), F32),
            pltpu.VMEM((cameras, width), F32),
        ]

    def exchange(to_mate, to_other):
        other = lax.ppermute(to_other, SEG, others)
        mate = lax.ppermute(to_mate, SEG, mates)
        return mate, other

    def call(kernel, name, outs, operands, scratches=(), spaces=None):
        return pl.pallas_call(
            kernel,
            out_shape=outs,
            in_specs=spaces or vmem(len(operands)),
            out_specs=tuple(vmem(len(outs))),
            scratch_shapes=list(scratches),
            compiler_params=params,
            name=name,
        )(*operands)

    plane = out_f32(2, cameras, width)
    to_mate, to_other, own, place, errors, jac, given, cam_jac = call(
        first_kernel,
        "first",
        (
            out_f32(9 * SIDE, LANES),
            out_f32(9 * SIDE, LANES),
            out_f32(9, PAD_ROWS, LANES),
            jax.ShapeDtypeStruct((cameras, width), I32),
            plane,
            out_f32(7, cameras, width),
            out_f32(3, 16, LANES),
            jax.ShapeDtypeStruct(cam_jac.shape, cam_jac.dtype),
        ),
        tuple(pltpu.with_memory_space_constraint(value, pltpu.HBM) for value in inputs),
        scratch(18)
        + [pltpu.VMEM(value.shape, value.dtype) for value in inputs[1:]]
        + [pltpu.VMEM((3, LANES, LANES), F32), pltpu.SemaphoreType.DMA((len(inputs),))],
        [pl.BlockSpec(memory_space=pltpu.HBM) for _ in inputs],
    )
    mate, other = exchange(to_mate, to_other)
    (precond,) = call(side_kernel, "side", (out_f32(16, LANES),), (cam_jac, jac, given))
    own_shape = out_f32(3, PAD_ROWS, LANES)
    to_mate, to_other, own, errors, inverse, state = call(
        second_kernel,
        "second",
        (
            out_f32(3 * SIDE, LANES),
            out_f32(3 * SIDE, LANES),
            own_shape,
            plane,
            out_f32(6, PAD_ROWS, LANES),
            out_f32(3, 16, LANES),
        ),
        (cam_jac, jac, place, errors, own, mate, other, given, precond),
        scratch(6),
    )
    mate, other = exchange(to_mate, to_other)
    to_mate, to_other, own, errors, tilde, rows = call(
        third_kernel,
        "third",
        (
            out_f32(3 * SIDE + 6, LANES),
            out_f32(3 * SIDE, LANES),
            own_shape,
            plane,
            out_f32(3, 16, LANES),
            out_f32(6, LANES),
        ),
        (cam_jac, jac, place, errors, own, mate, other, inverse, given, state),
        scratch(6),
    )
    mate, other = exchange(to_mate, to_other)
    values, dots = call(
        sum_kernel,
        "sum",
        (own_shape, out_f32(chips, LANES)),
        (own, mate, other, inverse, rows),
    )
    dots = lax.all_to_all(dots, "chip", 0, 0, tiled=True)
    return call(
        finish_kernel,
        "finish",
        (out_f32(9, 16), out_f32(9, 16)),
        (cam_jac, jac, place, errors, values, given, state, tilde, dots),
        [pltpu.VMEM((2, LANES, LANES), F32)],
    )


def solution(mesh):
    finer = Mesh(mesh.devices.reshape(-1, 2), SEG)
    return jax.shard_map(
        shards,
        mesh=finer,
        in_specs=(
            P(None, SEG, None),
            P(None, SEG, None),
            P(SEG, None),
            P(SEG),
            P(SEG, None),
            P(SEG, None),
            P(SEG),
            P(SEG),
            P(None, SEG),
            P(None, SEG),
        ),
        out_specs=(P(None, SEG), P(None, SEG)),
        check_vma=False,
    )
```

```python
import jax
import jax.numpy as jnp
from jax import lax
from jax.experimental import pallas as pl
from jax.experimental.pallas import tpu as pltpu
from jax.sharding import Mesh
from jax.sharding import PartitionSpec as P


F32 = jnp.float32
BF16 = jnp.bfloat16
I32 = jnp.int32
LANES = 128
ENTRY_PAIRS = ((0, 0), (0, 1), (0, 2), (1, 1), (1, 2), (2, 2))

SIDE = 6
NEXT_SLOTS = 3
PREV_SLOTS = 6
OWN_FRONT = 9
INTERIOR = 12
ROWS = 14
PAD_ROWS = 16


def row_of(block, index, rows):
    return jnp.broadcast_to(block[index : index + 1, :], (rows, block.shape[1]))


def sub_iota(rows, width):
    return lax.broadcasted_iota(I32, (rows, width), 0)


def lane_iota(rows, width):
    return lax.broadcasted_iota(I32, (rows, width), 1)


def nt(left, right, **kw):
    return lax.dot_general(
        left, right, (((1,), (1,)), ((), ())), preferred_element_type=F32, **kw
    )


def split_two(value):
    high = value.astype(BF16)
    low = (value - high.astype(F32)).astype(BF16)
    return high.astype(F32), low.astype(F32)


def flip_block(block_ref):
    return jnp.transpose(block_ref[...])[:16]


def one_hot_rows(index_row, rows, width):
    packed = jnp.broadcast_to(index_row, (16, width)).astype(BF16)
    parts = []
    for start in range(0, rows, 16):
        ids = (sub_iota(16, width) + start).astype(F32).astype(BF16)
        parts.append(jnp.where(packed == ids, jnp.ones_like(packed), jnp.zeros_like(packed)))
    return parts[0] if len(parts) == 1 else jnp.concatenate(parts, axis=0)


def scatter_rows(value_refs, high_ref, low_ref, cameras, width, group):
    ids = sub_iota(16, width).astype(F32).astype(BF16)

    def step(number, total):
        for inner in range(group):
            pick = pl.ds(number * group + inner, 1)
            lanes = one_hot_rows(low_ref[pick, :], LANES, width).astype(jnp.float8_e4m3fn)
            mask = jnp.broadcast_to(high_ref[pick, :], (16, width)).astype(BF16) == ids
            rows = []
            for ref, index in value_refs:
                spread = jnp.broadcast_to(ref[index, pick, :], (16, width)).astype(BF16)
                rows.append(jnp.where(mask, spread, jnp.zeros_like(spread)))
            piece = nt(jnp.concatenate(rows, axis=0), lanes)
            total = piece if total is None else total + piece
        return total

    if group == cameras:
        return step(0, None)
    start = jnp.zeros((16 * len(value_refs), LANES), F32)
    return lax.fori_loop(0, cameras // group, step, start)


def fold_parts(total, index):
    start = 2 * PAD_ROWS * index
    return total[start : start + PAD_ROWS] + total[start + PAD_ROWS : start + 2 * PAD_ROWS]


def gather_rows(tables, row_index, lane_index, rows):
    halves = []
    for top in range(0, row_index.shape[0], 8):
        pieces = []
        for start in range(0, row_index.shape[1], LANES):
            row_part = row_index[top : top + 8, start : start + LANES]
            lane_part = lane_index[top : top + 8, start : start + LANES]
            outs = [None] * len(tables)
            for row in range(rows):
                here = row_part == row
                for number, table in enumerate(tables):
                    spread = jnp.broadcast_to(table[row : row + 1, :], (8, LANES))
                    got = jnp.take_along_axis(spread, lane_part, axis=1, mode="promise_in_bounds")
                    outs[number] = got if row == 0 else jnp.where(here, got, outs[number])
            pieces.append(outs)
        halves.append([jnp.concatenate([p[n] for p in pieces], axis=1) for n in range(len(tables))])
    return [jnp.concatenate([h[n] for h in halves], axis=0) for n in range(len(tables))]


def errors_of(cam_ref, vector, weights):
    rows = []
    for row in range(2):
        running = None
        for column in range(9):
            term = cam_ref[9 * row + column].astype(F32) * vector[:, column : column + 1]
            running = term if running is None else running + term
        rows.append(running * weights)
    return rows


def send_rows(mate_ref, other_ref, index, block):
    odd = lax.axis_index("core") == 1
    to_next = block[:SIDE]
    to_prev = block[SIDE : 2 * SIDE]
    mate_ref[SIDE * index : SIDE * (index + 1), :] = jnp.where(odd, to_prev, to_next)
    other_ref[SIDE * index : SIDE * (index + 1), :] = jnp.where(odd, to_next, to_prev)


def point_table(back, front):
    border = back.shape[1]
    eight = sub_iota(8, border)
    lanes = lane_iota(8, border)
    lefts, rights = [], []
    for listed, base in ((back, 0), (front, OWN_FRONT)):
        high = listed >> 7
        low = listed & 127
        hit = jnp.broadcast_to(high, (8, border)) == eight
        row_value = ((lanes >> 7) + (base + 1)).astype(F32)
        lane_value = (lanes & 127).astype(F32)
        zero = jnp.zeros((8, border), F32)
        lefts.append(
            jnp.concatenate(
                [jnp.where(hit, row_value, zero), jnp.where(hit, lane_value, zero)], axis=0
            ).astype(BF16)
        )
        rights.append(one_hot_rows(low.astype(F32), LANES, border))
    table = nt(lefts[0], rights[0]) + nt(lefts[1], rights[1])
    row_plus = table[:8]
    lane = table[8:]
    free = jnp.where(row_plus == 0.0, 1.0, 0.0)
    upper = jnp.where(sub_iota(LANES, LANES) <= lane_iota(LANES, LANES), 1.0, 0.0).astype(BF16)
    seen = lax.dot_general(
        free.astype(BF16), upper, (((1,), (0,)), ((), ())), preferred_element_type=F32
    )
    total = jnp.broadcast_to(seen[:, LANES - 1 : LANES], (8, LANES))
    before = jnp.zeros((8, LANES), F32)
    rows = sub_iota(8, LANES)
    for row in range(7):
        before = before + jnp.where(rows > row, row_of(total, row, 8), 0.0)
    rank = before + seen - free
    return jnp.where(
        free > 0.0, rank + float(INTERIOR * LANES), (row_plus - 1.0) * float(LANES) + lane
    ).astype(I32)


def first_kernel(
    cam_hbm, point_hbm, obs_hbm, count_hbm, back_hbm, front_hbm, damp_hbm, cam_damp_hbm,
    right_hbm, guess_hbm,
    mate_ref, other_ref, own_ref, index_ref, errors_ref, jac_ref, state_ref,
    value_ref, high_ref, low_ref,
    cam_ref, point_ref, obs_ref, count_ref, back_ref, front_ref, damp_ref, cam_damp_ref,
    right_ref, guess_ref, flip_ref, sems,
):
    sources = (
        back_hbm, front_hbm, obs_hbm, guess_hbm, right_hbm, cam_damp_hbm, count_hbm, point_hbm,
        cam_hbm, damp_hbm,
    )
    targets = (
        back_ref, front_ref, obs_ref, guess_ref, right_ref, cam_damp_ref, count_ref, point_ref,
        cam_ref, damp_ref,
    )
    copies = [
        pltpu.make_async_copy(source, target, sems.at[number])
        for number, (source, target) in enumerate(zip(sources, targets))
    ]
    for copy in copies:
        copy.start()
    cameras, width = obs_ref.shape
    border = back_ref.shape[1]
    points = damp_ref.shape[0] * damp_ref.shape[1]
    for copy in copies[:2]:
        copy.wait()
    table = point_table(back_ref[...], front_ref[...])
    for copy in copies[2:7]:
        copy.wait()
    observed = obs_ref[...]
    own_place = gather_rows([table], observed >> 7, observed & 127, points // LANES)[0]
    place = jnp.where(
        observed < points,
        own_place,
        jnp.where(
            observed < points + border,
            observed + (PREV_SLOTS * LANES - points),
            observed + (NEXT_SLOTS * LANES - points - border),
        ),
    )
    index_ref[...] = place
    high_ref[...] = (place >> 7).astype(F32)
    low_ref[...] = (place & 127).astype(F32)
    valid = lane_iota(16, LANES) < 9
    flip_ref[0, :9, :16] = guess_ref[...]
    flip_ref[1, :9, :16] = right_ref[...]
    flip_ref[2, 0:1, :16] = cam_damp_ref[...]
    flip_ref[2, 1:2, :16] = count_ref[...].astype(F32)
    guess = jnp.where(valid, flip_block(flip_ref.at[0]), 0.0)
    right = jnp.where(valid, flip_block(flip_ref.at[1]), 0.0)
    sides = flip_block(flip_ref.at[2])
    damp = jnp.where(valid, sides[:, 0:1], 0.0)
    weights = (lane_iota(cameras, width).astype(F32) < sides[:, 1:2]).astype(F32)
    state_ref[0] = guess
    state_ref[1] = right
    state_ref[2] = damp
    copies[7].wait()
    jac = [point_ref[entry].astype(F32) * weights for entry in range(6)]
    for entry in range(6):
        jac_ref[entry] = jac[entry]
    jac_ref[6] = weights
    products = [jac[a] * jac[b] + jac[3 + a] * jac[3 + b] for a, b in ENTRY_PAIRS]
    copies[8].wait()
    copies[9].wait()
    errors = errors_of(cam_ref, guess, weights)
    errors_ref[0] = errors[0]
    errors_ref[1] = errors[1]
    products += [errors[0] * jac[j] + errors[1] * jac[3 + j] for j in range(3)]
    for number, product in enumerate(products):
        value_ref[2 * number], value_ref[2 * number + 1] = split_two(product)
    total = scatter_rows(
        [(value_ref, number) for number in range(18)], high_ref, low_ref, cameras, width, 8
    )
    ids = sub_iota(16, LANES).astype(F32).astype(BF16)
    damping = None
    new_high = (table >> 7).astype(F32)
    new_low = (table & 127).astype(F32)
    first, rest = split_two(damp_ref[...])
    last = damp_ref[...] - first - rest
    for row in range(points // LANES):
        lanes = one_hot_rows(new_low[row : row + 1, :], LANES, LANES)
        mask = row_of(new_high, row, 16).astype(BF16) == ids
        parts = []
        for part in (first, rest, last):
            spread = row_of(part, row, 16).astype(BF16)
            parts.append(jnp.where(mask, spread, jnp.zeros_like(spread)))
        piece = nt(jnp.concatenate(parts, axis=0), lanes)
        damping = piece if damping is None else damping + piece
    damping = damping[:16] + damping[16:32] + damping[32:]
    for number in range(9):
        block = fold_parts(total, number)
        if number in (0, 3, 5):
            block = block + damping
        own_ref[number] = block
        send_rows(mate_ref, other_ref, number, block)


def complete(own_ref, mate_ref, other_ref, number):
    odd = lax.axis_index("core") == 1
    block = own_ref[number]
    mate = mate_ref[SIDE * number : SIDE * (number + 1), :]
    other = other_ref[SIDE * number : SIDE * (number + 1), :]
    after = jnp.where(odd, other, mate)
    before = jnp.where(odd, mate, other)
    tail = jnp.zeros((PAD_ROWS - 2 * SIDE, LANES), F32)
    return block + jnp.concatenate([after, before, tail], axis=0)


def symmetric_inverse(entries):
    cofactors = [
        entries[3] * entries[5] - entries[4] * entries[4],
        entries[2] * entries[4] - entries[1] * entries[5],
        entries[1] * entries[4] - entries[2] * entries[3],
        entries[0] * entries[5] - entries[2] * entries[2],
        entries[1] * entries[2] - entries[0] * entries[4],
        entries[0] * entries[3] - entries[1] * entries[1],
    ]
    determinant = entries[0] * cofactors[0] + entries[1] * cofactors[1] + entries[2] * cofactors[2]
    determinant = jnp.where(determinant == 0.0, 1.0, determinant)
    return [member / determinant for member in cofactors]


def apply_inverse(inverse, sums):
    return [
        inverse[0] * sums[0] + inverse[1] * sums[1] + inverse[2] * sums[2],
        inverse[1] * sums[0] + inverse[3] * sums[1] + inverse[4] * sums[2],
        inverse[2] * sums[0] + inverse[4] * sums[1] + inverse[5] * sums[2],
    ]


def pack_columns(cols):
    lanes = lane_iota(16, LANES)
    out = jnp.zeros((16, LANES), F32)
    for number, col in enumerate(cols):
        out = jnp.where(lanes == number, col, out)
    return out


def project(cam_ref, jac_ref, errors_ref, values, place):
    high = place >> 7
    low = place & 127
    picked = gather_rows(values, high, low, ROWS)
    adjusted = []
    for row in range(2):
        back = (
            picked[0] * jac_ref[3 * row]
            + picked[1] * jac_ref[3 * row + 1]
            + picked[2] * jac_ref[3 * row + 2]
        )
        adjusted.append(errors_ref[row] - back)
    cols = []
    for column in range(9):
        term = (
            cam_ref[column].astype(F32) * adjusted[0]
            + cam_ref[9 + column].astype(F32) * adjusted[1]
        )
        cols.append(jnp.sum(term, axis=1, keepdims=True))
    return pack_columns(cols)


def next_scatter(
    cam_ref, jac_ref, vector, place, value_ref, high_ref, low_ref,
    mate_ref, other_ref, own_ref, errors_ref,
):
    cameras, width = place.shape
    errors = errors_of(cam_ref, vector, jac_ref[6])
    errors_ref[0] = errors[0]
    errors_ref[1] = errors[1]
    for j in range(3):
        product = errors[0] * jac_ref[j] + errors[1] * jac_ref[3 + j]
        value_ref[2 * j], value_ref[2 * j + 1] = split_two(product)
    high_ref[...] = (place >> 7).astype(F32)
    low_ref[...] = (place & 127).astype(F32)
    total = scatter_rows(
        [(value_ref, number) for number in range(6)], high_ref, low_ref, cameras, width, 8
    )
    blocks = []
    for number in range(3):
        block = fold_parts(total, number)
        own_ref[number] = block
        send_rows(mate_ref, other_ref, number, block)
        blocks.append(block)
    return errors, blocks


def side_kernel(cam_ref, jac_ref, given, precond_ref):
    cols = []
    for column in range(9):
        squared = cam_ref[column].astype(F32) ** 2 + cam_ref[9 + column].astype(F32) ** 2
        cols.append(jnp.sum(squared * jac_ref[6], axis=1, keepdims=True))
    valid = lane_iota(16, LANES) < 9
    precond_ref[...] = jnp.where(valid, 1.0 / (pack_columns(cols) + given[2]), 0.0)


def second_kernel(
    cam_ref, jac_ref, index_ref, errors_in, own_in, mate_in, other_in, state_in, precond_in,
    mate_ref, other_ref, own_ref, errors_ref, inverse_ref, state_ref,
    value_ref, high_ref, low_ref,
):
    blocks = [complete(own_in, mate_in, other_in, number) for number in range(9)]
    inverse = symmetric_inverse(blocks[:6])
    for number in range(6):
        inverse_ref[number] = inverse[number]
    place = index_ref[...]
    values = apply_inverse(inverse, blocks[6:])
    image = project(cam_ref, jac_ref, errors_in, values, place)
    guess, right, damp = state_in[0], state_in[1], state_in[2]
    precond = precond_in[...]
    residual = right - (damp * guess + image)
    scaled = precond * residual
    state_ref[0] = residual
    state_ref[1] = scaled
    state_ref[2] = precond
    next_scatter(
        cam_ref, jac_ref, scaled, place, value_ref, high_ref, low_ref,
        mate_ref, other_ref, own_ref, errors_ref,
    )


def unshared_rows():
    chip = lax.axis_index("chip")
    core = lax.axis_index("core")
    first = jnp.logical_and(chip == 0, core == 0)
    last = jnp.logical_and(chip == lax.axis_size("chip") - 1, core == 1)
    start = jnp.where(first, SIDE, INTERIOR)
    stop = jnp.where(last, SIDE, 0)
    rows = sub_iota(PAD_ROWS, LANES)
    return jnp.logical_or(rows >= start, rows < stop)


def column_sums(block):
    return jnp.sum(block, axis=0, keepdims=True)


def third_kernel(
    cam_ref, jac_ref, index_ref, errors_in, own_in, mate_in, other_in, inverse_in, given, state_in,
    mate_ref, other_ref, own_ref, errors_ref, state_ref, rows_ref,
    value_ref, high_ref, low_ref,
):
    sums = [complete(own_in, mate_in, other_in, number) for number in range(3)]
    inverse = [inverse_in[number] for number in range(6)]
    values = apply_inverse(inverse, sums)
    place = index_ref[...]
    image = project(cam_ref, jac_ref, errors_in, values, place)
    damp = given[2]
    residual, scaled, precond = state_in[0], state_in[1], state_in[2]
    image = damp * scaled + image
    tilde_residual = residual - image
    tilde = precond * tilde_residual
    state_ref[0] = image
    state_ref[1] = tilde_residual
    state_ref[2] = tilde
    errors, blocks = next_scatter(
        cam_ref, jac_ref, tilde, place, value_ref, high_ref, low_ref,
        mate_ref, other_ref, own_ref, errors_ref,
    )
    energy = column_sums(damp * tilde * tilde)
    squares = column_sums(errors[0] * errors[0] + errors[1] * errors[1])
    for start in range(0, squares.shape[1], LANES):
        energy = energy + squares[:, start : start + LANES]
    lone = unshared_rows()
    for value, point in zip(apply_inverse(inverse, blocks), blocks):
        energy = energy - column_sums(jnp.where(lone, value * point, 0.0))
    rows = [
        column_sums(residual * scaled),
        column_sums(image * scaled),
        column_sums(tilde_residual * tilde),
        column_sums(image * tilde),
        column_sums(image * (precond * image)),
        energy,
    ]
    for number, row in enumerate(rows):
        rows_ref[number : number + 1, :] = row
        mate_ref[3 * SIDE + number : 3 * SIDE + number + 1, :] = row


def sum_kernel(own_in, mate_in, other_in, inverse_in, rows_in, values_ref, dots_ref):
    sums = [complete(own_in, mate_in, other_in, number) for number in range(3)]
    inverse = [inverse_in[number] for number in range(6)]
    values = apply_inverse(inverse, sums)
    shared = None
    for number in range(3):
        values_ref[number] = values[number]
        term = values[number] * sums[number]
        shared = term if shared is None else shared + term
    border = column_sums(jnp.where(unshared_rows(), 0.0, shared))
    rows = rows_in[...] + mate_in[3 * SIDE : 3 * SIDE + 6, :]
    rows = rows - jnp.where(sub_iota(6, LANES) == 5, border, 0.0)
    totals = jnp.sum(rows, axis=1, keepdims=True)
    line = column_sums(jnp.where(sub_iota(6, LANES) == lane_iota(6, LANES), totals, 0.0))
    dots_ref[...] = jnp.broadcast_to(line, dots_ref.shape)


def finish_kernel(
    cam_ref, jac_ref, index_ref, errors_in, values_in, given, state_in, tilde_in, dots_ref,
    step_ref, residual_ref, flip_ref,
):
    values = [values_in[number] for number in range(3)]
    image = project(cam_ref, jac_ref, errors_in, values, index_ref[...])
    guess, damp = given[0], given[2]
    scaled, precond = state_in[1], state_in[2]
    first, tilde_residual, tilde = (tilde_in[number] for number in range(3))
    image = damp * tilde + image
    total = column_sums(dots_ref[...])
    inner, curve, tilde_inner, cross, back_inner, tilde_curve = (
        total[:, number : number + 1] for number in range(6)
    )
    mixed = cross - tilde_curve
    back_curve = back_inner - mixed
    first_step = inner / curve
    shift = first_step - 1.0
    inner_next = tilde_inner - 2.0 * shift * cross + shift * shift * back_inner
    curve_next = tilde_curve - 2.0 * shift * mixed + shift * shift * back_curve
    ratio = inner_next / inner
    against = cross - shift * back_inner
    second_step = inner_next / (curve_next + 2.0 * ratio * against + ratio * ratio * curve)
    direction = tilde - shift * (precond * first) + ratio * scaled
    moved = image - shift * (first - image) + ratio * first
    flip_ref[0, :16, :] = guess + first_step * scaled + second_step * direction
    flip_ref[1, :16, :] = tilde_residual - shift * first - second_step * moved
    step_ref[...] = jnp.transpose(flip_ref[0])[:9, :16]
    residual_ref[...] = jnp.transpose(flip_ref[1])[:9, :16]


def vmem(count):
    return [pl.BlockSpec(memory_space=pltpu.VMEM) for _ in range(count)]


def out_f32(*shape):
    return jax.ShapeDtypeStruct(shape, F32)


SEG = ("chip", "core")


def shards(
    cam_jac, point_jac, obs_point, obs_count, back_list, front_list, point_damp, cam_damp,
    right_side, start_guess,
):
    cameras, width = obs_point.shape
    chips = lax.axis_size("chip")
    count = 2 * chips
    mates = [(i, i ^ 1) for i in range(count)]
    others = []
    for i in range(1, count - 1, 2):
        others += [(i, i + 1), (i + 1, i)]
    params = pltpu.CompilerParams(vmem_limit_bytes=16 * 2**20)
    inputs = (
        cam_jac, point_jac, obs_point, obs_count.reshape(1, -1), back_list, front_list,
        point_damp.reshape(-1, LANES), cam_damp.reshape(1, -1), right_side, start_guess,
    )

    def scratch(values):
        return [
            pltpu.VMEM((values, cameras, width), F32),
            pltpu.VMEM((cameras, width), F32),
            pltpu.VMEM((cameras, width), F32),
        ]

    def exchange(to_mate, to_other):
        other = lax.ppermute(to_other, SEG, others)
        mate = lax.ppermute(to_mate, SEG, mates)
        return mate, other

    def call(kernel, outs, operands, scratches=(), spaces=None):
        return pl.pallas_call(
            kernel,
            out_shape=outs,
            in_specs=spaces or vmem(len(operands)),
            out_specs=tuple(vmem(len(outs))),
            scratch_shapes=list(scratches),
            compiler_params=params,
        )(*operands)

    plane = out_f32(2, cameras, width)
    to_mate, to_other, own, place, errors, jac, given = call(
        first_kernel,
        (
            out_f32(9 * SIDE, LANES),
            out_f32(9 * SIDE, LANES),
            out_f32(9, PAD_ROWS, LANES),
            jax.ShapeDtypeStruct((cameras, width), I32),
            plane,
            out_f32(7, cameras, width),
            out_f32(3, 16, LANES),
        ),
        tuple(pltpu.with_memory_space_constraint(value, pltpu.HBM) for value in inputs),
        scratch(18)
        + [pltpu.VMEM(value.shape, value.dtype) for value in inputs]
        + [pltpu.VMEM((3, LANES, LANES), F32), pltpu.SemaphoreType.DMA((len(inputs),))],
        [pl.BlockSpec(memory_space=pltpu.HBM) for _ in inputs],
    )
    mate, other = exchange(to_mate, to_other)
    (precond,) = call(side_kernel, (out_f32(16, LANES),), (cam_jac, jac, given))
    own_shape = out_f32(3, PAD_ROWS, LANES)
    to_mate, to_other, own, errors, inverse, state = call(
        second_kernel,
        (
            out_f32(3 * SIDE, LANES),
            out_f32(3 * SIDE, LANES),
            own_shape,
            plane,
            out_f32(6, PAD_ROWS, LANES),
            out_f32(3, 16, LANES),
        ),
        (cam_jac, jac, place, errors, own, mate, other, given, precond),
        scratch(6),
    )
    mate, other = exchange(to_mate, to_other)
    to_mate, to_other, own, errors, tilde, rows = call(
        third_kernel,
        (
            out_f32(3 * SIDE + 6, LANES),
            out_f32(3 * SIDE, LANES),
            own_shape,
            plane,
            out_f32(3, 16, LANES),
            out_f32(6, LANES),
        ),
        (cam_jac, jac, place, errors, own, mate, other, inverse, given, state),
        scratch(6),
    )
    mate, other = exchange(to_mate, to_other)
    values, dots = call(
        sum_kernel, (own_shape, out_f32(chips, LANES)), (own, mate, other, inverse, rows)
    )
    dots = lax.all_to_all(dots, "chip", 0, 0, tiled=True)
    return call(
        finish_kernel,
        (out_f32(9, 16), out_f32(9, 16)),
        (cam_jac, jac, place, errors, values, given, state, tilde, dots),
        [pltpu.VMEM((2, LANES, LANES), F32)],
    )


def solution(mesh):
    finer = Mesh(mesh.devices.reshape(-1, 2), SEG)
    return jax.shard_map(
        shards,
        mesh=finer,
        in_specs=(
            P(None, SEG, None),
            P(None, SEG, None),
            P(SEG, None),
            P(SEG),
            P(SEG, None),
            P(SEG, None),
            P(SEG),
            P(SEG),
            P(None, SEG),
            P(None, SEG),
        ),
        out_specs=(P(None, SEG), P(None, SEG)),
        check_vma=False,
    )
```

```python
import jax
import jax.numpy as jnp
from jax import lax
from jax.experimental import pallas as pl
from jax.experimental.pallas import tpu as pltpu
from jax.sharding import Mesh
from jax.sharding import PartitionSpec as P


F32 = jnp.float32
BF16 = jnp.bfloat16
I32 = jnp.int32
LANES = 128
ENTRY_PAIRS = ((0, 0), (0, 1), (0, 2), (1, 1), (1, 2), (2, 2))

SIDE = 6
NEXT_SLOTS = 3
PREV_SLOTS = 6
OWN_FRONT = 9
INTERIOR = 12
PAD_ROWS = 16


def row_of(block, index, rows):
    return jnp.broadcast_to(block[index : index + 1, :], (rows, block.shape[1]))


def sub_iota(rows, width):
    return lax.broadcasted_iota(I32, (rows, width), 0)


def lane_iota(rows, width):
    return lax.broadcasted_iota(I32, (rows, width), 1)


def nt(left, right, **kw):
    return lax.dot_general(
        left, right, (((1,), (1,)), ((), ())), preferred_element_type=F32, **kw
    )


def split_two(value):
    high = value.astype(BF16)
    low = (value - high.astype(F32)).astype(BF16)
    return high.astype(F32), low.astype(F32)


def flip_block(block_ref):
    return jnp.transpose(block_ref[...])[:16]


def one_hot_rows(index_row, rows, width):
    packed = jnp.broadcast_to(index_row, (16, width)).astype(BF16)
    parts = []
    for start in range(0, rows, 16):
        ids = (sub_iota(16, width) + start).astype(F32).astype(BF16)
        parts.append(jnp.where(packed == ids, jnp.ones_like(packed), jnp.zeros_like(packed)))
    return parts[0] if len(parts) == 1 else jnp.concatenate(parts, axis=0)


def scatter_rows(value_refs, high_ref, low_ref, cameras, width, group):
    ids = sub_iota(16, width).astype(F32).astype(BF16)

    def step(number, total):
        for inner in range(group):
            pick = pl.ds(number * group + inner, 1)
            lanes = one_hot_rows(low_ref[pick, :], LANES, width).astype(jnp.float8_e4m3fn)
            mask = jnp.broadcast_to(high_ref[pick, :], (16, width)).astype(BF16) == ids
            rows = []
            for ref, index in value_refs:
                spread = jnp.broadcast_to(ref[index, pick, :], (16, width)).astype(BF16)
                rows.append(jnp.where(mask, spread, jnp.zeros_like(spread)))
            piece = nt(jnp.concatenate(rows, axis=0), lanes)
            total = piece if total is None else total + piece
        return total

    if group == cameras:
        return step(0, None)
    start = jnp.zeros((16 * len(value_refs), LANES), F32)
    return lax.fori_loop(0, cameras // group, step, start)


def fold_parts(total, index):
    start = 2 * PAD_ROWS * index
    return total[start : start + PAD_ROWS] + total[start + PAD_ROWS : start + 2 * PAD_ROWS]


def gather_rows(tables, row_index, lane_index, rows):
    halves = []
    for top in range(0, row_index.shape[0], 8):
        pieces = []
        for start in range(0, row_index.shape[1], LANES):
            row_part = row_index[top : top + 8, start : start + LANES]
            lane_part = lane_index[top : top + 8, start : start + LANES]
            outs = [None] * len(tables)
            for row in range(rows):
                here = row_part == row
                for number, table in enumerate(tables):
                    spread = jnp.broadcast_to(table[row : row + 1, :], (8, LANES))
                    got = jnp.take_along_axis(spread, lane_part, axis=1, mode="promise_in_bounds")
                    outs[number] = got if row == 0 else jnp.where(here, got, outs[number])
            pieces.append(outs)
        halves.append([jnp.concatenate([p[n] for p in pieces], axis=1) for n in range(len(tables))])
    return [jnp.concatenate([h[n] for h in halves], axis=0) for n in range(len(tables))]


def errors_of(cam_ref, vector, weights):
    rows = []
    for row in range(2):
        running = None
        for column in range(9):
            term = cam_ref[9 * row + column].astype(F32) * vector[:, column : column + 1]
            running = term if running is None else running + term
        rows.append(running * weights)
    return rows


def send_rows(mate_ref, other_ref, index, block):
    odd = lax.axis_index("core") == 1
    to_next = block[:SIDE]
    to_prev = block[SIDE : 2 * SIDE]
    mate_ref[SIDE * index : SIDE * (index + 1), :] = jnp.where(odd, to_prev, to_next)
    other_ref[SIDE * index : SIDE * (index + 1), :] = jnp.where(odd, to_next, to_prev)


def point_table(back, front):
    border = back.shape[1]
    eight = sub_iota(8, border)
    lanes = lane_iota(8, border)
    lefts, rights = [], []
    for listed, base in ((back, 0), (front, OWN_FRONT)):
        high = listed >> 7
        low = listed & 127
        hit = jnp.broadcast_to(high, (8, border)) == eight
        row_value = ((lanes >> 7) + (base + 1)).astype(F32)
        lane_value = (lanes & 127).astype(F32)
        zero = jnp.zeros((8, border), F32)
        lefts.append(
            jnp.concatenate(
                [jnp.where(hit, row_value, zero), jnp.where(hit, lane_value, zero)], axis=0
            ).astype(BF16)
        )
        rights.append(one_hot_rows(low.astype(F32), LANES, border))
    table = nt(lefts[0], rights[0]) + nt(lefts[1], rights[1])
    row_plus = table[:8]
    lane = table[8:]
    free = jnp.where(row_plus == 0.0, 1.0, 0.0)
    upper = jnp.where(sub_iota(LANES, LANES) <= lane_iota(LANES, LANES), 1.0, 0.0).astype(BF16)
    seen = lax.dot_general(
        free.astype(BF16), upper, (((1,), (0,)), ((), ())), preferred_element_type=F32
    )
    total = jnp.broadcast_to(seen[:, LANES - 1 : LANES], (8, LANES))
    before = jnp.zeros((8, LANES), F32)
    rows = sub_iota(8, LANES)
    for row in range(7):
        before = before + jnp.where(rows > row, row_of(total, row, 8), 0.0)
    rank = before + seen - free
    return jnp.where(
        free > 0.0, rank + float(INTERIOR * LANES), (row_plus - 1.0) * float(LANES) + lane
    ).astype(I32)


def first_kernel(
    cam_hbm, point_hbm, obs_hbm, count_hbm, back_hbm, front_hbm, damp_hbm, cam_damp_hbm,
    right_hbm, guess_hbm,
    mate_ref, other_ref, own_ref, index_ref, errors_ref, jac_ref, state_ref,
    value_ref, high_ref, low_ref,
    cam_ref, point_ref, obs_ref, count_ref, back_ref, front_ref, damp_ref, cam_damp_ref,
    right_ref, guess_ref, flip_ref, sems,
):
    sources = (
        back_hbm, front_hbm, obs_hbm, guess_hbm, right_hbm, cam_damp_hbm, count_hbm, point_hbm,
        cam_hbm, damp_hbm,
    )
    targets = (
        back_ref, front_ref, obs_ref, guess_ref, right_ref, cam_damp_ref, count_ref, point_ref,
        cam_ref, damp_ref,
    )
    copies = [
        pltpu.make_async_copy(source, target, sems.at[number])
        for number, (source, target) in enumerate(zip(sources, targets))
    ]
    for copy in copies:
        copy.start()
    cameras, width = obs_ref.shape
    border = back_ref.shape[1]
    points = damp_ref.shape[0] * damp_ref.shape[1]
    for copy in copies[:2]:
        copy.wait()
    table = point_table(back_ref[...], front_ref[...])
    for copy in copies[2:7]:
        copy.wait()
    observed = obs_ref[...]
    own_place = gather_rows([table], observed >> 7, observed & 127, points // LANES)[0]
    place = jnp.where(
        observed < points,
        own_place,
        jnp.where(
            observed < points + border,
            observed + (PREV_SLOTS * LANES - points),
            observed + (NEXT_SLOTS * LANES - points - border),
        ),
    )
    index_ref[...] = place
    high_ref[...] = (place >> 7).astype(F32)
    low_ref[...] = (place & 127).astype(F32)
    valid = lane_iota(16, LANES) < 9
    flip_ref[0, :9, :16] = guess_ref[...]
    flip_ref[1, :9, :16] = right_ref[...]
    flip_ref[2, 0:1, :16] = cam_damp_ref[...]
    flip_ref[2, 1:2, :16] = count_ref[...].astype(F32)
    guess = jnp.where(valid, flip_block(flip_ref.at[0]), 0.0)
    right = jnp.where(valid, flip_block(flip_ref.at[1]), 0.0)
    sides = flip_block(flip_ref.at[2])
    damp = jnp.where(valid, sides[:, 0:1], 0.0)
    weights = (lane_iota(cameras, width).astype(F32) < sides[:, 1:2]).astype(F32)
    state_ref[0] = guess
    state_ref[1] = right
    state_ref[2] = damp
    copies[7].wait()
    jac = [point_ref[entry].astype(F32) * weights for entry in range(6)]
    for entry in range(6):
        jac_ref[entry] = jac[entry]
    jac_ref[6] = weights
    products = [jac[a] * jac[b] + jac[3 + a] * jac[3 + b] for a, b in ENTRY_PAIRS]
    copies[8].wait()
    copies[9].wait()
    ids = sub_iota(16, LANES).astype(F32).astype(BF16)
    damping = None
    new_high = (table >> 7).astype(F32)
    new_low = (table & 127).astype(F32)
    first, rest = split_two(damp_ref[...])
    last = damp_ref[...] - first - rest
    for row in range(points // LANES):
        lanes = one_hot_rows(new_low[row : row + 1, :], LANES, LANES)
        mask = row_of(new_high, row, 16).astype(BF16) == ids
        parts = []
        for part in (first, rest, last):
            spread = row_of(part, row, 16).astype(BF16)
            parts.append(jnp.where(mask, spread, jnp.zeros_like(spread)))
        piece = nt(jnp.concatenate(parts, axis=0), lanes)
        damping = piece if damping is None else damping + piece
    damping = damping[:16] + damping[16:32] + damping[32:]
    errors = errors_of(cam_ref, guess, weights)
    errors_ref[0] = errors[0]
    errors_ref[1] = errors[1]
    products += [errors[0] * jac[j] + errors[1] * jac[3 + j] for j in range(3)]
    for number, product in enumerate(products):
        value_ref[2 * number], value_ref[2 * number + 1] = split_two(product)
    total = scatter_rows(
        [(value_ref, number) for number in range(18)], high_ref, low_ref, cameras, width, 8
    )
    for number in range(9):
        block = fold_parts(total, number)
        if number in (0, 3, 5):
            block = block + damping
        own_ref[number] = block
        send_rows(mate_ref, other_ref, number, block)


def complete(own_ref, mate_ref, other_ref, number):
    odd = lax.axis_index("core") == 1
    block = own_ref[number]
    mate = mate_ref[SIDE * number : SIDE * (number + 1), :]
    other = other_ref[SIDE * number : SIDE * (number + 1), :]
    after = jnp.where(odd, other, mate)
    before = jnp.where(odd, mate, other)
    tail = jnp.zeros((PAD_ROWS - 2 * SIDE, LANES), F32)
    return block + jnp.concatenate([after, before, tail], axis=0)


def symmetric_inverse(entries):
    cofactors = [
        entries[3] * entries[5] - entries[4] * entries[4],
        entries[2] * entries[4] - entries[1] * entries[5],
        entries[1] * entries[4] - entries[2] * entries[3],
        entries[0] * entries[5] - entries[2] * entries[2],
        entries[1] * entries[2] - entries[0] * entries[4],
        entries[0] * entries[3] - entries[1] * entries[1],
    ]
    determinant = entries[0] * cofactors[0] + entries[1] * cofactors[1] + entries[2] * cofactors[2]
    determinant = jnp.where(determinant == 0.0, 1.0, determinant)
    return [member / determinant for member in cofactors]


def apply_inverse(inverse, sums):
    return [
        inverse[0] * sums[0] + inverse[1] * sums[1] + inverse[2] * sums[2],
        inverse[1] * sums[0] + inverse[3] * sums[1] + inverse[4] * sums[2],
        inverse[2] * sums[0] + inverse[4] * sums[1] + inverse[5] * sums[2],
    ]


def pack_columns(cols):
    lanes = lane_iota(16, LANES)
    out = jnp.zeros((16, LANES), F32)
    for number, col in enumerate(cols):
        out = jnp.where(lanes == number, col, out)
    return out


def gather_side(values, place, block_base, rows, extra):
    odd_base, even_base = block_base
    odd = lax.axis_index("core") == 1
    base = jnp.where(odd, odd_base, even_base)
    sides = [
        jnp.where(odd, v[odd_base : odd_base + rows], v[even_base : even_base + rows])
        for v in values
    ]
    lines = [([side[r : r + 1] for side in sides], base + r) for r in range(rows)]
    lines += [([v[r : r + 1] for v in values], r) for r in extra]
    halves = []
    for top in range(0, place.shape[0], 8):
        pieces = []
        for start in range(0, place.shape[1], LANES):
            part = place[top : top + 8, start : start + LANES]
            row_part = part >> 7
            lane_part = part & 127
            outs = [jnp.zeros((8, LANES), F32) for _ in values]
            for tables, number in lines:
                here = row_part == number
                for k, table in enumerate(tables):
                    spread = jnp.broadcast_to(table, (8, LANES))
                    got = jnp.take_along_axis(spread, lane_part, axis=1, mode="promise_in_bounds")
                    outs[k] = jnp.where(here, got, outs[k])
            pieces.append(outs)
        halves.append([jnp.concatenate([p[n] for p in pieces], axis=1) for n in range(3)])
    return [jnp.concatenate([h[n] for h in halves], axis=0) for n in range(3)]


def subtract_points(jac_ref, errors_ref, picked):
    return [
        errors_ref[row]
        - (
            picked[0] * jac_ref[3 * row]
            + picked[1] * jac_ref[3 * row + 1]
            + picked[2] * jac_ref[3 * row + 2]
        )
        for row in range(2)
    ]


def with_mate(own_ref, mate_ref, number):
    odd = lax.axis_index("core") == 1
    mate = mate_ref[SIDE * number : SIDE * (number + 1), :]
    none = jnp.zeros_like(mate)
    tail = jnp.zeros((PAD_ROWS - 2 * SIDE, LANES), F32)
    after = jnp.where(odd, none, mate)
    before = jnp.where(odd, mate, none)
    return own_ref[number] + jnp.concatenate([after, before, tail], axis=0)


def early_first_kernel(jac_ref, index_ref, errors_in, own_in, mate_in, left_ref):
    blocks = [with_mate(own_in, mate_in, number) for number in range(9)]
    values = apply_inverse(symmetric_inverse(blocks[:6]), blocks[6:])
    picked = gather_side(values, index_ref[...], (SIDE, 0), SIDE, (INTERIOR, INTERIOR + 1))
    left_ref[0], left_ref[1] = subtract_points(jac_ref, errors_in, picked)


def early_kernel(jac_ref, index_ref, errors_in, own_in, mate_in, inverse_in, left_ref):
    sums = [with_mate(own_in, mate_in, number) for number in range(3)]
    values = apply_inverse([inverse_in[number] for number in range(6)], sums)
    picked = gather_side(values, index_ref[...], (SIDE, 0), SIDE, (INTERIOR, INTERIOR + 1))
    left_ref[0], left_ref[1] = subtract_points(jac_ref, errors_in, picked)


def project(cam_ref, jac_ref, left_ref, values, place):
    picked = gather_side(values, place, (0, SIDE), SIDE, ())
    adjusted = subtract_points(jac_ref, left_ref, picked)
    cols = []
    for column in range(9):
        term = (
            cam_ref[column].astype(F32) * adjusted[0]
            + cam_ref[9 + column].astype(F32) * adjusted[1]
        )
        cols.append(jnp.sum(term, axis=1, keepdims=True))
    return pack_columns(cols)


def next_scatter(
    cam_ref, jac_ref, vector, place, value_ref, high_ref, low_ref,
    mate_ref, other_ref, own_ref, errors_ref,
):
    cameras, width = place.shape
    errors = errors_of(cam_ref, vector, jac_ref[6])
    errors_ref[0] = errors[0]
    errors_ref[1] = errors[1]
    for j in range(3):
        product = errors[0] * jac_ref[j] + errors[1] * jac_ref[3 + j]
        value_ref[2 * j], value_ref[2 * j + 1] = split_two(product)
    high_ref[...] = (place >> 7).astype(F32)
    low_ref[...] = (place & 127).astype(F32)
    total = scatter_rows(
        [(value_ref, number) for number in range(6)], high_ref, low_ref, cameras, width, 8
    )
    blocks = []
    for number in range(3):
        block = fold_parts(total, number)
        own_ref[number] = block
        send_rows(mate_ref, other_ref, number, block)
        blocks.append(block)
    return errors, blocks


def side_kernel(cam_ref, jac_ref, given, precond_ref):
    cols = []
    for column in range(9):
        squared = cam_ref[column].astype(F32) ** 2 + cam_ref[9 + column].astype(F32) ** 2
        cols.append(jnp.sum(squared * jac_ref[6], axis=1, keepdims=True))
    valid = lane_iota(16, LANES) < 9
    precond_ref[...] = jnp.where(valid, 1.0 / (pack_columns(cols) + given[2]), 0.0)


def second_kernel(
    cam_ref, jac_ref, index_ref, errors_in, own_in, mate_in, other_in, state_in, precond_in,
    mate_ref, other_ref, own_ref, errors_ref, inverse_ref, state_ref,
    value_ref, high_ref, low_ref,
):
    blocks = [complete(own_in, mate_in, other_in, number) for number in range(9)]
    inverse = symmetric_inverse(blocks[:6])
    for number in range(6):
        inverse_ref[number] = inverse[number]
    place = index_ref[...]
    values = apply_inverse(inverse, blocks[6:])
    image = project(cam_ref, jac_ref, errors_in, values, place)
    guess, right, damp = state_in[0], state_in[1], state_in[2]
    precond = precond_in[...]
    residual = right - (damp * guess + image)
    scaled = precond * residual
    state_ref[0] = residual
    state_ref[1] = scaled
    state_ref[2] = precond
    next_scatter(
        cam_ref, jac_ref, scaled, place, value_ref, high_ref, low_ref,
        mate_ref, other_ref, own_ref, errors_ref,
    )


def unshared_rows():
    chip = lax.axis_index("chip")
    core = lax.axis_index("core")
    first = jnp.logical_and(chip == 0, core == 0)
    last = jnp.logical_and(chip == lax.axis_size("chip") - 1, core == 1)
    start = jnp.where(first, SIDE, INTERIOR)
    stop = jnp.where(last, SIDE, 0)
    rows = sub_iota(PAD_ROWS, LANES)
    return jnp.logical_or(rows >= start, rows < stop)


def column_sums(block):
    return jnp.sum(block, axis=0, keepdims=True)


def third_kernel(
    cam_ref, jac_ref, index_ref, errors_in, own_in, mate_in, other_in, inverse_in, given, state_in,
    mate_ref, other_ref, own_ref, errors_ref, state_ref, rows_ref,
    value_ref, high_ref, low_ref,
):
    sums = [complete(own_in, mate_in, other_in, number) for number in range(3)]
    inverse = [inverse_in[number] for number in range(6)]
    values = apply_inverse(inverse, sums)
    place = index_ref[...]
    image = project(cam_ref, jac_ref, errors_in, values, place)
    damp = given[2]
    residual, scaled, precond = state_in[0], state_in[1], state_in[2]
    image = damp * scaled + image
    tilde_residual = residual - image
    tilde = precond * tilde_residual
    state_ref[0] = image
    state_ref[1] = tilde_residual
    state_ref[2] = tilde
    errors, blocks = next_scatter(
        cam_ref, jac_ref, tilde, place, value_ref, high_ref, low_ref,
        mate_ref, other_ref, own_ref, errors_ref,
    )
    energy = column_sums(damp * tilde * tilde)
    squares = column_sums(errors[0] * errors[0] + errors[1] * errors[1])
    for start in range(0, squares.shape[1], LANES):
        energy = energy + squares[:, start : start + LANES]
    lone = unshared_rows()
    for value, point in zip(apply_inverse(inverse, blocks), blocks):
        energy = energy - column_sums(jnp.where(lone, value * point, 0.0))
    rows = [
        column_sums(residual * scaled),
        column_sums(image * scaled),
        column_sums(tilde_residual * tilde),
        column_sums(image * tilde),
        column_sums(image * (precond * image)),
        energy,
    ]
    for number, row in enumerate(rows):
        rows_ref[number : number + 1, :] = row
        mate_ref[3 * SIDE + number : 3 * SIDE + number + 1, :] = row


def sum_kernel(own_in, mate_in, other_in, inverse_in, rows_in, values_ref, dots_ref):
    sums = [complete(own_in, mate_in, other_in, number) for number in range(3)]
    inverse = [inverse_in[number] for number in range(6)]
    values = apply_inverse(inverse, sums)
    shared = None
    for number in range(3):
        values_ref[number] = values[number]
        term = values[number] * sums[number]
        shared = term if shared is None else shared + term
    border = column_sums(jnp.where(unshared_rows(), 0.0, shared))
    rows = rows_in[...] + mate_in[3 * SIDE : 3 * SIDE + 6, :]
    rows = rows - jnp.where(sub_iota(6, LANES) == 5, border, 0.0)
    totals = jnp.sum(rows, axis=1, keepdims=True)
    line = column_sums(jnp.where(sub_iota(6, LANES) == lane_iota(6, LANES), totals, 0.0))
    dots_ref[...] = jnp.broadcast_to(line, dots_ref.shape)


def finish_kernel(
    cam_ref, jac_ref, index_ref, errors_in, values_in, given, state_in, tilde_in, dots_ref,
    step_ref, residual_ref, flip_ref,
):
    values = [values_in[number] for number in range(3)]
    image = project(cam_ref, jac_ref, errors_in, values, index_ref[...])
    guess, damp = given[0], given[2]
    scaled, precond = state_in[1], state_in[2]
    first, tilde_residual, tilde = (tilde_in[number] for number in range(3))
    image = damp * tilde + image
    total = column_sums(dots_ref[...])
    inner, curve, tilde_inner, cross, back_inner, tilde_curve = (
        total[:, number : number + 1] for number in range(6)
    )
    mixed = cross - tilde_curve
    back_curve = back_inner - mixed
    first_step = inner / curve
    shift = first_step - 1.0
    inner_next = tilde_inner - 2.0 * shift * cross + shift * shift * back_inner
    curve_next = tilde_curve - 2.0 * shift * mixed + shift * shift * back_curve
    ratio = inner_next / inner
    against = cross - shift * back_inner
    second_step = inner_next / (curve_next + 2.0 * ratio * against + ratio * ratio * curve)
    direction = tilde - shift * (precond * first) + ratio * scaled
    moved = image - shift * (first - image) + ratio * first
    flip_ref[0, :16, :] = guess + first_step * scaled + second_step * direction
    flip_ref[1, :16, :] = tilde_residual - shift * first - second_step * moved
    step_ref[...] = jnp.transpose(flip_ref[0])[:9, :16]
    residual_ref[...] = jnp.transpose(flip_ref[1])[:9, :16]


def vmem(count):
    return [pl.BlockSpec(memory_space=pltpu.VMEM) for _ in range(count)]


def out_f32(*shape):
    return jax.ShapeDtypeStruct(shape, F32)


SEG = ("chip", "core")


def shards(
    cam_jac, point_jac, obs_point, obs_count, back_list, front_list, point_damp, cam_damp,
    right_side, start_guess,
):
    cameras, width = obs_point.shape
    chips = lax.axis_size("chip")
    count = 2 * chips
    mates = [(i, i ^ 1) for i in range(count)]
    others = []
    for i in range(1, count - 1, 2):
        others += [(i, i + 1), (i + 1, i)]
    params = pltpu.CompilerParams(vmem_limit_bytes=16 * 2**20)
    inputs = (
        cam_jac, point_jac, obs_point, obs_count.reshape(1, -1), back_list, front_list,
        point_damp.reshape(-1, LANES), cam_damp.reshape(1, -1), right_side, start_guess,
    )

    def scratch(values):
        return [
            pltpu.VMEM((values, cameras, width), F32),
            pltpu.VMEM((cameras, width), F32),
            pltpu.VMEM((cameras, width), F32),
        ]

    def exchange(to_mate, to_other):
        other = lax.ppermute(to_other, SEG, others)
        mate = lax.ppermute(to_mate, SEG, mates)
        return mate, other

    def call(kernel, outs, operands, scratches=(), spaces=None):
        return pl.pallas_call(
            kernel,
            out_shape=outs,
            in_specs=spaces or vmem(len(operands)),
            out_specs=tuple(vmem(len(outs))),
            scratch_shapes=list(scratches),
            compiler_params=params,
        )(*operands)

    plane = out_f32(2, cameras, width)
    to_mate, to_other, own, place, errors, jac, given = call(
        first_kernel,
        (
            out_f32(9 * SIDE, LANES),
            out_f32(9 * SIDE, LANES),
            out_f32(9, PAD_ROWS, LANES),
            jax.ShapeDtypeStruct((cameras, width), I32),
            plane,
            out_f32(7, cameras, width),
            out_f32(3, 16, LANES),
        ),
        tuple(pltpu.with_memory_space_constraint(value, pltpu.HBM) for value in inputs),
        scratch(18)
        + [pltpu.VMEM(value.shape, value.dtype) for value in inputs]
        + [pltpu.VMEM((3, LANES, LANES), F32), pltpu.SemaphoreType.DMA((len(inputs),))],
        [pl.BlockSpec(memory_space=pltpu.HBM) for _ in inputs],
    )
    mate, other = exchange(to_mate, to_other)
    (precond,) = call(side_kernel, (out_f32(16, LANES),), (cam_jac, jac, given))
    (left,) = call(early_first_kernel, (plane,), (jac, place, errors, own, mate))
    own_shape = out_f32(3, PAD_ROWS, LANES)
    to_mate, to_other, own, errors, inverse, state = call(
        second_kernel,
        (
            out_f32(3 * SIDE, LANES),
            out_f32(3 * SIDE, LANES),
            own_shape,
            plane,
            out_f32(6, PAD_ROWS, LANES),
            out_f32(3, 16, LANES),
        ),
        (cam_jac, jac, place, left, own, mate, other, given, precond),
        scratch(6),
    )
    mate, other = exchange(to_mate, to_other)
    (left,) = call(early_kernel, (plane,), (jac, place, errors, own, mate, inverse))
    to_mate, to_other, own, errors, tilde, rows = call(
        third_kernel,
        (
            out_f32(3 * SIDE + 6, LANES),
            out_f32(3 * SIDE, LANES),
            own_shape,
            plane,
            out_f32(3, 16, LANES),
            out_f32(6, LANES),
        ),
        (cam_jac, jac, place, left, own, mate, other, inverse, given, state),
        scratch(6),
    )
    mate, other = exchange(to_mate, to_other)
    (left,) = call(early_kernel, (plane,), (jac, place, errors, own, mate, inverse))
    values, dots = call(
        sum_kernel, (own_shape, out_f32(chips, LANES)), (own, mate, other, inverse, rows)
    )
    dots = lax.all_to_all(dots, "chip", 0, 0, tiled=True)
    return call(
        finish_kernel,
        (out_f32(9, 16), out_f32(9, 16)),
        (cam_jac, jac, place, left, values, given, state, tilde, dots),
        [pltpu.VMEM((2, LANES, LANES), F32)],
    )


def solution(mesh):
    finer = Mesh(mesh.devices.reshape(-1, 2), SEG)
    return jax.shard_map(
        shards,
        mesh=finer,
        in_specs=(
            P(None, SEG, None),
            P(None, SEG, None),
            P(SEG, None),
            P(SEG),
            P(SEG, None),
            P(SEG, None),
            P(SEG),
            P(SEG),
            P(None, SEG),
            P(None, SEG),
        ),
        out_specs=(P(None, SEG), P(None, SEG)),
        check_vma=False,
    )
```

```python
import jax
import jax.numpy as jnp
from jax import lax
from jax.experimental import pallas as pl
from jax.experimental.pallas import tpu as pltpu
from jax.sharding import Mesh
from jax.sharding import PartitionSpec as P


F32 = jnp.float32
BF16 = jnp.bfloat16
I32 = jnp.int32
LANES = 128
ENTRY_PAIRS = ((0, 0), (0, 1), (0, 2), (1, 1), (1, 2), (2, 2))

SIDE = 6
NEXT_SLOTS = 3
PREV_SLOTS = 6
OWN_FRONT = 9
INTERIOR = 12
PAD_ROWS = 16


def row_of(block, index, rows):
    return jnp.broadcast_to(block[index : index + 1, :], (rows, block.shape[1]))


def sub_iota(rows, width):
    return lax.broadcasted_iota(I32, (rows, width), 0)


def lane_iota(rows, width):
    return lax.broadcasted_iota(I32, (rows, width), 1)


def nt(left, right, **kw):
    return lax.dot_general(
        left, right, (((1,), (1,)), ((), ())), preferred_element_type=F32, **kw
    )


def split_two(value):
    high = value.astype(BF16)
    low = (value - high.astype(F32)).astype(BF16)
    return high.astype(F32), low.astype(F32)


def flip_block(block_ref):
    return jnp.transpose(block_ref[...])[:16]


def one_hot_rows(index_row, rows, width):
    packed = jnp.broadcast_to(index_row, (16, width)).astype(BF16)
    parts = []
    for start in range(0, rows, 16):
        ids = (sub_iota(16, width) + start).astype(F32).astype(BF16)
        parts.append(jnp.where(packed == ids, jnp.ones_like(packed), jnp.zeros_like(packed)))
    return parts[0] if len(parts) == 1 else jnp.concatenate(parts, axis=0)


def scatter_rows(value_refs, high_ref, low_ref, cameras, width, group):
    ids = sub_iota(16, width).astype(F32).astype(BF16)

    def step(number, total):
        for inner in range(group):
            pick = pl.ds(number * group + inner, 1)
            lanes = one_hot_rows(low_ref[pick, :], LANES, width).astype(jnp.float8_e4m3fn)
            mask = jnp.broadcast_to(high_ref[pick, :], (16, width)).astype(BF16) == ids
            rows = []
            for ref, index in value_refs:
                spread = jnp.broadcast_to(ref[index, pick, :], (16, width)).astype(BF16)
                rows.append(jnp.where(mask, spread, jnp.zeros_like(spread)))
            piece = nt(jnp.concatenate(rows, axis=0), lanes)
            total = piece if total is None else total + piece
        return total

    if group == cameras:
        return step(0, None)
    start = jnp.zeros((16 * len(value_refs), LANES), F32)
    return lax.fori_loop(0, cameras // group, step, start)


def fold_parts(total, index):
    start = 2 * PAD_ROWS * index
    return total[start : start + PAD_ROWS] + total[start + PAD_ROWS : start + 2 * PAD_ROWS]


def gather_rows(tables, row_index, lane_index, rows):
    halves = []
    for top in range(0, row_index.shape[0], 8):
        pieces = []
        for start in range(0, row_index.shape[1], LANES):
            row_part = row_index[top : top + 8, start : start + LANES]
            lane_part = lane_index[top : top + 8, start : start + LANES]
            outs = [None] * len(tables)
            for row in range(rows):
                here = row_part == row
                for number, table in enumerate(tables):
                    spread = jnp.broadcast_to(table[row : row + 1, :], (8, LANES))
                    got = jnp.take_along_axis(spread, lane_part, axis=1, mode="promise_in_bounds")
                    outs[number] = got if row == 0 else jnp.where(here, got, outs[number])
            pieces.append(outs)
        halves.append([jnp.concatenate([p[n] for p in pieces], axis=1) for n in range(len(tables))])
    return [jnp.concatenate([h[n] for h in halves], axis=0) for n in range(len(tables))]


def errors_of(cam_ref, vector, weights):
    rows = []
    for row in range(2):
        running = None
        for column in range(9):
            term = cam_ref[9 * row + column].astype(F32) * vector[:, column : column + 1]
            running = term if running is None else running + term
        rows.append(running * weights)
    return rows


def send_rows(mate_ref, other_ref, index, block):
    odd = lax.axis_index("core") == 1
    to_next = block[:SIDE]
    to_prev = block[SIDE : 2 * SIDE]
    mate_ref[SIDE * index : SIDE * (index + 1), :] = jnp.where(odd, to_prev, to_next)
    other_ref[SIDE * index : SIDE * (index + 1), :] = jnp.where(odd, to_next, to_prev)


def point_table(back, front):
    border = back.shape[1]
    eight = sub_iota(8, border)
    lanes = lane_iota(8, border)
    lefts, rights = [], []
    for listed, base in ((back, 0), (front, OWN_FRONT)):
        high = listed >> 7
        low = listed & 127
        hit = jnp.broadcast_to(high, (8, border)) == eight
        row_value = ((lanes >> 7) + (base + 1)).astype(F32)
        lane_value = (lanes & 127).astype(F32)
        zero = jnp.zeros((8, border), F32)
        lefts.append(
            jnp.concatenate(
                [jnp.where(hit, row_value, zero), jnp.where(hit, lane_value, zero)], axis=0
            ).astype(BF16)
        )
        rights.append(one_hot_rows(low.astype(F32), LANES, border))
    table = nt(lefts[0], rights[0]) + nt(lefts[1], rights[1])
    row_plus = table[:8]
    lane = table[8:]
    free = jnp.where(row_plus == 0.0, 1.0, 0.0)
    upper = jnp.where(sub_iota(LANES, LANES) <= lane_iota(LANES, LANES), 1.0, 0.0).astype(BF16)
    seen = lax.dot_general(
        free.astype(BF16), upper, (((1,), (0,)), ((), ())), preferred_element_type=F32
    )
    total = jnp.broadcast_to(seen[:, LANES - 1 : LANES], (8, LANES))
    before = jnp.zeros((8, LANES), F32)
    rows = sub_iota(8, LANES)
    for row in range(7):
        before = before + jnp.where(rows > row, row_of(total, row, 8), 0.0)
    rank = before + seen - free
    return jnp.where(
        free > 0.0, rank + float(INTERIOR * LANES), (row_plus - 1.0) * float(LANES) + lane
    ).astype(I32)


def first_kernel(
    cam_hbm, point_hbm, obs_hbm, count_hbm, back_hbm, front_hbm, damp_hbm, cam_damp_hbm,
    right_hbm, guess_hbm,
    mate_ref, other_ref, own_ref, index_ref, errors_ref, jac_ref, state_ref, cam_ref,
    value_ref, high_ref, low_ref,
    point_ref, obs_ref, count_ref, back_ref, front_ref, damp_ref, cam_damp_ref,
    right_ref, guess_ref, flip_ref, sems,
):
    sources = (
        back_hbm, front_hbm, obs_hbm, guess_hbm, right_hbm, cam_damp_hbm, count_hbm, point_hbm,
        cam_hbm, damp_hbm,
    )
    targets = (
        back_ref, front_ref, obs_ref, guess_ref, right_ref, cam_damp_ref, count_ref, point_ref,
        cam_ref, damp_ref,
    )
    copies = [
        pltpu.make_async_copy(source, target, sems.at[number])
        for number, (source, target) in enumerate(zip(sources, targets))
    ]
    for copy in copies:
        copy.start()
    cameras, width = obs_ref.shape
    border = back_ref.shape[1]
    points = damp_ref.shape[0] * damp_ref.shape[1]
    for copy in copies[:2]:
        copy.wait()
    table = point_table(back_ref[...], front_ref[...])
    copies[2].wait()
    observed = obs_ref[...]
    own_place = gather_rows([table], observed >> 7, observed & 127, points // LANES)[0]
    place = jnp.where(
        observed < points,
        own_place,
        jnp.where(
            observed < points + border,
            observed + (PREV_SLOTS * LANES - points),
            observed + (NEXT_SLOTS * LANES - points - border),
        ),
    )
    index_ref[...] = place
    high_ref[...] = (place >> 7).astype(F32)
    low_ref[...] = (place & 127).astype(F32)
    valid = lane_iota(16, LANES) < 9
    for copy in copies[3:7]:
        copy.wait()
    flip_ref[0, :9, :16] = guess_ref[...]
    flip_ref[1, :9, :16] = right_ref[...]
    flip_ref[2, 0:1, :16] = cam_damp_ref[...]
    flip_ref[2, 1:2, :16] = count_ref[...].astype(F32)
    guess = jnp.where(valid, flip_block(flip_ref.at[0]), 0.0)
    right = jnp.where(valid, flip_block(flip_ref.at[1]), 0.0)
    sides = flip_block(flip_ref.at[2])
    damp = jnp.where(valid, sides[:, 0:1], 0.0)
    weights = (lane_iota(cameras, width).astype(F32) < sides[:, 1:2]).astype(F32)
    state_ref[0] = guess
    state_ref[1] = right
    state_ref[2] = damp
    copies[7].wait()
    jac = [point_ref[entry].astype(F32) * weights for entry in range(6)]
    for entry in range(6):
        jac_ref[entry] = jac[entry]
    jac_ref[6] = weights
    products = [jac[a] * jac[b] + jac[3 + a] * jac[3 + b] for a, b in ENTRY_PAIRS]
    copies[8].wait()
    copies[9].wait()
    ids = sub_iota(16, LANES).astype(F32).astype(BF16)
    damping = None
    new_high = (table >> 7).astype(F32)
    new_low = (table & 127).astype(F32)
    first, rest = split_two(damp_ref[...])
    last = damp_ref[...] - first - rest
    for row in range(points // LANES):
        lanes = one_hot_rows(new_low[row : row + 1, :], LANES, LANES)
        mask = row_of(new_high, row, 16).astype(BF16) == ids
        parts = []
        for part in (first, rest, last):
            spread = row_of(part, row, 16).astype(BF16)
            parts.append(jnp.where(mask, spread, jnp.zeros_like(spread)))
        piece = nt(jnp.concatenate(parts, axis=0), lanes)
        damping = piece if damping is None else damping + piece
    damping = damping[:16] + damping[16:32] + damping[32:]
    errors = errors_of(cam_ref, guess, weights)
    errors_ref[0] = errors[0]
    errors_ref[1] = errors[1]
    products += [errors[0] * jac[j] + errors[1] * jac[3 + j] for j in range(3)]
    for number, product in enumerate(products):
        value_ref[2 * number], value_ref[2 * number + 1] = split_two(product)
    total = scatter_rows(
        [(value_ref, number) for number in range(18)], high_ref, low_ref, cameras, width, 8
    )
    for number in range(9):
        block = fold_parts(total, number)
        if number in (0, 3, 5):
            block = block + damping
        own_ref[number] = block
        send_rows(mate_ref, other_ref, number, block)


def complete(own_ref, mate_ref, other_ref, number):
    odd = lax.axis_index("core") == 1
    block = own_ref[number]
    mate = mate_ref[SIDE * number : SIDE * (number + 1), :]
    other = other_ref[SIDE * number : SIDE * (number + 1), :]
    after = jnp.where(odd, other, mate)
    before = jnp.where(odd, mate, other)
    tail = jnp.zeros((PAD_ROWS - 2 * SIDE, LANES), F32)
    return block + jnp.concatenate([after, before, tail], axis=0)


def symmetric_inverse(entries):
    cofactors = [
        entries[3] * entries[5] - entries[4] * entries[4],
        entries[2] * entries[4] - entries[1] * entries[5],
        entries[1] * entries[4] - entries[2] * entries[3],
        entries[0] * entries[5] - entries[2] * entries[2],
        entries[1] * entries[2] - entries[0] * entries[4],
        entries[0] * entries[3] - entries[1] * entries[1],
    ]
    determinant = entries[0] * cofactors[0] + entries[1] * cofactors[1] + entries[2] * cofactors[2]
    determinant = jnp.where(determinant == 0.0, 1.0, determinant)
    return [member / determinant for member in cofactors]


def apply_inverse(inverse, sums):
    return [
        inverse[0] * sums[0] + inverse[1] * sums[1] + inverse[2] * sums[2],
        inverse[1] * sums[0] + inverse[3] * sums[1] + inverse[4] * sums[2],
        inverse[2] * sums[0] + inverse[4] * sums[1] + inverse[5] * sums[2],
    ]


def pack_columns(cols):
    lanes = lane_iota(16, LANES)
    out = jnp.zeros((16, LANES), F32)
    for number, col in enumerate(cols):
        out = jnp.where(lanes == number, col, out)
    return out


def gather_side(values, place, block_base, rows, extra):
    odd_base, even_base = block_base
    odd = lax.axis_index("core") == 1
    base = jnp.where(odd, odd_base, even_base)
    sides = [
        jnp.where(odd, v[odd_base : odd_base + rows], v[even_base : even_base + rows])
        for v in values
    ]
    lines = [([side[r : r + 1] for side in sides], base + r) for r in range(rows)]
    lines += [([v[r : r + 1] for v in values], r) for r in extra]
    halves = []
    for top in range(0, place.shape[0], 8):
        pieces = []
        for start in range(0, place.shape[1], LANES):
            part = place[top : top + 8, start : start + LANES]
            row_part = part >> 7
            lane_part = part & 127
            outs = [jnp.zeros((8, LANES), F32) for _ in values]
            for tables, number in lines:
                here = row_part == number
                for k, table in enumerate(tables):
                    spread = jnp.broadcast_to(table, (8, LANES))
                    got = jnp.take_along_axis(spread, lane_part, axis=1, mode="promise_in_bounds")
                    outs[k] = jnp.where(here, got, outs[k])
            pieces.append(outs)
        halves.append([jnp.concatenate([p[n] for p in pieces], axis=1) for n in range(3)])
    return [jnp.concatenate([h[n] for h in halves], axis=0) for n in range(3)]


def subtract_points(jac_ref, errors_ref, picked):
    return [
        errors_ref[row]
        - (
            picked[0] * jac_ref[3 * row]
            + picked[1] * jac_ref[3 * row + 1]
            + picked[2] * jac_ref[3 * row + 2]
        )
        for row in range(2)
    ]


def with_mate(own_ref, mate_ref, number):
    odd = lax.axis_index("core") == 1
    mate = mate_ref[SIDE * number : SIDE * (number + 1), :]
    none = jnp.zeros_like(mate)
    tail = jnp.zeros((PAD_ROWS - 2 * SIDE, LANES), F32)
    after = jnp.where(odd, none, mate)
    before = jnp.where(odd, mate, none)
    return own_ref[number] + jnp.concatenate([after, before, tail], axis=0)


def early_first_kernel(jac_ref, index_ref, errors_in, own_in, mate_in, left_ref):
    blocks = [with_mate(own_in, mate_in, number) for number in range(9)]
    values = apply_inverse(symmetric_inverse(blocks[:6]), blocks[6:])
    picked = gather_side(values, index_ref[...], (SIDE, 0), SIDE, (INTERIOR, INTERIOR + 1))
    left_ref[0], left_ref[1] = subtract_points(jac_ref, errors_in, picked)


def early_kernel(jac_ref, index_ref, errors_in, own_in, mate_in, inverse_in, left_ref):
    sums = [with_mate(own_in, mate_in, number) for number in range(3)]
    values = apply_inverse([inverse_in[number] for number in range(6)], sums)
    picked = gather_side(values, index_ref[...], (SIDE, 0), SIDE, (INTERIOR, INTERIOR + 1))
    left_ref[0], left_ref[1] = subtract_points(jac_ref, errors_in, picked)


def project(cam_ref, jac_ref, left_ref, values, place):
    picked = gather_side(values, place, (0, SIDE), SIDE, ())
    adjusted = subtract_points(jac_ref, left_ref, picked)
    cols = []
    for column in range(9):
        term = (
            cam_ref[column].astype(F32) * adjusted[0]
            + cam_ref[9 + column].astype(F32) * adjusted[1]
        )
        cols.append(jnp.sum(term, axis=1, keepdims=True))
    return pack_columns(cols)


def next_scatter(
    cam_ref, jac_ref, vector, place, value_ref, high_ref, low_ref,
    mate_ref, other_ref, own_ref, errors_ref,
):
    cameras, width = place.shape
    errors = errors_of(cam_ref, vector, jac_ref[6])
    errors_ref[0] = errors[0]
    errors_ref[1] = errors[1]
    for j in range(3):
        product = errors[0] * jac_ref[j] + errors[1] * jac_ref[3 + j]
        value_ref[2 * j], value_ref[2 * j + 1] = split_two(product)
    high_ref[...] = (place >> 7).astype(F32)
    low_ref[...] = (place & 127).astype(F32)
    total = scatter_rows(
        [(value_ref, number) for number in range(6)], high_ref, low_ref, cameras, width, 8
    )
    blocks = []
    for number in range(3):
        block = fold_parts(total, number)
        own_ref[number] = block
        send_rows(mate_ref, other_ref, number, block)
        blocks.append(block)
    return errors, blocks


def side_kernel(cam_ref, jac_ref, given, precond_ref):
    cols = []
    for column in range(9):
        squared = cam_ref[column].astype(F32) ** 2 + cam_ref[9 + column].astype(F32) ** 2
        cols.append(jnp.sum(squared * jac_ref[6], axis=1, keepdims=True))
    valid = lane_iota(16, LANES) < 9
    precond_ref[...] = jnp.where(valid, 1.0 / (pack_columns(cols) + given[2]), 0.0)


def second_kernel(
    cam_ref, jac_ref, index_ref, errors_in, own_in, mate_in, other_in, state_in, precond_in,
    mate_ref, other_ref, own_ref, errors_ref, inverse_ref, state_ref,
    value_ref, high_ref, low_ref,
):
    blocks = [complete(own_in, mate_in, other_in, number) for number in range(9)]
    inverse = symmetric_inverse(blocks[:6])
    for number in range(6):
        inverse_ref[number] = inverse[number]
    place = index_ref[...]
    values = apply_inverse(inverse, blocks[6:])
    image = project(cam_ref, jac_ref, errors_in, values, place)
    guess, right, damp = state_in[0], state_in[1], state_in[2]
    precond = precond_in[...]
    residual = right - (damp * guess + image)
    scaled = precond * residual
    state_ref[0] = residual
    state_ref[1] = scaled
    state_ref[2] = precond
    next_scatter(
        cam_ref, jac_ref, scaled, place, value_ref, high_ref, low_ref,
        mate_ref, other_ref, own_ref, errors_ref,
    )


def unshared_rows():
    chip = lax.axis_index("chip")
    core = lax.axis_index("core")
    first = jnp.logical_and(chip == 0, core == 0)
    last = jnp.logical_and(chip == lax.axis_size("chip") - 1, core == 1)
    start = jnp.where(first, SIDE, INTERIOR)
    stop = jnp.where(last, SIDE, 0)
    rows = sub_iota(PAD_ROWS, LANES)
    return jnp.logical_or(rows >= start, rows < stop)


def column_sums(block):
    return jnp.sum(block, axis=0, keepdims=True)


def third_kernel(
    cam_ref, jac_ref, index_ref, errors_in, own_in, mate_in, other_in, inverse_in, given, state_in,
    mate_ref, other_ref, own_ref, errors_ref, state_ref, rows_ref,
    value_ref, high_ref, low_ref,
):
    sums = [complete(own_in, mate_in, other_in, number) for number in range(3)]
    inverse = [inverse_in[number] for number in range(6)]
    values = apply_inverse(inverse, sums)
    place = index_ref[...]
    image = project(cam_ref, jac_ref, errors_in, values, place)
    damp = given[2]
    residual, scaled, precond = state_in[0], state_in[1], state_in[2]
    image = damp * scaled + image
    tilde_residual = residual - image
    tilde = precond * tilde_residual
    state_ref[0] = image
    state_ref[1] = tilde_residual
    state_ref[2] = tilde
    errors, blocks = next_scatter(
        cam_ref, jac_ref, tilde, place, value_ref, high_ref, low_ref,
        mate_ref, other_ref, own_ref, errors_ref,
    )
    energy = column_sums(damp * tilde * tilde)
    squares = column_sums(errors[0] * errors[0] + errors[1] * errors[1])
    for start in range(0, squares.shape[1], LANES):
        energy = energy + squares[:, start : start + LANES]
    lone = unshared_rows()
    for value, point in zip(apply_inverse(inverse, blocks), blocks):
        energy = energy - column_sums(jnp.where(lone, value * point, 0.0))
    rows = [
        column_sums(residual * scaled),
        column_sums(image * scaled),
        column_sums(tilde_residual * tilde),
        column_sums(image * tilde),
        column_sums(image * (precond * image)),
        energy,
    ]
    for number, row in enumerate(rows):
        rows_ref[number : number + 1, :] = row
        mate_ref[3 * SIDE + number : 3 * SIDE + number + 1, :] = row


def sum_kernel(own_in, mate_in, other_in, inverse_in, rows_in, values_ref, dots_ref):
    sums = [complete(own_in, mate_in, other_in, number) for number in range(3)]
    inverse = [inverse_in[number] for number in range(6)]
    values = apply_inverse(inverse, sums)
    shared = None
    for number in range(3):
        values_ref[number] = values[number]
        term = values[number] * sums[number]
        shared = term if shared is None else shared + term
    border = column_sums(jnp.where(unshared_rows(), 0.0, shared))
    rows = rows_in[...] + mate_in[3 * SIDE : 3 * SIDE + 6, :]
    rows = rows - jnp.where(sub_iota(6, LANES) == 5, border, 0.0)
    totals = jnp.sum(rows, axis=1, keepdims=True)
    line = column_sums(jnp.where(sub_iota(6, LANES) == lane_iota(6, LANES), totals, 0.0))
    dots_ref[...] = jnp.broadcast_to(line, dots_ref.shape)


def finish_kernel(
    cam_ref, jac_ref, index_ref, errors_in, values_in, given, state_in, tilde_in, dots_ref,
    step_ref, residual_ref, flip_ref,
):
    values = [values_in[number] for number in range(3)]
    image = project(cam_ref, jac_ref, errors_in, values, index_ref[...])
    guess, damp = given[0], given[2]
    scaled, precond = state_in[1], state_in[2]
    first, tilde_residual, tilde = (tilde_in[number] for number in range(3))
    image = damp * tilde + image
    total = column_sums(dots_ref[...])
    inner, curve, tilde_inner, cross, back_inner, tilde_curve = (
        total[:, number : number + 1] for number in range(6)
    )
    mixed = cross - tilde_curve
    back_curve = back_inner - mixed
    first_step = inner / curve
    shift = first_step - 1.0
    inner_next = tilde_inner - 2.0 * shift * cross + shift * shift * back_inner
    curve_next = tilde_curve - 2.0 * shift * mixed + shift * shift * back_curve
    ratio = inner_next / inner
    against = cross - shift * back_inner
    second_step = inner_next / (curve_next + 2.0 * ratio * against + ratio * ratio * curve)
    direction = tilde - shift * (precond * first) + ratio * scaled
    moved = image - shift * (first - image) + ratio * first
    flip_ref[0, :16, :] = guess + first_step * scaled + second_step * direction
    flip_ref[1, :16, :] = tilde_residual - shift * first - second_step * moved
    step_ref[...] = jnp.transpose(flip_ref[0])[:9, :16]
    residual_ref[...] = jnp.transpose(flip_ref[1])[:9, :16]


def vmem(count):
    return [pl.BlockSpec(memory_space=pltpu.VMEM) for _ in range(count)]


def out_f32(*shape):
    return jax.ShapeDtypeStruct(shape, F32)


SEG = ("chip", "core")


def shards(
    cam_jac, point_jac, obs_point, obs_count, back_list, front_list, point_damp, cam_damp,
    right_side, start_guess,
):
    cameras, width = obs_point.shape
    chips = lax.axis_size("chip")
    count = 2 * chips
    mates = [(i, i ^ 1) for i in range(count)]
    others = []
    for i in range(1, count - 1, 2):
        others += [(i, i + 1), (i + 1, i)]
    params = pltpu.CompilerParams(vmem_limit_bytes=16 * 2**20)
    inputs = (
        cam_jac, point_jac, obs_point, obs_count.reshape(1, -1), back_list, front_list,
        point_damp.reshape(-1, LANES), cam_damp.reshape(1, -1), right_side, start_guess,
    )

    def scratch(values):
        return [
            pltpu.VMEM((values, cameras, width), F32),
            pltpu.VMEM((cameras, width), F32),
            pltpu.VMEM((cameras, width), F32),
        ]

    def exchange(to_mate, to_other):
        other = lax.ppermute(to_other, SEG, others)
        mate = lax.ppermute(to_mate, SEG, mates)
        return mate, other

    def call(kernel, outs, operands, scratches=(), spaces=None):
        return pl.pallas_call(
            kernel,
            out_shape=outs,
            in_specs=spaces or vmem(len(operands)),
            out_specs=tuple(vmem(len(outs))),
            scratch_shapes=list(scratches),
            compiler_params=params,
        )(*operands)

    plane = out_f32(2, cameras, width)
    to_mate, to_other, own, place, errors, jac, given, cam_jac = call(
        first_kernel,
        (
            out_f32(9 * SIDE, LANES),
            out_f32(9 * SIDE, LANES),
            out_f32(9, PAD_ROWS, LANES),
            jax.ShapeDtypeStruct((cameras, width), I32),
            plane,
            out_f32(7, cameras, width),
            out_f32(3, 16, LANES),
            jax.ShapeDtypeStruct(cam_jac.shape, cam_jac.dtype),
        ),
        tuple(pltpu.with_memory_space_constraint(value, pltpu.HBM) for value in inputs),
        scratch(18)
        + [pltpu.VMEM(value.shape, value.dtype) for value in inputs[1:]]
        + [pltpu.VMEM((3, LANES, LANES), F32), pltpu.SemaphoreType.DMA((len(inputs),))],
        [pl.BlockSpec(memory_space=pltpu.HBM) for _ in inputs],
    )
    mate, other = exchange(to_mate, to_other)
    (precond,) = call(side_kernel, (out_f32(16, LANES),), (cam_jac, jac, given))
    (left,) = call(early_first_kernel, (plane,), (jac, place, errors, own, mate))
    own_shape = out_f32(3, PAD_ROWS, LANES)
    to_mate, to_other, own, errors, inverse, state = call(
        second_kernel,
        (
            out_f32(3 * SIDE, LANES),
            out_f32(3 * SIDE, LANES),
            own_shape,
            plane,
            out_f32(6, PAD_ROWS, LANES),
            out_f32(3, 16, LANES),
        ),
        (cam_jac, jac, place, left, own, mate, other, given, precond),
        scratch(6),
    )
    mate, other = exchange(to_mate, to_other)
    (left,) = call(early_kernel, (plane,), (jac, place, errors, own, mate, inverse))
    to_mate, to_other, own, errors, tilde, rows = call(
        third_kernel,
        (
            out_f32(3 * SIDE + 6, LANES),
            out_f32(3 * SIDE, LANES),
            own_shape,
            plane,
            out_f32(3, 16, LANES),
            out_f32(6, LANES),
        ),
        (cam_jac, jac, place, left, own, mate, other, inverse, given, state),
        scratch(6),
    )
    mate, other = exchange(to_mate, to_other)
    (left,) = call(early_kernel, (plane,), (jac, place, errors, own, mate, inverse))
    values, dots = call(
        sum_kernel, (own_shape, out_f32(chips, LANES)), (own, mate, other, inverse, rows)
    )
    dots = lax.all_to_all(dots, "chip", 0, 0, tiled=True)
    return call(
        finish_kernel,
        (out_f32(9, 16), out_f32(9, 16)),
        (cam_jac, jac, place, left, values, given, state, tilde, dots),
        [pltpu.VMEM((2, LANES, LANES), F32)],
    )


def solution(mesh):
    finer = Mesh(mesh.devices.reshape(-1, 2), SEG)
    return jax.shard_map(
        shards,
        mesh=finer,
        in_specs=(
            P(None, SEG, None),
            P(None, SEG, None),
            P(SEG, None),
            P(SEG),
            P(SEG, None),
            P(SEG, None),
            P(SEG),
            P(SEG),
            P(None, SEG),
            P(None, SEG),
        ),
        out_specs=(P(None, SEG), P(None, SEG)),
        check_vma=False,
    )
```
